32 devices in a mesh: ta: 4 (over z), gz: 4 (over x, core), gy: 2 (over y).
Axes of the slice: x: 2, y: 2, z: 4, core: 2. Of those that a mesh axis runs over, the one named last changes fastest.
Arguments:
- source: float32 [2, 4, 3, 16, 16, 256], P(None, None, None, 'ta', 'gz', 'gy'), may hold values from -6 to 6
- start_guess: float32 [2, 4, 3, 16, 16, 256], P(None, None, None, 'ta', 'gz', 'gy'), may hold values from -3 to 3
- gauge_links: float32 [4, 2, 3, 3, 16, 16, 256], P(None, None, None, None, 'ta', 'gz', 'gy'), may hold values from -1 to 1, as said below
- clover: float32 [2, 2, 6, 6, 16, 16, 256], P(None, None, None, None, 'ta', 'gz', 'gy'), may hold values from -1.5 to 5.9, as said below
Outputs:
- update: float32 [2, 4, 3, 16, 16, 256], P(None, None, None, 'ta', 'gz', 'gy')
- profile: float32 [16], P('ta')
The draws below stay inside these ranges and needn't reach their ends.
Inputs may be any that keep to these rules, and one draw needn't show every extreme that they name: `gauge_links`: every link is a special unitary 3x3 matrix. `clover`: each chiral block is Hermitian.
All inputs are finite; a program needn't handle non-finite values.
Results may differ from the reference program's by a relative error of at most 0.0003.
Values sent between devices are 32-bit elements; how exact they have to be, the bound alone decides.
A program may use at most 64 MiB of HBM per device.

```python
import jax
import jax.numpy as jnp
import numpy as np
from jax import lax

LX = 32
BLOCK = 4
MR_STEPS = 4
NT = 16
NZ = 16
NY = 8
NX = 32


def normalise(vec_re, vec_im):
    inverse_norm = lax.rsqrt(jnp.sum(vec_re * vec_re + vec_im * vec_im, axis=1, keepdims=True))
    return (vec_re * inverse_norm, vec_im * inverse_norm)


def draw_gauge_links(key, part):
    raw_draw = jax.random.normal(jax.random.fold_in(key, 11), (4, 2, 2, 3, NT, NZ, NY * NX), jnp.float32)
    first_re, first_im = normalise(raw_draw[:, 0, 0], raw_draw[:, 0, 1])
    other_re = raw_draw[:, 1, 0]
    other_im = raw_draw[:, 1, 1]
    inner_re = jnp.sum(first_re * other_re + first_im * other_im, axis=1, keepdims=True)
    inner_im = jnp.sum(first_re * other_im - first_im * other_re, axis=1, keepdims=True)
    second_re, second_im = normalise(other_re - (inner_re * first_re - inner_im * first_im), other_im - (inner_re * first_im + inner_im * first_re))
    third_re = []
    third_im = []
    for colour_index in range(3):
        next_one = (colour_index + 1) % 3
        next_two = (colour_index + 2) % 3
        cross_re = first_re[:, next_one] * second_re[:, next_two] - first_im[:, next_one] * second_im[:, next_two] - (first_re[:, next_two] * second_re[:, next_one] - first_im[:, next_two] * second_im[:, next_one])
        cross_im = first_re[:, next_one] * second_im[:, next_two] + first_im[:, next_one] * second_re[:, next_two] - (first_re[:, next_two] * second_im[:, next_one] + first_im[:, next_two] * second_re[:, next_one])
        third_re.append(cross_re)
        third_im.append(-cross_im)
    link_re = jnp.stack([first_re, second_re, jnp.stack(third_re, axis=1)], axis=1)
    link_im = jnp.stack([first_im, second_im, jnp.stack(third_im, axis=1)], axis=1)
    return jnp.stack([link_re, link_im], axis=1)


def draw_clover(key, part):
    full_shape = (2, 2, 6, 6, NT, NZ, NY * NX)
    raw_draw = jnp.clip(0.3 * jax.random.normal(jax.random.fold_in(key, 23), full_shape, jnp.float32), -1.5, 1.5)
    herm_re = 0.5 * (raw_draw[:, 0] + jnp.swapaxes(raw_draw[:, 0], 1, 2))
    herm_im = 0.5 * (raw_draw[:, 1] - jnp.swapaxes(raw_draw[:, 1], 1, 2))
    diagonal = 4.4 * jnp.eye(6, dtype=jnp.float32)[None, :, :, None, None, None]
    return jnp.stack([herm_re + diagonal, herm_im], axis=1)


def shard_levels(own_key, shape, shards, least, high):
    def one(axis_at, blocks):
        steps = jax.random.uniform(jax.random.fold_in(jax.random.fold_in(own_key, 6), axis_at), (blocks,), jnp.float32, least / len(shards), high / len(shards))
        return jnp.repeat(jnp.exp(steps), shape[axis_at] // blocks).reshape((-1,) + (1,) * (len(shape) - axis_at - 1))

    loudness = one(*shards[0])
    for cut in shards[1:]:
        loudness = loudness * one(*cut)
    return loudness


def gaussian(stream_key, extent, spread, bound, cuts=(), held_as=jnp.bfloat16):
    values = jax.random.normal(stream_key, extent, jnp.float32) * spread
    if len(cuts) > 0:
        values = shard_levels(stream_key, extent, cuts, -0.22, 0.18) * values
    return jnp.clip(values, min=-bound, max=bound).astype(held_as)


def setup_inputs(seed: int = 0) -> dict:
    key_of = jax.random.split(jax.random.key(seed), 5)
    return {
        "source": gaussian(key_of[0], (2, 4, 3, NT, NZ, NY * NX), 1.0, 6.0, ((3, 4), (4, 4), (5, 2)), jnp.float32),
        "start_guess": gaussian(key_of[1], (2, 4, 3, NT, NZ, NY * NX), 0.5, 3.0, ((3, 4), (4, 4), (5, 2)), jnp.float32),
        "gauge_links": draw_gauge_links(jax.random.fold_in(key_of[4], 71), 0),
        "clover": draw_clover(jax.random.fold_in(key_of[4], 71), 0),
    }


EPSILON = 1e-6


def upper_pair(direction):
    if direction == 0:
        return np.eye(2), np.zeros((2, 2))
    if direction == 1:
        return np.zeros((2, 2)), -np.array([[1.0, 0.0], [0.0, -1.0]])
    if direction == 2:
        return np.array([[0.0, -1.0], [1.0, 0.0]]), np.zeros((2, 2))
    return np.zeros((2, 2)), -np.array([[0.0, 1.0], [1.0, 0.0]])


def hop_table(direction, sign_flip):
    upper_re, upper_im = upper_pair(direction)
    table_re = np.eye(4)
    table_im = np.zeros((4, 4))
    table_re[:2, 2:] = sign_flip * upper_re
    table_im[:2, 2:] = sign_flip * upper_im
    table_re[2:, :2] = sign_flip * upper_re.T
    table_im[2:, :2] = -sign_flip * upper_im.T
    return table_re, table_im


def spin_apply(spin_tables, spinor):
    table_re, table_im = spin_tables
    re_rows = []
    im_rows = []
    for row_index in range(table_re.shape[0]):
        result_re = jnp.zeros_like(spinor[0, 0])
        result_im = jnp.zeros_like(spinor[0, 0])
        for col_index in range(table_re.shape[1]):
            coef_re = float(table_re[row_index, col_index])
            coef_im = float(table_im[row_index, col_index])
            if coef_re != 0.0:
                result_re = result_re + coef_re * spinor[0, col_index]
                result_im = result_im + coef_re * spinor[1, col_index]
            if coef_im != 0.0:
                result_re = result_re - coef_im * spinor[1, col_index]
                result_im = result_im + coef_im * spinor[0, col_index]
        re_rows.append(result_re)
        im_rows.append(result_im)
    return jnp.stack([jnp.stack(re_rows), jnp.stack(im_rows)])


def colour_apply(gauge_link, spinor):
    result_re = jnp.zeros((spinor.shape[1],) + gauge_link.shape[1:2] + spinor.shape[3:], spinor.dtype)
    result_im = jnp.zeros_like(result_re)
    for col_index in range(3):
        link_re = gauge_link[0, :, col_index][None]
        link_im = gauge_link[1, :, col_index][None]
        vec_re = spinor[0, :, col_index][:, None]
        vec_im = spinor[1, :, col_index][:, None]
        result_re = result_re + link_re * vec_re - link_im * vec_im
        result_im = result_im + link_re * vec_im + link_im * vec_re
    return jnp.stack([result_re, result_im])


def colour_adjoint(gauge_link, spinor):
    result_re = jnp.zeros((spinor.shape[1],) + gauge_link.shape[1:2] + spinor.shape[3:], spinor.dtype)
    result_im = jnp.zeros_like(result_re)
    for col_index in range(3):
        link_re = gauge_link[0, col_index, :][None]
        link_im = gauge_link[1, col_index, :][None]
        vec_re = spinor[0, :, col_index][:, None]
        vec_im = spinor[1, :, col_index][:, None]
        result_re = result_re + link_re * vec_re + link_im * vec_im
        result_im = result_im + link_re * vec_im - link_im * vec_re
    return jnp.stack([result_re, result_im])


def site_apply(clover, spinor):
    halves = spinor.reshape((2, 2, 6) + spinor.shape[3:])
    result_re = jnp.zeros(halves.shape[1:], spinor.dtype)
    result_im = jnp.zeros_like(result_re)
    for col_index in range(6):
        matrix_re = clover[:, 0, :, col_index]
        matrix_im = clover[:, 1, :, col_index]
        vec_re = halves[0][:, col_index][:, None]
        vec_im = halves[1][:, col_index][:, None]
        result_re = result_re + matrix_re * vec_re - matrix_im * vec_im
        result_im = result_im + matrix_re * vec_im + matrix_im * vec_re
    return jnp.stack([result_re, result_im]).reshape(spinor.shape)


def local_neighbour(spinor, direction, offset):
    if direction == 0:
        return jnp.roll(spinor, -offset, axis=3)
    if direction == 1:
        return jnp.roll(spinor, -offset, axis=4)
    if direction == 2:
        return jnp.roll(spinor, -offset * LX, axis=5)
    shifted = jnp.roll(spinor, -offset, axis=5)
    wrapped = jnp.roll(spinor, offset * (LX - 1), axis=5)
    position = jnp.arange(spinor.shape[5]) % LX
    edge_index = LX - 1 if offset > 0 else 0
    return jnp.where(position == edge_index, wrapped, shifted)


def lattice_neighbour(spinor, direction, offset):
    rolled = local_neighbour(spinor, direction, offset)
    if direction != 0:
        return rolled
    edge_index = NT - 1 if offset > 0 else 0
    sign_flip = jnp.where(jnp.arange(NT) == edge_index, -1.0, 1.0).astype(jnp.float32)
    return rolled * sign_flip[:, None, None]


def block_mask(site_shape, direction, offset):
    if direction == 0:
        coordinate = jnp.arange(site_shape[0])[:, None, None]
    elif direction == 1:
        coordinate = jnp.arange(site_shape[1])[None, :, None]
    elif direction == 2:
        coordinate = (jnp.arange(site_shape[2]) // LX)[None, None, :]
    else:
        coordinate = (jnp.arange(site_shape[2]) % LX)[None, None, :]
    position = coordinate % BLOCK
    edge_index = BLOCK - 1 if offset > 0 else 0
    return (position != edge_index).astype(jnp.float32)


def apply_operator(spinor, gauge_links, clover, neighbour, masked):
    summed = site_apply(clover, spinor)
    site_shape = spinor.shape[3:]
    for direction in range(4):
        gauge_link = gauge_links[direction]
        forward = spin_apply(hop_table(direction, -1.0), colour_apply(gauge_link, neighbour(spinor, direction, 1)))
        behind = spin_apply(hop_table(direction, 1.0), neighbour(colour_adjoint(gauge_link, spinor), direction, -1))
        if masked:
            forward = forward * block_mask(site_shape, direction, 1)
            behind = behind * block_mask(site_shape, direction, -1)
        summed = summed - 0.5 * (forward + behind)
    return summed


def block_spread(site_values):
    time_len, depth_len, flat_len = site_values.shape
    rows_len = flat_len // LX
    blocked = site_values.reshape((time_len // BLOCK, BLOCK, depth_len // BLOCK, BLOCK, rows_len // BLOCK, BLOCK, LX // BLOCK, BLOCK))
    totals = jnp.sum(blocked, axis=(1, 3, 5, 7), keepdims=True)
    return jnp.broadcast_to(totals, blocked.shape).reshape(site_values.shape)


def minimal_residual(initial_residual, gauge_links, clover):
    correction = jnp.zeros_like(initial_residual)
    remainder = initial_residual
    for repeat in range(MR_STEPS):
        applied = apply_operator(remainder, gauge_links, clover, local_neighbour, True)
        margin_re = block_spread(jnp.sum(applied[0] * remainder[0] + applied[1] * remainder[1], axis=(0, 1)))
        margin_im = block_spread(jnp.sum(applied[0] * remainder[1] - applied[1] * remainder[0], axis=(0, 1)))
        norm_sq = block_spread(jnp.sum(applied * applied, axis=(0, 1, 2))) + EPSILON
        alpha_re = margin_re / norm_sq
        alpha_im = margin_im / norm_sq
        correction = correction + jnp.stack([alpha_re * remainder[0] - alpha_im * remainder[1], alpha_re * remainder[1] + alpha_im * remainder[0]])
        remainder = remainder - jnp.stack([alpha_re * applied[0] - alpha_im * applied[1], alpha_re * applied[1] + alpha_im * applied[0]])
    return correction, remainder


def reference(source, start_guess, gauge_links, clover):
    initial_residual = source - apply_operator(start_guess, gauge_links, clover, lattice_neighbour, False)
    correction, remainder = minimal_residual(initial_residual, gauge_links, clover)
    update = start_guess + correction
    latest = source - apply_operator(update, gauge_links, clover, lattice_neighbour, False)
    profile = jnp.sum(latest * latest, axis=(0, 1, 2, 4, 5)) / jnp.sum(source * source, axis=(0, 1, 2, 4, 5))
    return update, profile
```

```python
import functools

import jax
import jax.numpy as jnp
from jax import lax
from jax.experimental import pallas as pl
from jax.experimental.pallas import tpu as pltpu
from jax.sharding import PartitionSpec as P

LX = 32
BLOCK = 4
MR_STEPS = 4
EPSILON = 1e-6
AXES = ("ta", "gz", "gy")
RE, IM = 0, 1
SUB, LANE = 8, 128
VMEM_LIMIT = 24 * 2**20

PAIR = (
    {(0, RE): (1, RE, 0), (0, IM): (1, IM, 0), (1, RE): (1, RE, 1), (1, IM): (1, IM, 1)},
    {(0, RE): (1, IM, 0), (0, IM): (-1, RE, 0), (1, RE): (-1, IM, 1), (1, IM): (1, RE, 1)},
    {(0, RE): (-1, RE, 1), (0, IM): (-1, IM, 1), (1, RE): (1, RE, 0), (1, IM): (1, IM, 0)},
    {(0, RE): (1, IM, 1), (0, IM): (-1, RE, 1), (1, RE): (1, IM, 0), (1, IM): (-1, RE, 0)},
)
PAIR_H = (
    {(0, RE): (1, RE, 0), (0, IM): (1, IM, 0), (1, RE): (1, RE, 1), (1, IM): (1, IM, 1)},
    {(0, RE): (-1, IM, 0), (0, IM): (1, RE, 0), (1, RE): (1, IM, 1), (1, IM): (-1, RE, 1)},
    {(0, RE): (1, RE, 1), (0, IM): (1, IM, 1), (1, RE): (-1, RE, 0), (1, IM): (-1, IM, 0)},
    {(0, RE): (-1, IM, 1), (0, IM): (1, RE, 1), (1, RE): (-1, IM, 0), (1, IM): (1, RE, 0)},
)


def signed_add(base, sign, value):
    return base + value if sign > 0 else base - value


def project(field, mu, s):
    parts = ([], [])
    for part in (RE, IM):
        for colour in range(3):
            spins = []
            for spin in range(2):
                sign, from_part, from_spin = PAIR[mu][(spin, part)]
                spins.append(
                    signed_add(field[part, spin, colour], -s * sign, field[from_part, 2 + from_spin, colour])
                )
            parts[part].append(jnp.stack(spins))
    return parts


def link_row(links, mu, row, half):
    re = im = None
    for col in range(3):
        u_re, u_im = links[mu, RE, row, col][None], links[mu, IM, row, col][None]
        h_re, h_im = half[RE][col], half[IM][col]
        t_re = u_re * h_re - u_im * h_im
        t_im = u_re * h_im + u_im * h_re
        re, im = (t_re, t_im) if re is None else (re + t_re, im + t_im)
    return re, im


def adjoint_row(links, mu, row, half):
    re = im = None
    for col in range(3):
        u_re, u_im = links[mu, RE, col, row][None], links[mu, IM, col, row][None]
        h_re, h_im = half[RE][col], half[IM][col]
        t_re = u_re * h_re + u_im * h_im
        t_im = u_re * h_im - u_im * h_re
        re, im = (t_re, t_im) if re is None else (re + t_re, im + t_im)
    return re, im


def add_hops(acc, mu, colour, ahead, behind):
    difference = tuple(b - a for a, b in zip(ahead, behind))
    for part in (RE, IM):
        acc[part, 0:2, colour] += ahead[part] + behind[part]
        for spin in range(2):
            sign, from_part, from_spin = PAIR_H[mu][(spin, part)]
            old = acc[part, 2 + spin, colour]
            acc[part, 2 + spin, colour] = signed_add(old, sign, difference[from_part][from_spin])


def site_term(clover, field, emit):
    def pair(part, index):
        return jnp.stack([field[part, index // 3, index % 3], field[part, 2 + index // 3, index % 3]])

    vec = [[pair(part, j) for j in range(6)] for part in (RE, IM)]
    for row in range(6):
        diagonal = clover[:, RE, row, row]
        re, im = diagonal * vec[RE][row], diagonal * vec[IM][row]
        for col in range(6):
            if col == row:
                continue
            low, high = min(row, col), max(row, col)
            m_re, m_im = clover[:, RE, low, high], clover[:, IM, low, high]
            if row < col:
                re = re + m_re * vec[RE][col] - m_im * vec[IM][col]
                im = im + m_re * vec[IM][col] + m_im * vec[RE][col]
            else:
                re = re + m_re * vec[RE][col] + m_im * vec[IM][col]
                im = im + m_re * vec[IM][col] - m_im * vec[RE][col]
        for chirality in range(2):
            emit(RE, 2 * chirality + row // 3, row % 3, re[chirality])
            emit(IM, 2 * chirality + row // 3, row % 3, im[chirality])


def swap_halves(value):
    axis = value.ndim - 3
    return jnp.concatenate(
        [lax.slice_in_dim(value, 1, 2, axis=axis), lax.slice_in_dim(value, 0, 1, axis=axis)], axis=axis
    )


def turn(value, shift, axis):
    shift = shift % value.shape[axis]
    return pltpu.roll(value, shift, axis) if shift else value


def cyclic(value, mu, units, early):
    axis = value.ndim - 2
    if mu == 3:
        return turn(value, units, axis + 1)
    if mu == 2:
        return turn(value, units * LX, axis + 1)
    if mu == 1:
        return turn(value, units, axis)
    units = units % BLOCK
    if units == 0:
        return value
    if units == 2:
        return swap_halves(value)
    rolled = turn(value, BLOCK, axis)
    swapped = swap_halves(rolled)
    return jnp.where(early, swapped, rolled) if units == 1 else jnp.where(early, rolled, swapped)


def kernel(
    sizes, x_in, source_in, links_in, clover_in, update_out, profile_out,
    x, source, links, clover, inner, rest, corr, acc, behind_store,
    send_buf, recv_buf, stat_send, stat_recv,
    in_sem, send_sem, recv_sem, stat_send_sem, stat_recv_sem,
):
    count = {axis: size for axis, size in zip(AXES, sizes)}
    group = count["gz"] * count["gy"]
    me = {axis: lax.axis_index(axis) for axis in AXES}

    def peer(index):
        return {
            "gz": lax.rem(me["gz"] + index // count["gy"], count["gz"]),
            "gy": lax.rem(me["gy"] + index % count["gy"], count["gy"]),
        }

    def beside(axis, step):
        return {axis: lax.rem(me[axis] + step + count[axis], count[axis])}

    barrier = pltpu.get_barrier_semaphore()
    for step in (1, -1):
        pl.semaphore_signal(barrier, inc=1, device_id=beside("ta", step), device_id_type=pl.DeviceIdType.MESH)
    loads = [pltpu.make_async_copy(x_in, x, in_sem.at[0])]
    loads += [pltpu.make_async_copy(links_in.at[mu], links.at[mu], in_sem.at[1 + mu]) for mu in range(4)]
    loads.append(pltpu.make_async_copy(clover_in, clover, in_sem.at[5]))
    loads.append(pltpu.make_async_copy(source_in, source, in_sem.at[6]))
    for load in loads:
        load.start()

    for index in range(1, group):
        pl.semaphore_signal(barrier, inc=1, device_id=peer(index), device_id_type=pl.DeviceIdType.MESH)

    site = (2, SUB, LANE)
    row = lax.broadcasted_iota(jnp.int32, site, 1)
    lane = lax.broadcasted_iota(jnp.int32, site, 2)
    coord = (
        lax.broadcasted_iota(jnp.int32, site, 0) * 2 + row // BLOCK,
        row % BLOCK,
        lane // LX,
        lane % LX,
    )
    early = row < BLOCK
    high = tuple(c % BLOCK == BLOCK - 1 for c in coord)

    def x_neighbour(value, step):
        axis = value.ndim - 1
        if step > 0:
            return jnp.where(coord[3] == LX - 1, turn(value, LX - 1, axis), turn(value, -1, axis))
        return jnp.where(coord[3] == 0, turn(value, 1 - LX, axis), turn(value, 1, axis))

    def flat(half):
        return [half[part][colour][spin] for part in (RE, IM) for spin in range(2) for colour in range(3)]

    def pack(half, mu, edge, store, factor=None):
        values = flat(half)
        for j in range(3):
            packed = cyclic(values[4 * j], mu, -edge, early)
            for k in range(1, BLOCK):
                packed = jnp.where(coord[mu] == k, cyclic(values[4 * j + k], mu, k - edge, early), packed)
            store[j] = packed if factor is None else packed * factor

    def unpack(store, mu, edge):
        values = []
        for j in range(3):
            packed = store[j]
            values += [cyclic(packed, mu, edge - k, early) for k in range(BLOCK)]
        return [[jnp.stack([values[6 * p + c], values[6 * p + 3 + c]]) for c in range(3)] for p in (RE, IM)]

    def face_copy(turn_index, mu, side):
        slot = turn_index * 6 + mu * 2 + side
        return pltpu.make_async_remote_copy(
            src_ref=send_buf.at[slot],
            dst_ref=recv_buf.at[slot],
            send_sem=send_sem,
            recv_sem=recv_sem.at[turn_index * 3 + mu],
            device_id=beside(AXES[mu], -1 if side == 0 else 1),
            device_id_type=pl.DeviceIdType.MESH,
        )

    def faces_wait(turn_index, mu):
        pair = recv_buf.at[pl.ds(turn_index * 6 + mu * 2, 2)]
        pltpu.make_async_copy(pair, pair, recv_sem.at[turn_index * 3 + mu]).wait()

    def start_wrapped_first(turn_index):
        last = me["ta"] == count["ta"] - 1

        @pl.when(last)
        def _():
            face_copy(turn_index, 0, 1).start()
            face_copy(turn_index, 0, 0).start()

        @pl.when(jnp.logical_not(last))
        def _():
            face_copy(turn_index, 0, 0).start()
            face_copy(turn_index, 0, 1).start()

    first_t = jnp.where(me["ta"] == 0, -1.0, 1.0).astype(jnp.float32)
    last_t = jnp.where(me["ta"] == count["ta"] - 1, -1.0, 1.0).astype(jnp.float32)

    def prepare_ahead(turn_index, field, mu):
        pack(project(field, mu, 1), mu, 0, send_buf.at[turn_index * 6 + mu * 2], first_t if mu == 0 else None)

    def prepare_behind(turn_index, field, mu, keep):
        half = project(field, mu, -1)
        rows = [adjoint_row(links, mu, a, half) for a in range(3)]
        behind = [[rows[a][part] for a in range(3)] for part in (RE, IM)]
        pack(behind, mu, BLOCK - 1, send_buf.at[turn_index * 6 + mu * 2 + 1], last_t if mu == 0 else None)
        if keep:
            for part in (RE, IM):
                for a in range(3):
                    behind_store[mu, part, a] = behind[part][a]

    loads[0].wait()
    prepare_ahead(0, x, 0)
    loads[1].wait()
    prepare_behind(0, x, 0, True)
    prepare_ahead(0, x, 2)
    pl.semaphore_wait(barrier, group - 1 + 2)
    start_wrapped_first(0)
    face_copy(0, 2, 0).start()
    loads[3].wait()
    prepare_behind(0, x, 2, True)
    face_copy(0, 2, 1).start()
    prepare_ahead(0, x, 1)
    face_copy(0, 1, 0).start()
    loads[2].wait()
    prepare_behind(0, x, 1, True)
    face_copy(0, 1, 1).start()

    def zero_acc():
        acc[...] = jnp.zeros_like(acc)

    zero_acc()
    loads[4].wait()

    def x_hops(field):
        ahead_half = [[x_neighbour(v, 1) for v in values] for values in project(field, 3, 1)]
        behind_half = project(field, 3, -1)
        for a in range(3):
            ahead = link_row(links, 3, a, ahead_half)
            behind = tuple(x_neighbour(v, -1) for v in adjoint_row(links, 3, a, behind_half))
            yield a, ahead, behind

    for a, ahead, behind in x_hops(x):
        add_hops(acc, 3, a, ahead, behind)

    for mu in range(4):
        factor = jnp.where(high[mu], 0.0, -0.5).astype(jnp.float32)
        for part in (RE, IM):
            for a in range(3):
                inner[mu, part, a] = links[mu, part, a] * factor[None]

    loads[5].wait()
    loads[6].wait()

    def emit_rest(part, spin, colour, value):
        rest[part, spin, colour] = source[part, spin, colour] - value

    site_term(clover, x, emit_rest)
    source_sq = jnp.zeros(site, jnp.float32)
    for part in (RE, IM):
        for spin in range(4):
            for colour in range(3):
                value = source[part, spin, colour]
                source_sq = source_sq + value * value

    def slice_sums(value):
        sums = jnp.broadcast_to(jnp.sum(value, axis=2, keepdims=True), site)
        picked = jnp.where(coord[0] == lane, sums, 0.0)
        return jnp.sum(picked[0] + picked[1], axis=0, keepdims=True)

    stat_send[1:2] = slice_sums(source_sq)

    for mu in (1, 2, 0):
        faces_wait(0, mu)
        arrived = unpack(recv_buf.at[mu * 2], mu, BLOCK - 1)
        local = project(x, mu, 1)
        ahead_half = [
            [
                jnp.where(coord[mu] == BLOCK - 1, arrived[part][c], cyclic(local[part][c], mu, -1, early))
                for c in range(3)
            ]
            for part in (RE, IM)
        ]
        below = unpack(recv_buf.at[mu * 2 + 1], mu, 0)
        for a in range(3):
            ahead = link_row(links, mu, a, ahead_half)
            behind = tuple(
                jnp.where(coord[mu] == 0, below[part][a], cyclic(behind_store[mu, part, a], mu, 1, early))
                for part in (RE, IM)
            )
            add_hops(acc, mu, a, ahead, behind)

    for part in (RE, IM):
        for spin in range(4):
            rest[part, spin] += 0.5 * acc[part, spin]
            corr[part, spin] = jnp.zeros_like(corr[part, spin])

    row8 = lax.broadcasted_iota(jnp.int32, (SUB, LANE), 0)
    lane8 = lax.broadcasted_iota(jnp.int32, (SUB, LANE), 1)

    def block_sums(values):
        packed = None
        for index, value in enumerate(values):
            total = jnp.sum(value[0] + value[1], axis=0, keepdims=True)
            total = jnp.broadcast_to(total, (SUB, LANE))
            packed = total if packed is None else jnp.where(row8 == index, total, packed)
        place = lane8 % BLOCK
        total = None
        for offset in range(1 - BLOCK, BLOCK):
            moved = [turn(packed, start - offset, 1) for start in range(0, LANE, LX)]
            while len(moved) > 1:
                moved = [p + q for p, q in zip(moved[::2], moved[1::2])]
            part = moved[0]
            if offset:
                part = jnp.where((place + offset >= 0) & (place + offset < BLOCK), part, 0.0)
            total = part if total is None else total + part
        packed = total
        return [jnp.broadcast_to(packed[i : i + 1], (SUB, LANE)) for i in range(len(values))]

    def mr_step(_, carry):
        def emit(part, spin, colour, value):
            acc[part, spin, colour] = value

        site_term(clover, rest, emit)
        for mu in range(4):
            ahead_half = [[cyclic(v, mu, -1, early) for v in values] for values in project(rest, mu, 1)]
            behind_half = project(rest, mu, -1)
            for a in range(3):
                ahead = link_row(inner, mu, a, ahead_half)
                behind = tuple(cyclic(v, mu, 1, early) for v in adjoint_row(inner, mu, a, behind_half))
                add_hops(acc, mu, a, ahead, behind)
        margin_re = margin_im = norm = jnp.zeros(site, jnp.float32)
        for spin in range(4):
            for colour in range(3):
                a_re, a_im = acc[RE, spin, colour], acc[IM, spin, colour]
                r_re, r_im = rest[RE, spin, colour], rest[IM, spin, colour]
                margin_re = margin_re + (a_re * r_re + a_im * r_im)
                margin_im = margin_im + (a_re * r_im - a_im * r_re)
                norm = norm + (a_re * a_re + a_im * a_im)
        sum_re, sum_im, sum_norm = block_sums([margin_re, margin_im, norm])
        sum_norm = sum_norm + EPSILON
        alpha_re = (sum_re / sum_norm)[None]
        alpha_im = (sum_im / sum_norm)[None]
        for spin in range(4):
            for colour in range(3):
                a_re, a_im = acc[RE, spin, colour], acc[IM, spin, colour]
                r_re, r_im = rest[RE, spin, colour], rest[IM, spin, colour]
                corr[RE, spin, colour] += alpha_re * r_re - alpha_im * r_im
                corr[IM, spin, colour] += alpha_re * r_im + alpha_im * r_re
                rest[RE, spin, colour] = r_re - (alpha_re * a_re - alpha_im * a_im)
                rest[IM, spin, colour] = r_im - (alpha_re * a_im + alpha_im * a_re)
        return carry

    lax.fori_loop(0, MR_STEPS, mr_step, 0)

    for mu in (0, 2, 1):
        prepare_ahead(1, corr, mu)
        face_copy(1, mu, 0).start()
        prepare_behind(1, corr, mu, False)
        face_copy(1, mu, 1).start()
    for part in (RE, IM):
        for spin in range(4):
            update_out[part, spin] = x[part, spin] + corr[part, spin]
    zero_acc()
    for a, ahead, behind in x_hops(corr):
        ahead = tuple(jnp.where(high[3], v, 0.0) for v in ahead)
        behind = tuple(jnp.where(coord[3] % BLOCK == 0, v, 0.0) for v in behind)
        add_hops(acc, 3, a, ahead, behind)
    for mu in (1, 2, 0):
        faces_wait(1, mu)
        arrived = unpack(recv_buf.at[6 + mu * 2], mu, BLOCK - 1)
        below = unpack(recv_buf.at[6 + mu * 2 + 1], mu, 0)
        for a in range(3):
            ahead = tuple(jnp.where(high[mu], v, 0.0) for v in link_row(links, mu, a, arrived))
            behind = tuple(jnp.where(coord[mu] == 0, below[part][a], 0.0) for part in (RE, IM))
            add_hops(acc, mu, a, ahead, behind)
    latest_sq = jnp.zeros(site, jnp.float32)
    for part in (RE, IM):
        for spin in range(4):
            for colour in range(3):
                value = rest[part, spin, colour] + 0.5 * acc[part, spin, colour]
                latest_sq = latest_sq + value * value

    stat_send[0:1] = slice_sums(latest_sq)
    stat_copies = [
        pltpu.make_async_remote_copy(
            src_ref=stat_send,
            dst_ref=stat_recv.at[index - 1],
            send_sem=stat_send_sem,
            recv_sem=stat_recv_sem,
            device_id=peer(index),
            device_id_type=pl.DeviceIdType.MESH,
        )
        for index in range(1, group)
    ]
    for copy in stat_copies:
        copy.start()
    pltpu.make_async_copy(send_buf, send_buf, send_sem).wait()
    stats = stat_send[...]
    pltpu.make_async_copy(stat_recv, stat_recv, stat_recv_sem).wait()
    for index in range(1, group):
        stats = stats + stat_recv[index - 1]
    profile_out[...] = stats[0:1] / stats[1:2]
    pltpu.make_async_copy(stat_recv, stat_recv, stat_send_sem).wait()


def finish(held, row, update, profile, sem):
    store = pltpu.make_async_copy(held, update, sem)
    store.start()
    profile[...] = row[0, 0 : profile.shape[0]]
    store.wait()


in_hbm = functools.partial(pltpu.with_memory_space_constraint, memory_space=pltpu.HBM)
in_vmem = functools.partial(pltpu.with_memory_space_constraint, memory_space=pltpu.VMEM)


def solution(mesh):
    sizes = tuple(mesh.shape[axis] for axis in AXES)
    group = mesh.shape["gz"] * mesh.shape["gy"]

    def local(source, start_guess, gauge_links, clover):
        times, depth, flat = source.shape[3:]
        assert times == depth == BLOCK and flat == LANE == BLOCK * LX
        tiles = (times * depth // SUB, SUB, LANE)
        spinor = source.shape[:3] + tiles
        gauge = gauge_links.shape[:4] + tiles
        site = clover.shape[:4] + tiles
        face = (12, 3) + tiles
        f32 = jnp.float32
        update, profile = pl.pallas_call(
            functools.partial(kernel, sizes),
            out_shape=(pltpu.VMEM(spinor, f32), pltpu.VMEM((1, LANE), f32)),
            in_specs=[pl.BlockSpec(memory_space=pltpu.HBM)] * 4,
            out_specs=(pl.BlockSpec(memory_space=pltpu.VMEM),) * 2,
            scratch_shapes=[
                pltpu.VMEM(spinor, f32),
                pltpu.VMEM(spinor, f32),
                pltpu.VMEM(gauge, f32),
                pltpu.VMEM(site, f32),
                pltpu.VMEM(gauge, f32),
                pltpu.VMEM(spinor, f32),
                pltpu.VMEM(spinor, f32),
                pltpu.VMEM(spinor, f32),
                pltpu.VMEM((3, 2, 3, 2) + tiles, f32),
                pltpu.VMEM(face, f32),
                pltpu.VMEM(face, f32),
                pltpu.VMEM((2, LANE), f32),
                pltpu.VMEM((group - 1, 2, LANE), f32),
                pltpu.SemaphoreType.DMA((7,)),
                pltpu.SemaphoreType.DMA,
                pltpu.SemaphoreType.DMA((6,)),
                pltpu.SemaphoreType.DMA,
                pltpu.SemaphoreType.DMA,
            ],
            compiler_params=pltpu.CompilerParams(
                collective_id=0, has_side_effects=True, vmem_limit_bytes=VMEM_LIMIT
            ),
        )(
            in_hbm(start_guess.reshape(spinor)),
            in_hbm(source.reshape(spinor)),
            in_hbm(gauge_links.reshape(gauge)),
            in_hbm(clover.reshape(site)),
        )
        update, profile = pl.pallas_call(
            finish,
            out_shape=(jax.ShapeDtypeStruct(spinor, f32), jax.ShapeDtypeStruct((times,), f32)),
            in_specs=[pl.BlockSpec(memory_space=pltpu.VMEM)] * 2,
            out_specs=(pl.BlockSpec(memory_space=pl.ANY), pl.BlockSpec(memory_space=pltpu.VMEM)),
            scratch_shapes=[pltpu.SemaphoreType.DMA],
        )(
            in_vmem(update),
            in_vmem(profile),
        )
        return update.reshape(source.shape), profile

    spinor_spec = P(None, None, None, "ta", "gz", "gy")
    matrix_spec = P(None, None, None, None, "ta", "gz", "gy")
    return jax.shard_map(
        local,
        mesh=mesh,
        in_specs=(spinor_spec, spinor_spec, matrix_spec, matrix_spec),
        out_specs=(spinor_spec, P("ta")),
        check_vma=False,
    )
```

```python
import functools

import jax
import jax.numpy as jnp
from jax import lax
from jax.experimental import pallas as pl
from jax.experimental.pallas import tpu as pltpu
from jax.sharding import PartitionSpec as P

LX = 32
BLOCK = 4
MR_STEPS = 4
EPSILON = 1e-6
AXES = ("ta", "gz", "gy")
RE, IM = 0, 1
SUB, LANE = 8, 128
VMEM_LIMIT = 24 * 2**20

PAIR = (
    {(0, RE): (1, RE, 0), (0, IM): (1, IM, 0), (1, RE): (1, RE, 1), (1, IM): (1, IM, 1)},
    {(0, RE): (1, IM, 0), (0, IM): (-1, RE, 0), (1, RE): (-1, IM, 1), (1, IM): (1, RE, 1)},
    {(0, RE): (-1, RE, 1), (0, IM): (-1, IM, 1), (1, RE): (1, RE, 0), (1, IM): (1, IM, 0)},
    {(0, RE): (1, IM, 1), (0, IM): (-1, RE, 1), (1, RE): (1, IM, 0), (1, IM): (-1, RE, 0)},
)
PAIR_H = (
    {(0, RE): (1, RE, 0), (0, IM): (1, IM, 0), (1, RE): (1, RE, 1), (1, IM): (1, IM, 1)},
    {(0, RE): (-1, IM, 0), (0, IM): (1, RE, 0), (1, RE): (1, IM, 1), (1, IM): (-1, RE, 1)},
    {(0, RE): (1, RE, 1), (0, IM): (1, IM, 1), (1, RE): (-1, RE, 0), (1, IM): (-1, IM, 0)},
    {(0, RE): (-1, IM, 1), (0, IM): (1, RE, 1), (1, RE): (-1, IM, 0), (1, IM): (1, RE, 0)},
)


PAIRS = {pair: i for i, pair in enumerate((low, high) for high in range(6) for low in range(high))}


def signed_add(base, sign, value):
    return base + value if sign > 0 else base - value


def project(field, mu, s):
    parts = ([], [])
    for part in (RE, IM):
        for colour in range(3):
            spins = []
            for spin in range(2):
                sign, from_part, from_spin = PAIR[mu][(spin, part)]
                spins.append(
                    signed_add(field[part, spin, colour], -s * sign, field[from_part, 2 + from_spin, colour])
                )
            parts[part].append(jnp.stack(spins))
    return parts


def link_row(links, mu, row, half):
    re = im = None
    for col in range(3):
        u_re, u_im = links[mu, RE, row, col][None], links[mu, IM, row, col][None]
        h_re, h_im = half[RE][col], half[IM][col]
        t_re = u_re * h_re - u_im * h_im
        t_im = u_re * h_im + u_im * h_re
        re, im = (t_re, t_im) if re is None else (re + t_re, im + t_im)
    return re, im


def adjoint_row(links, mu, row, half):
    re = im = None
    for col in range(3):
        u_re, u_im = links[mu, RE, col, row][None], links[mu, IM, col, row][None]
        h_re, h_im = half[RE][col], half[IM][col]
        t_re = u_re * h_re + u_im * h_im
        t_im = u_re * h_im - u_im * h_re
        re, im = (t_re, t_im) if re is None else (re + t_re, im + t_im)
    return re, im


def add_hops(acc, mu, colour, ahead, behind):
    difference = tuple(b - a for a, b in zip(ahead, behind))
    for part in (RE, IM):
        acc[part, 0:2, colour] += ahead[part] + behind[part]
        for spin in range(2):
            sign, from_part, from_spin = PAIR_H[mu][(spin, part)]
            old = acc[part, 2 + spin, colour]
            acc[part, 2 + spin, colour] = signed_add(old, sign, difference[from_part][from_spin])


def site_term(clover, field, emit):
    def pair(part, index):
        return jnp.stack([field[part, index // 3, index % 3], field[part, 2 + index // 3, index % 3]])

    vec = [[pair(part, j) for j in range(6)] for part in (RE, IM)]
    for row in range(6):
        diagonal = clover[:, RE, row, row]
        re, im = diagonal * vec[RE][row], diagonal * vec[IM][row]
        for col in range(6):
            if col == row:
                continue
            low, high = min(row, col), max(row, col)
            m_re, m_im = clover[:, RE, low, high], clover[:, IM, low, high]
            if row < col:
                re = re + m_re * vec[RE][col] - m_im * vec[IM][col]
                im = im + m_re * vec[IM][col] + m_im * vec[RE][col]
            else:
                re = re + m_re * vec[RE][col] + m_im * vec[IM][col]
                im = im + m_re * vec[IM][col] - m_im * vec[RE][col]
        for chirality in range(2):
            emit(RE, 2 * chirality + row // 3, row % 3, re[chirality])
            emit(IM, 2 * chirality + row // 3, row % 3, im[chirality])


def three_products(first, second, third, re, im, both):
    def dot(weights, values):
        total = None
        for weight, value in zip(weights, values):
            total = weight * value if total is None else total + weight * value
        return total

    shared = dot(first, both)
    return shared - dot(third, im), shared + dot(second, re)


def block_site_term(clover, twist, tile, field, emit):
    for chirality in range(2):
        vec = [[field(part, 2 * chirality + j // 3, j % 3) for j in range(6)] for part in (RE, IM)]
        both = [r + i for r, i in zip(*vec)]
        for row in range(6):
            diagonal = clover[chirality, RE, row, row, tile]
            re, im, shared = diagonal * vec[RE][row], diagonal * vec[IM][row], None
            for col in range(6):
                if col == row:
                    continue
                low, high = min(row, col), max(row, col)
                term = clover[chirality, RE, low, high, tile] * both[col]
                shared = term if shared is None else shared + term
                less = twist[chirality, PAIRS[low, high], 0, tile]
                more = twist[chirality, PAIRS[low, high], 1, tile]
                if row < col:
                    re, im = re - more * vec[IM][col], im + less * vec[RE][col]
                else:
                    re, im = re + less * vec[IM][col], im - more * vec[RE][col]
            emit(RE, 2 * chirality + row // 3, row % 3, re + shared)
            emit(IM, 2 * chirality + row // 3, row % 3, im + shared)


def swap_halves(value):
    axis = value.ndim - 3
    return jnp.concatenate(
        [lax.slice_in_dim(value, 1, 2, axis=axis), lax.slice_in_dim(value, 0, 1, axis=axis)], axis=axis
    )


def turn(value, shift, axis):
    shift = shift % value.shape[axis]
    return pltpu.roll(value, shift, axis) if shift else value


def cyclic(value, mu, units, early):
    axis = value.ndim - 2
    if mu == 3:
        return turn(value, units, axis + 1)
    if mu == 2:
        return turn(value, units * LX, axis + 1)
    if mu == 1:
        return turn(value, units, axis)
    units = units % BLOCK
    if units == 0:
        return value
    if units == 2:
        return swap_halves(value)
    rolled = turn(value, BLOCK, axis)
    swapped = swap_halves(rolled)
    return jnp.where(early, swapped, rolled) if units == 1 else jnp.where(early, rolled, swapped)


def kernel(
    sizes, x_in, source_in, links_in, clover_in, update_out, profile_out,
    x, source, links, clover, inner, twist, rest, corr, acc, twice, alpha, halves, behind_store,
    send_buf, recv_buf, stat_send, stat_recv,
    in_sem, send_sem, recv_sem, stat_send_sem, stat_recv_sem,
):
    count = {axis: size for axis, size in zip(AXES, sizes)}
    group = count["gz"] * count["gy"]
    me = {axis: lax.axis_index(axis) for axis in AXES}

    def peer(index):
        return {
            "gz": lax.rem(me["gz"] + index // count["gy"], count["gz"]),
            "gy": lax.rem(me["gy"] + index % count["gy"], count["gy"]),
        }

    def beside(axis, step):
        return {axis: lax.rem(me[axis] + step + count[axis], count[axis])}

    barrier = pltpu.get_barrier_semaphore()
    for step in (1, -1):
        pl.semaphore_signal(barrier, inc=1, device_id=beside("ta", step), device_id_type=pl.DeviceIdType.MESH)
    loads = [pltpu.make_async_copy(x_in, x, in_sem.at[0])]
    loads += [pltpu.make_async_copy(links_in.at[mu], links.at[mu], in_sem.at[1 + mu]) for mu in range(4)]
    loads.append(pltpu.make_async_copy(clover_in, clover, in_sem.at[5]))
    loads.append(pltpu.make_async_copy(source_in, source, in_sem.at[6]))
    for load in loads:
        load.start()

    for index in range(1, group):
        pl.semaphore_signal(barrier, inc=1, device_id=peer(index), device_id_type=pl.DeviceIdType.MESH)

    site = (2, SUB, LANE)
    row = lax.broadcasted_iota(jnp.int32, site, 1)
    lane = lax.broadcasted_iota(jnp.int32, site, 2)
    coord = (
        lax.broadcasted_iota(jnp.int32, site, 0) * 2 + row // BLOCK,
        row % BLOCK,
        lane // LX,
        lane % LX,
    )
    early = row < BLOCK
    high = tuple(c % BLOCK == BLOCK - 1 for c in coord)

    def x_neighbour(value, step):
        axis = value.ndim - 1
        if step > 0:
            return jnp.where(coord[3] == LX - 1, turn(value, LX - 1, axis), turn(value, -1, axis))
        return jnp.where(coord[3] == 0, turn(value, 1 - LX, axis), turn(value, 1, axis))

    def flat(half):
        return [half[part][colour][spin] for part in (RE, IM) for spin in range(2) for colour in range(3)]

    def pack(half, mu, edge, store, factor=None):
        values = flat(half)
        for j in range(3):
            packed = cyclic(values[4 * j], mu, -edge, early)
            for k in range(1, BLOCK):
                packed = jnp.where(coord[mu] == k, cyclic(values[4 * j + k], mu, k - edge, early), packed)
            store[j] = packed if factor is None else packed * factor

    def unpack(store, mu, edge):
        values = []
        for j in range(3):
            packed = store[j]
            values += [cyclic(packed, mu, edge - k, early) for k in range(BLOCK)]
        return [[jnp.stack([values[6 * p + c], values[6 * p + 3 + c]]) for c in range(3)] for p in (RE, IM)]

    def face_copy(turn_index, mu, side):
        slot = turn_index * 6 + mu * 2 + side
        return pltpu.make_async_remote_copy(
            src_ref=send_buf.at[slot],
            dst_ref=recv_buf.at[slot],
            send_sem=send_sem,
            recv_sem=recv_sem.at[turn_index * 3 + mu],
            device_id=beside(AXES[mu], -1 if side == 0 else 1),
            device_id_type=pl.DeviceIdType.MESH,
        )

    def faces_wait(turn_index, mu):
        pair = recv_buf.at[pl.ds(turn_index * 6 + mu * 2, 2)]
        pltpu.make_async_copy(pair, pair, recv_sem.at[turn_index * 3 + mu]).wait()

    def start_wrapped_first(turn_index):
        last = me["ta"] == count["ta"] - 1

        @pl.when(last)
        def _():
            face_copy(turn_index, 0, 1).start()
            face_copy(turn_index, 0, 0).start()

        @pl.when(jnp.logical_not(last))
        def _():
            face_copy(turn_index, 0, 0).start()
            face_copy(turn_index, 0, 1).start()

    first_t = jnp.where(me["ta"] == 0, -1.0, 1.0).astype(jnp.float32)
    last_t = jnp.where(me["ta"] == count["ta"] - 1, -1.0, 1.0).astype(jnp.float32)

    def prepare_ahead(turn_index, field, mu):
        pack(project(field, mu, 1), mu, 0, send_buf.at[turn_index * 6 + mu * 2], first_t if mu == 0 else None)

    def prepare_behind(turn_index, field, mu, keep):
        half = project(field, mu, -1)
        rows = [adjoint_row(links, mu, a, half) for a in range(3)]
        behind = [[rows[a][part] for a in range(3)] for part in (RE, IM)]
        pack(behind, mu, BLOCK - 1, send_buf.at[turn_index * 6 + mu * 2 + 1], last_t if mu == 0 else None)
        if keep:
            for part in (RE, IM):
                for a in range(3):
                    behind_store[mu, part, a] = behind[part][a]

    loads[0].wait()
    prepare_ahead(0, x, 0)
    loads[1].wait()
    prepare_behind(0, x, 0, True)
    prepare_ahead(0, x, 2)
    pl.semaphore_wait(barrier, group - 1 + 2)
    start_wrapped_first(0)
    face_copy(0, 2, 0).start()
    loads[3].wait()
    prepare_behind(0, x, 2, True)
    face_copy(0, 2, 1).start()
    prepare_ahead(0, x, 1)
    face_copy(0, 1, 0).start()
    loads[2].wait()
    prepare_behind(0, x, 1, True)
    face_copy(0, 1, 1).start()

    def zero_acc():
        acc[...] = jnp.zeros_like(acc)

    zero_acc()
    loads[4].wait()

    def x_hops(field):
        ahead_half = [[x_neighbour(v, 1) for v in values] for values in project(field, 3, 1)]
        behind_half = project(field, 3, -1)
        for a in range(3):
            ahead = link_row(links, 3, a, ahead_half)
            behind = tuple(x_neighbour(v, -1) for v in adjoint_row(links, 3, a, behind_half))
            yield a, ahead, behind

    for a, ahead, behind in x_hops(x):
        add_hops(acc, 3, a, ahead, behind)

    for mu in range(4):
        factor = jnp.where(high[mu], 0.0, -0.5).astype(jnp.float32)
        for a in range(3):
            for b in range(3):
                re, im = links[mu, RE, a, b] * factor, links[mu, IM, a, b] * factor
                inner[0, mu, 0, a, b] = re
                inner[0, mu, 1, a, b] = im - re
                inner[0, mu, 2, a, b] = im + re
                re, im = cyclic(re, mu, 1, early), cyclic(im, mu, 1, early)
                inner[1, mu, 0, b, a] = re
                inner[1, mu, 1, b, a] = -im - re
                inner[1, mu, 2, b, a] = re - im

    loads[5].wait()
    for chirality in range(2):
        for (low, high_row), index in PAIRS.items():
            re, im = clover[chirality, RE, low, high_row], clover[chirality, IM, low, high_row]
            twist[chirality, index, 0] = im - re
            twist[chirality, index, 1] = im + re
    loads[6].wait()

    def emit_rest(part, spin, colour, value):
        rest[part, spin, colour] = source[part, spin, colour] - value

    site_term(clover, x, emit_rest)
    source_sq = jnp.zeros(site, jnp.float32)
    for part in (RE, IM):
        for spin in range(4):
            for colour in range(3):
                value = source[part, spin, colour]
                source_sq = source_sq + value * value

    def slice_sums(value):
        sums = jnp.broadcast_to(jnp.sum(value, axis=2, keepdims=True), site)
        picked = jnp.where(coord[0] == lane, sums, 0.0)
        return jnp.sum(picked[0] + picked[1], axis=0, keepdims=True)

    stat_send[1:2] = slice_sums(source_sq)

    for mu in (1, 2, 0):
        faces_wait(0, mu)
        arrived = unpack(recv_buf.at[mu * 2], mu, BLOCK - 1)
        local = project(x, mu, 1)
        ahead_half = [
            [
                jnp.where(coord[mu] == BLOCK - 1, arrived[part][c], cyclic(local[part][c], mu, -1, early))
                for c in range(3)
            ]
            for part in (RE, IM)
        ]
        below = unpack(recv_buf.at[mu * 2 + 1], mu, 0)
        for a in range(3):
            ahead = link_row(links, mu, a, ahead_half)
            behind = tuple(
                jnp.where(coord[mu] == 0, below[part][a], cyclic(behind_store[mu, part, a], mu, 1, early))
                for part in (RE, IM)
            )
            add_hops(acc, mu, a, ahead, behind)

    for part in (RE, IM):
        for spin in range(4):
            rest[part, spin] += 0.5 * acc[part, spin]
            corr[part, spin] = jnp.zeros_like(corr[part, spin])

    row8 = lax.broadcasted_iota(jnp.int32, (SUB, LANE), 0)
    lane8 = lax.broadcasted_iota(jnp.int32, (SUB, LANE), 1)

    def block_sums(values):
        packed = None
        for index, value in enumerate(values):
            total = jnp.sum(value, axis=0, keepdims=True)
            total = jnp.broadcast_to(total, (SUB, LANE))
            packed = total if packed is None else jnp.where(row8 == index, total, packed)
        place = lane8 % BLOCK
        total = None
        for offset in range(1 - BLOCK, BLOCK):
            moved = [turn(packed, start - offset, 1) for start in range(0, LANE, LX)]
            while len(moved) > 1:
                moved = [p + q for p, q in zip(moved[::2], moved[1::2])]
            part = moved[0]
            if offset:
                part = jnp.where((place + offset >= 0) & (place + offset < BLOCK), part, 0.0)
            total = part if total is None else total + part
        packed = total
        return [jnp.broadcast_to(packed[i : i + 1], (SUB, LANE)) for i in range(len(values))]

    def store_halves(origin):
        for mu in (3, 2, 1, 0):
            for index, s in enumerate((1, -1)):
                half = project(origin, mu, s)
                for part in (RE, IM):
                    for colour in range(3):
                        moved = cyclic(half[part][colour], mu, -s, early)
                        for spin in range(2):
                            halves[index, mu, part, spin, colour] = moved[spin]

    def site_apply(origin, target):
        for tile in range(2):
            def emit(part, spin, colour, value):
                target[part, spin, colour, tile] = value

            block_site_term(clover, twist, tile, lambda p, s, c: origin[p, s, c, tile], emit)

    def add_inner_hops(target):
        def hop_row(tile, row, carry):
            total = {(part, spin): target[part, spin, row, tile] for part in (RE, IM) for spin in range(4)}
            for mu in range(4):
                for index in range(2):
                    weights = [[inner[index, mu, form, row, col, tile] for col in range(3)] for form in range(3)]
                    got = []
                    for spin in range(2):
                        re, im = ([halves[index, mu, part, spin, c, tile] for c in range(3)] for part in (RE, IM))
                        both = [r + i for r, i in zip(re, im)]
                        got.append(three_products(*weights, re, im, both))
                    for part in (RE, IM):
                        for spin in range(2):
                            total[part, spin] = total[part, spin] + got[spin][part]
                            sign, from_part, from_spin = PAIR_H[mu][(spin, part)]
                            total[part, 2 + spin] = signed_add(
                                total[part, 2 + spin], sign if index else -sign, got[from_spin][from_part]
                            )
            for (part, spin), value in total.items():
                target[part, spin, row, tile] = value
            return carry

        for tile in range(2):
            for row in range(3):
                hop_row(tile, row, 0)

    def times_alpha(field, spin, colour, tile):
        re, im = field[RE, spin, colour, tile], field[IM, spin, colour, tile]
        a_re, a_im = alpha[0], alpha[1]
        return a_re * re - a_im * im, a_re * im + a_im * re

    def subtract_scaled(target, scaled, spin, colour, tile):
        for part in (RE, IM):
            target[part, spin, colour, tile] -= scaled[part]

    def next_margins():
        zero = jnp.zeros((SUB, LANE), jnp.float32)

        def one_tile(tile, carry):
            margin_re, margin_im, norm = carry
            for spin in range(4):
                for colour in range(3):
                    a_re, a_im = acc[RE, spin, colour, tile], acc[IM, spin, colour, tile]
                    r_re, r_im = rest[RE, spin, colour, tile], rest[IM, spin, colour, tile]
                    margin_re = margin_re + (a_re * r_re + a_im * r_im)
                    margin_im = margin_im + (a_re * r_im - a_im * r_re)
                    norm = norm + (a_re * a_re + a_im * a_im)
            return margin_re, margin_im, norm

        return lax.fori_loop(0, 2, one_tile, (zero, zero, zero))

    def set_alpha(margins):
        sum_re, sum_im, sum_norm = block_sums(margins)
        sum_norm = sum_norm + EPSILON
        alpha[0] = sum_re / sum_norm
        alpha[1] = sum_im / sum_norm

    def advance(tile):
        for spin in range(4):
            for colour in range(3):
                scaled = times_alpha(rest, spin, colour, tile)
                for part in (RE, IM):
                    corr[part, spin, colour, tile] += scaled[part]
                subtract_scaled(rest, times_alpha(acc, spin, colour, tile), spin, colour, tile)

    def full_step(_, margins):
        set_alpha(margins)
        store_halves(acc)
        site_apply(acc, twice)
        add_inner_hops(twice)
        zero = jnp.zeros((SUB, LANE), jnp.float32)

        def one_tile(tile, carry):
            margin_re, margin_im, norm = carry
            advance(tile)
            for spin in range(4):
                for colour in range(3):
                    subtract_scaled(acc, times_alpha(twice, spin, colour, tile), spin, colour, tile)
                    a_re, a_im = acc[RE, spin, colour, tile], acc[IM, spin, colour, tile]
                    r_re, r_im = rest[RE, spin, colour, tile], rest[IM, spin, colour, tile]
                    margin_re = margin_re + (a_re * r_re + a_im * r_im)
                    margin_im = margin_im + (a_re * r_im - a_im * r_re)
                    norm = norm + (a_re * a_re + a_im * a_im)
            return margin_re, margin_im, norm

        return lax.fori_loop(0, 2, one_tile, (zero, zero, zero))

    store_halves(rest)
    site_apply(rest, acc)
    add_inner_hops(acc)
    margins = lax.fori_loop(0, MR_STEPS - 1, full_step, next_margins())
    set_alpha(margins)
    for tile in range(2):
        advance(tile)

    for mu in (0, 2, 1):
        prepare_ahead(1, corr, mu)
        face_copy(1, mu, 0).start()
        prepare_behind(1, corr, mu, False)
        face_copy(1, mu, 1).start()
    for part in (RE, IM):
        for spin in range(4):
            update_out[part, spin] = x[part, spin] + corr[part, spin]
    zero_acc()
    for a, ahead, behind in x_hops(corr):
        ahead = tuple(jnp.where(high[3], v, 0.0) for v in ahead)
        behind = tuple(jnp.where(coord[3] % BLOCK == 0, v, 0.0) for v in behind)
        add_hops(acc, 3, a, ahead, behind)
    for mu in (1, 2, 0):
        faces_wait(1, mu)
        arrived = unpack(recv_buf.at[6 + mu * 2], mu, BLOCK - 1)
        below = unpack(recv_buf.at[6 + mu * 2 + 1], mu, 0)
        for a in range(3):
            ahead = tuple(jnp.where(high[mu], v, 0.0) for v in link_row(links, mu, a, arrived))
            behind = tuple(jnp.where(coord[mu] == 0, below[part][a], 0.0) for part in (RE, IM))
            add_hops(acc, mu, a, ahead, behind)
    latest_sq = jnp.zeros(site, jnp.float32)
    for part in (RE, IM):
        for spin in range(4):
            for colour in range(3):
                value = rest[part, spin, colour] + 0.5 * acc[part, spin, colour]
                latest_sq = latest_sq + value * value

    stat_send[0:1] = slice_sums(latest_sq)
    stat_copies = [
        pltpu.make_async_remote_copy(
            src_ref=stat_send,
            dst_ref=stat_recv.at[index - 1],
            send_sem=stat_send_sem,
            recv_sem=stat_recv_sem,
            device_id=peer(index),
            device_id_type=pl.DeviceIdType.MESH,
        )
        for index in range(1, group)
    ]
    for copy in stat_copies:
        copy.start()
    pltpu.make_async_copy(send_buf, send_buf, send_sem).wait()
    stats = stat_send[...]
    pltpu.make_async_copy(stat_recv, stat_recv, stat_recv_sem).wait()
    for index in range(1, group):
        stats = stats + stat_recv[index - 1]
    profile_out[...] = (stats[0:1] / stats[1:2])[0, 0 : profile_out.shape[0]]
    pltpu.make_async_copy(stat_recv, stat_recv, stat_send_sem).wait()


def finish(held, ratio, update, profile, sems):
    stores = [pltpu.make_async_copy(held, update, sems.at[0]), pltpu.make_async_copy(ratio, profile, sems.at[1])]
    for store in stores:
        store.start()
    for store in stores:
        store.wait()


in_hbm = functools.partial(pltpu.with_memory_space_constraint, memory_space=pltpu.HBM)
in_vmem = functools.partial(pltpu.with_memory_space_constraint, memory_space=pltpu.VMEM)


def solution(mesh):
    sizes = tuple(mesh.shape[axis] for axis in AXES)
    group = mesh.shape["gz"] * mesh.shape["gy"]

    def local(source, start_guess, gauge_links, clover):
        times, depth, flat = source.shape[3:]
        assert times == depth == BLOCK and flat == LANE == BLOCK * LX
        tiles = (times * depth // SUB, SUB, LANE)
        spinor = source.shape[:3] + tiles
        gauge = gauge_links.shape[:4] + tiles
        site = clover.shape[:4] + tiles
        face = (12, 3) + tiles
        f32 = jnp.float32
        update, profile = pl.pallas_call(
            functools.partial(kernel, sizes),
            out_shape=(pltpu.VMEM(spinor, f32), pltpu.VMEM((times,), f32)),
            in_specs=[pl.BlockSpec(memory_space=pltpu.HBM)] * 4,
            out_specs=(pl.BlockSpec(memory_space=pltpu.VMEM),) * 2,
            scratch_shapes=[
                pltpu.VMEM(spinor, f32),
                pltpu.VMEM(spinor, f32),
                pltpu.VMEM(gauge, f32),
                pltpu.VMEM(site, f32),
                pltpu.VMEM((2, 4, 3, 3, 3) + tiles, f32),
                pltpu.VMEM((2, len(PAIRS), 2) + tiles, f32),
                pltpu.VMEM(spinor, f32),
                pltpu.VMEM(spinor, f32),
                pltpu.VMEM(spinor, f32),
                pltpu.VMEM(spinor, f32),
                pltpu.VMEM((2, SUB, LANE), f32),
                pltpu.VMEM((2, 4, 2, 2, 3) + tiles, f32),
                pltpu.VMEM((3, 2, 3, 2) + tiles, f32),
                pltpu.VMEM(face, f32),
                pltpu.VMEM(face, f32),
                pltpu.VMEM((2, LANE), f32),
                pltpu.VMEM((group - 1, 2, LANE), f32),
                pltpu.SemaphoreType.DMA((7,)),
                pltpu.SemaphoreType.DMA,
                pltpu.SemaphoreType.DMA((6,)),
                pltpu.SemaphoreType.DMA,
                pltpu.SemaphoreType.DMA,
            ],
            compiler_params=pltpu.CompilerParams(
                collective_id=0, has_side_effects=True, vmem_limit_bytes=VMEM_LIMIT,
            ),
        )(
            in_hbm(start_guess.reshape(spinor)),
            in_hbm(source.reshape(spinor)),
            in_hbm(gauge_links.reshape(gauge)),
            in_hbm(clover.reshape(site)),
        )
        update, profile = pl.pallas_call(
            finish,
            out_shape=(jax.ShapeDtypeStruct(spinor, f32), jax.ShapeDtypeStruct((times,), f32)),
            in_specs=[pl.BlockSpec(memory_space=pltpu.VMEM)] * 2,
            out_specs=(pl.BlockSpec(memory_space=pl.ANY),) * 2,
            scratch_shapes=[pltpu.SemaphoreType.DMA((2,))],
        )(
            in_vmem(update),
            in_vmem(profile),
        )
        return update.reshape(source.shape), profile

    spinor_spec = P(None, None, None, "ta", "gz", "gy")
    matrix_spec = P(None, None, None, None, "ta", "gz", "gy")
    return jax.shard_map(
        local,
        mesh=mesh,
        in_specs=(spinor_spec, spinor_spec, matrix_spec, matrix_spec),
        out_specs=(spinor_spec, P("ta")),
        check_vma=False,
    )
```

```python
import functools

import jax
import jax.numpy as jnp
from jax import lax
from jax.experimental import pallas as pl
from jax.experimental.pallas import tpu as pltpu
from jax.sharding import PartitionSpec as P

LX = 32
BLOCK = 4
MR_STEPS = 4
EPSILON = 1e-6
AXES = ("ta", "gz", "gy")
RE, IM = 0, 1
SUB, LANE = 8, 128
VMEM_LIMIT = 24 * 2**20

PAIR = (
    {(0, RE): (1, RE, 0), (0, IM): (1, IM, 0), (1, RE): (1, RE, 1), (1, IM): (1, IM, 1)},
    {(0, RE): (1, IM, 0), (0, IM): (-1, RE, 0), (1, RE): (-1, IM, 1), (1, IM): (1, RE, 1)},
    {(0, RE): (-1, RE, 1), (0, IM): (-1, IM, 1), (1, RE): (1, RE, 0), (1, IM): (1, IM, 0)},
    {(0, RE): (1, IM, 1), (0, IM): (-1, RE, 1), (1, RE): (1, IM, 0), (1, IM): (-1, RE, 0)},
)
PAIR_H = (
    {(0, RE): (1, RE, 0), (0, IM): (1, IM, 0), (1, RE): (1, RE, 1), (1, IM): (1, IM, 1)},
    {(0, RE): (-1, IM, 0), (0, IM): (1, RE, 0), (1, RE): (1, IM, 1), (1, IM): (-1, RE, 1)},
    {(0, RE): (1, RE, 1), (0, IM): (1, IM, 1), (1, RE): (-1, RE, 0), (1, IM): (-1, IM, 0)},
    {(0, RE): (-1, IM, 1), (0, IM): (1, RE, 1), (1, RE): (-1, IM, 0), (1, IM): (1, RE, 0)},
)


PAIRS = {pair: i for i, pair in enumerate((low, high) for high in range(6) for low in range(high))}


def signed_add(base, sign, value):
    return base + value if sign > 0 else base - value


def project(field, mu, s):
    parts = ([], [])
    for part in (RE, IM):
        for colour in range(3):
            spins = []
            for spin in range(2):
                sign, from_part, from_spin = PAIR[mu][(spin, part)]
                spins.append(
                    signed_add(field[part, spin, colour], -s * sign, field[from_part, 2 + from_spin, colour])
                )
            parts[part].append(jnp.stack(spins))
    return parts


def link_row(links, mu, row, half):
    re = im = None
    for col in range(3):
        u_re, u_im = links[mu, RE, row, col][None], links[mu, IM, row, col][None]
        h_re, h_im = half[RE][col], half[IM][col]
        t_re = u_re * h_re - u_im * h_im
        t_im = u_re * h_im + u_im * h_re
        re, im = (t_re, t_im) if re is None else (re + t_re, im + t_im)
    return re, im


def adjoint_row(links, mu, row, half):
    re = im = None
    for col in range(3):
        u_re, u_im = links[mu, RE, col, row][None], links[mu, IM, col, row][None]
        h_re, h_im = half[RE][col], half[IM][col]
        t_re = u_re * h_re + u_im * h_im
        t_im = u_re * h_im - u_im * h_re
        re, im = (t_re, t_im) if re is None else (re + t_re, im + t_im)
    return re, im


def add_hops(acc, mu, colour, ahead, behind):
    difference = tuple(b - a for a, b in zip(ahead, behind))
    for part in (RE, IM):
        acc[part, 0:2, colour] += ahead[part] + behind[part]
        for spin in range(2):
            sign, from_part, from_spin = PAIR_H[mu][(spin, part)]
            old = acc[part, 2 + spin, colour]
            acc[part, 2 + spin, colour] = signed_add(old, sign, difference[from_part][from_spin])


def site_term(clover, field, emit):
    def pair(part, index):
        return jnp.stack([field[part, index // 3, index % 3], field[part, 2 + index // 3, index % 3]])

    vec = [[pair(part, j) for j in range(6)] for part in (RE, IM)]
    for row in range(6):
        diagonal = clover[:, RE, row, row]
        re, im = diagonal * vec[RE][row], diagonal * vec[IM][row]
        for col in range(6):
            if col == row:
                continue
            low, high = min(row, col), max(row, col)
            m_re, m_im = clover[:, RE, low, high], clover[:, IM, low, high]
            if row < col:
                re = re + m_re * vec[RE][col] - m_im * vec[IM][col]
                im = im + m_re * vec[IM][col] + m_im * vec[RE][col]
            else:
                re = re + m_re * vec[RE][col] + m_im * vec[IM][col]
                im = im + m_re * vec[IM][col] - m_im * vec[RE][col]
        for chirality in range(2):
            emit(RE, 2 * chirality + row // 3, row % 3, re[chirality])
            emit(IM, 2 * chirality + row // 3, row % 3, im[chirality])


def three_products(first, second, third, re, im, both):
    def dot(weights, values):
        total = None
        for weight, value in zip(weights, values):
            total = weight * value if total is None else total + weight * value
        return total

    shared = dot(first, both)
    return shared - dot(third, im), shared + dot(second, re)


def block_site_term(diagonals, triples, field, emit):
    for chirality in range(2):
        vec = [[field(part, 2 * chirality + j // 3, j % 3) for j in range(6)] for part in (RE, IM)]
        both = [r + i for r, i in zip(*vec)]
        for row in range(6):
            diagonal = diagonals(chirality, row)
            re, im, shared = diagonal * vec[RE][row], diagonal * vec[IM][row], None
            for col in range(6):
                if col == row:
                    continue
                low, high = min(row, col), max(row, col)
                real, less, more = triples(chirality, low, high)
                term = real * both[col]
                shared = term if shared is None else shared + term
                if row < col:
                    re, im = re - more * vec[IM][col], im + less * vec[RE][col]
                else:
                    re, im = re + less * vec[IM][col], im - more * vec[RE][col]
            emit(RE, 2 * chirality + row // 3, row % 3, re + shared)
            emit(IM, 2 * chirality + row // 3, row % 3, im + shared)


def swap_halves(value):
    axis = value.ndim - 3
    return jnp.concatenate(
        [lax.slice_in_dim(value, 1, 2, axis=axis), lax.slice_in_dim(value, 0, 1, axis=axis)], axis=axis
    )


def turn(value, shift, axis):
    shift = shift % value.shape[axis]
    return pltpu.roll(value, shift, axis) if shift else value


def cyclic(value, mu, units, early):
    axis = value.ndim - 2
    if mu == 3:
        return turn(value, units, axis + 1)
    if mu == 2:
        return turn(value, units * LX, axis + 1)
    if mu == 1:
        return turn(value, units, axis)
    units = units % BLOCK
    if units == 0:
        return value
    if units == 2:
        return swap_halves(value)
    rolled = turn(value, BLOCK, axis)
    swapped = swap_halves(rolled)
    return jnp.where(early, swapped, rolled) if units == 1 else jnp.where(early, rolled, swapped)


def kernel(
    sizes, x_in, source_in, links_in, clover_in, update_out, profile_out,
    x, source, links, clover, inner, twist, rest, corr, acc, twice, alpha, halves, edge, edge_out, edge_halves,
    edge_inner, edge_time, edge_diagonal, edge_pair, behind_store,
    send_buf, recv_buf, stat_send, stat_recv,
    in_sem, send_sem, recv_sem, stat_send_sem, stat_recv_sem,
):
    count = {axis: size for axis, size in zip(AXES, sizes)}
    group = count["gz"] * count["gy"]
    me = {axis: lax.axis_index(axis) for axis in AXES}

    def peer(index):
        return {
            "gz": lax.rem(me["gz"] + index // count["gy"], count["gz"]),
            "gy": lax.rem(me["gy"] + index % count["gy"], count["gy"]),
        }

    def spread(index):
        depth = index // count["gy"]
        return 2 * min(depth, count["gz"] - depth) + 3 * (index % count["gy"] != 0)

    def beside(axis, step):
        return {axis: lax.rem(me[axis] + step + count[axis], count[axis])}

    barrier = pltpu.get_barrier_semaphore()
    for step in (1, -1):
        pl.semaphore_signal(barrier, inc=1, device_id=beside("ta", step), device_id_type=pl.DeviceIdType.MESH)
    loads = [pltpu.make_async_copy(x_in, x, in_sem.at[0])]
    loads += [pltpu.make_async_copy(links_in.at[mu], links.at[mu], in_sem.at[1 + mu]) for mu in range(4)]
    loads.append(pltpu.make_async_copy(clover_in, clover, in_sem.at[5]))
    loads.append(pltpu.make_async_copy(source_in, source, in_sem.at[6]))
    for load in loads:
        load.start()

    for index in range(1, group):
        pl.semaphore_signal(barrier, inc=1, device_id=peer(index), device_id_type=pl.DeviceIdType.MESH)

    site = (2, SUB, LANE)
    row = lax.broadcasted_iota(jnp.int32, site, 1)
    lane = lax.broadcasted_iota(jnp.int32, site, 2)
    coord = (
        lax.broadcasted_iota(jnp.int32, site, 0) * 2 + row // BLOCK,
        row % BLOCK,
        lane // LX,
        lane % LX,
    )
    early = row < BLOCK
    row8 = lax.broadcasted_iota(jnp.int32, (SUB, LANE), 0)
    lane8 = lax.broadcasted_iota(jnp.int32, (SUB, LANE), 1)
    early8 = row8 < BLOCK
    high = tuple(c % BLOCK == BLOCK - 1 for c in coord)

    def x_neighbour(value, step):
        axis = value.ndim - 1
        if step > 0:
            return jnp.where(coord[3] == LX - 1, turn(value, LX - 1, axis), turn(value, -1, axis))
        return jnp.where(coord[3] == 0, turn(value, 1 - LX, axis), turn(value, 1, axis))

    def flat(half):
        return [half[part][colour][spin] for part in (RE, IM) for spin in range(2) for colour in range(3)]

    def pack(half, mu, edge, store, factor=None):
        values = flat(half)
        for j in range(3):
            packed = cyclic(values[4 * j], mu, -edge, early)
            for k in range(1, BLOCK):
                packed = jnp.where(coord[mu] == k, cyclic(values[4 * j + k], mu, k - edge, early), packed)
            store[j] = packed if factor is None else packed * factor

    def unpack(store, mu, edge):
        values = []
        for j in range(3):
            packed = store[j]
            values += [cyclic(packed, mu, edge - k, early) for k in range(BLOCK)]
        return [[jnp.stack([values[6 * p + c], values[6 * p + 3 + c]]) for c in range(3)] for p in (RE, IM)]

    def face_copy(turn_index, mu, side):
        slot = turn_index * 6 + mu * 2 + side
        return pltpu.make_async_remote_copy(
            src_ref=send_buf.at[slot],
            dst_ref=recv_buf.at[slot],
            send_sem=send_sem,
            recv_sem=recv_sem.at[turn_index * 3 + mu],
            device_id=beside(AXES[mu], -1 if side == 0 else 1),
            device_id_type=pl.DeviceIdType.MESH,
        )

    def faces_wait(turn_index, mu):
        pair = recv_buf.at[pl.ds(turn_index * 6 + mu * 2, 2)]
        pltpu.make_async_copy(pair, pair, recv_sem.at[turn_index * 3 + mu]).wait()

    def start_wrapped_first(turn_index):
        last = me["ta"] == count["ta"] - 1

        @pl.when(last)
        def _():
            face_copy(turn_index, 0, 1).start()
            face_copy(turn_index, 0, 0).start()

        @pl.when(jnp.logical_not(last))
        def _():
            face_copy(turn_index, 0, 0).start()
            face_copy(turn_index, 0, 1).start()

    first_t = jnp.where(me["ta"] == 0, -1.0, 1.0).astype(jnp.float32)
    last_t = jnp.where(me["ta"] == count["ta"] - 1, -1.0, 1.0).astype(jnp.float32)

    def prepare_ahead(turn_index, field, mu):
        pack(project(field, mu, 1), mu, 0, send_buf.at[turn_index * 6 + mu * 2], first_t if mu == 0 else None)

    def prepare_behind(turn_index, field, mu, keep):
        half = project(field, mu, -1)
        rows = [adjoint_row(links, mu, a, half) for a in range(3)]
        behind = [[rows[a][part] for a in range(3)] for part in (RE, IM)]
        pack(behind, mu, BLOCK - 1, send_buf.at[turn_index * 6 + mu * 2 + 1], last_t if mu == 0 else None)
        if keep:
            for part in (RE, IM):
                for a in range(3):
                    behind_store[mu, part, a] = behind[part][a]

    loads[0].wait()
    prepare_ahead(0, x, 0)
    loads[1].wait()
    prepare_behind(0, x, 0, True)
    prepare_ahead(0, x, 2)
    pl.semaphore_wait(barrier, group - 1 + 2)
    start_wrapped_first(0)
    face_copy(0, 2, 0).start()
    loads[3].wait()
    prepare_behind(0, x, 2, True)
    face_copy(0, 2, 1).start()
    prepare_ahead(0, x, 1)
    face_copy(0, 1, 0).start()
    loads[2].wait()
    prepare_behind(0, x, 1, True)
    face_copy(0, 1, 1).start()

    def zero_acc():
        acc[...] = jnp.zeros_like(acc)

    zero_acc()
    loads[4].wait()

    def x_hops(field):
        ahead_half = [[x_neighbour(v, 1) for v in values] for values in project(field, 3, 1)]
        behind_half = project(field, 3, -1)
        for a in range(3):
            ahead = link_row(links, 3, a, ahead_half)
            behind = tuple(x_neighbour(v, -1) for v in adjoint_row(links, 3, a, behind_half))
            yield a, ahead, behind

    for a, ahead, behind in x_hops(x):
        add_hops(acc, 3, a, ahead, behind)

    for mu in range(4):
        factor = jnp.where(high[mu], 0.0, -0.5).astype(jnp.float32)
        for a in range(3):
            for b in range(3):
                re, im = links[mu, RE, a, b] * factor, links[mu, IM, a, b] * factor
                inner[0, mu, 0, a, b] = re
                inner[0, mu, 1, a, b] = im - re
                inner[0, mu, 2, a, b] = im + re
                re, im = cyclic(re, mu, 1, early), cyclic(im, mu, 1, early)
                inner[1, mu, 0, b, a] = re
                inner[1, mu, 1, b, a] = -im - re
                inner[1, mu, 2, b, a] = re - im

    loads[5].wait()
    for chirality in range(2):
        for (low, high_row), index in PAIRS.items():
            re, im = clover[chirality, RE, low, high_row], clover[chirality, IM, low, high_row]
            twist[chirality, index, 0] = im - re
            twist[chirality, index, 1] = im + re
    def outer(first, second):
        return jnp.where(early8, first, second)

    for index in range(2):
        for mu in range(1, 4):
            for form in range(3):
                for a in range(3):
                    for b in range(3):
                        edge_inner[index, mu - 1, form, a, b] = outer(*(inner[index, mu, form, a, b, i] for i in range(2)))
    for form in range(3):
        for a in range(3):
            for b in range(3):
                edge_time[form, a, b] = outer(inner[0, 0, form, a, b, 1], inner[1, 0, form, a, b, 0])
    for chirality in range(2):
        for a in range(6):
            edge_diagonal[chirality, a] = outer(*(clover[chirality, RE, a, a, i] for i in range(2)))
        for (low, high_row), index in PAIRS.items():
            edge_pair[chirality, index, 0] = outer(*(clover[chirality, RE, low, high_row, i] for i in range(2)))
            for form in range(2):
                edge_pair[chirality, index, 1 + form] = outer(*(twist[chirality, index, form, i] for i in range(2)))
    loads[6].wait()

    def emit_rest(part, spin, colour, value):
        rest[part, spin, colour] = source[part, spin, colour] - value

    site_term(clover, x, emit_rest)
    source_sq = jnp.zeros(site, jnp.float32)
    for part in (RE, IM):
        for spin in range(4):
            for colour in range(3):
                value = source[part, spin, colour]
                source_sq = source_sq + value * value

    def slice_sums(value, time):
        sums = jnp.broadcast_to(jnp.sum(value, axis=1, keepdims=True), (SUB, LANE))
        return jnp.sum(jnp.where(time == lane8, sums, 0.0), axis=0, keepdims=True)

    stat_send[1:2] = slice_sums(source_sq[0], coord[0][0]) + slice_sums(source_sq[1], coord[0][1])

    local = project(x, 0, 1)
    ahead_half = [
        [jnp.where(coord[0] == BLOCK - 1, 0.0, cyclic(local[part][c], 0, -1, early)) for c in range(3)]
        for part in (RE, IM)
    ]
    for a in range(3):
        ahead = link_row(links, 0, a, ahead_half)
        behind = tuple(
            jnp.where(coord[0] == 0, 0.0, cyclic(behind_store[0, part, a], 0, 1, early)) for part in (RE, IM)
        )
        add_hops(acc, 0, a, ahead, behind)

    for mu in (1, 2):
        faces_wait(0, mu)
        arrived = unpack(recv_buf.at[mu * 2], mu, BLOCK - 1)
        local = project(x, mu, 1)
        ahead_half = [
            [
                jnp.where(coord[mu] == BLOCK - 1, arrived[part][c], cyclic(local[part][c], mu, -1, early))
                for c in range(3)
            ]
            for part in (RE, IM)
        ]
        below = unpack(recv_buf.at[mu * 2 + 1], mu, 0)
        for a in range(3):
            ahead = link_row(links, mu, a, ahead_half)
            behind = tuple(
                jnp.where(coord[mu] == 0, below[part][a], cyclic(behind_store[mu, part, a], mu, 1, early))
                for part in (RE, IM)
            )
            add_hops(acc, mu, a, ahead, behind)

    for part in (RE, IM):
        for spin in range(4):
            rest[part, spin] += 0.5 * acc[part, spin]
            corr[part, spin] = jnp.zeros_like(corr[part, spin])

    def block_sums(values):
        packed = None
        for index, value in enumerate(values):
            total = jnp.sum(value, axis=0, keepdims=True)
            total = jnp.broadcast_to(total, (SUB, LANE))
            packed = total if packed is None else jnp.where(row8 == index, total, packed)
        place = lane8 % BLOCK
        total = None
        for offset in range(1 - BLOCK, BLOCK):
            moved = [turn(packed, start - offset, 1) for start in range(0, LANE, LX)]
            while len(moved) > 1:
                moved = [p + q for p, q in zip(moved[::2], moved[1::2])]
            part = moved[0]
            if offset:
                part = jnp.where((place + offset >= 0) & (place + offset < BLOCK), part, 0.0)
            total = part if total is None else total + part
        packed = total
        return [jnp.broadcast_to(packed[i : i + 1], (SUB, LANE)) for i in range(len(values))]

    def store_halves(origin):
        for mu in (3, 2, 1, 0):
            for index, s in enumerate((1, -1)):
                half = project(origin, mu, s)
                for part in (RE, IM):
                    for colour in range(3):
                        moved = cyclic(half[part][colour], mu, -s, early)
                        for spin in range(2):
                            halves[index, mu, part, spin, colour] = moved[spin]

    def site_apply(origin, target):
        for tile in range(2):
            def emit(part, spin, colour, value):
                target[part, spin, colour, tile] = value

            block_site_term(
                lambda chirality, row: clover[chirality, RE, row, row, tile],
                lambda chirality, low, high: (
                    clover[chirality, RE, low, high, tile],
                    twist[chirality, PAIRS[low, high], 0, tile],
                    twist[chirality, PAIRS[low, high], 1, tile],
                ),
                lambda part, spin, colour: origin[part, spin, colour, tile],
                emit,
            )

    def gather_hop(total, mu, index, got):
        for part in (RE, IM):
            for spin in range(2):
                total[part, spin] = total[part, spin] + got[spin][part]
                sign, from_part, from_spin = PAIR_H[mu][(spin, part)]
                total[part, 2 + spin] = signed_add(
                    total[part, 2 + spin], sign if index else -sign, got[from_spin][from_part]
                )

    def add_inner_hops(target):
        def hop_row(tile, row, carry):
            total = {(part, spin): target[part, spin, row, tile] for part in (RE, IM) for spin in range(4)}
            for mu in range(4):
                for index in range(2):
                    weights = [[inner[index, mu, form, row, col, tile] for col in range(3)] for form in range(3)]
                    got = []
                    for spin in range(2):
                        re, im = ([halves[index, mu, part, spin, c, tile] for c in range(3)] for part in (RE, IM))
                        both = [r + i for r, i in zip(re, im)]
                        got.append(three_products(*weights, re, im, both))
                    gather_hop(total, mu, index, got)
            for (part, spin), value in total.items():
                target[part, spin, row, tile] = value
            return carry

        for tile in range(2):
            for row in range(3):
                hop_row(tile, row, 0)

    def time_faces(turn_index):
        later, sooner = [], []
        for j in range(3):
            packed = recv_buf[turn_index * 6, j]
            moved = turn(packed, BLOCK, 1)
            later += [moved[0], packed[0], moved[1], packed[1]]
            packed = recv_buf[turn_index * 6 + 1, j]
            moved = turn(packed, BLOCK, 1)
            sooner += [packed[0], moved[0], packed[1], moved[1]]
        hops = {}
        for spin in range(2):
            for a in range(3):
                ahead = [None, None]
                for c in range(3):
                    u_re, u_im = links[0, RE, a, c, 1], links[0, IM, a, c, 1]
                    h_re, h_im = later[3 * spin + c], later[6 + 3 * spin + c]
                    terms = u_re * h_re - u_im * h_im, u_re * h_im + u_im * h_re
                    ahead = [t if old is None else old + t for old, t in zip(ahead, terms)]
                for part in (RE, IM):
                    behind = 0.5 * sooner[6 * part + 3 * spin + a]
                    hops[part, spin, a] = jnp.where(early8, behind, 0.5 * ahead[part])
                    hops[part, 2 + spin, a] = jnp.where(early8, behind, -0.5 * ahead[part])
        return hops

    facing = jnp.where(early8, 1.0, -1.0).astype(jnp.float32)

    def add_edge_operator(hops):
        for key, value in hops.items():
            edge[key] = value
            rest[key + (0,)] += jnp.where(early8, value, 0.0)
            rest[key + (1,)] += jnp.where(early8, 0.0, value)
        for mu in (3, 2, 1):
            for index, s in enumerate((1, -1)):
                half = project(edge, mu, s)
                for part in (RE, IM):
                    for colour in range(3):
                        moved = cyclic(half[part][colour], mu, -s, early)
                        for spin in range(2):
                            edge_halves[index, mu - 1, part, spin, colour] = moved[spin]
        mixed = {
            (part, spin, colour): turn(hops[part, spin, colour] + facing * hops[part, 2 + spin, colour], BLOCK, 0)
            for part in (RE, IM) for spin in range(2) for colour in range(3)
        }

        def emit(part, spin, colour, value):
            edge_out[part, spin, colour] = value

        block_site_term(
            lambda chirality, row: edge_diagonal[chirality, row],
            lambda chirality, low, high: tuple(edge_pair[chirality, PAIRS[low, high], form] for form in range(3)),
            lambda part, spin, colour: edge[part, spin, colour],
            emit,
        )
        for row in range(3):
            total = {(part, spin): edge_out[part, spin, row] for part in (RE, IM) for spin in range(4)}
            for mu in range(1, 4):
                for index in range(2):
                    weights = [[edge_inner[index, mu - 1, form, row, col] for col in range(3)] for form in range(3)]
                    got = []
                    for spin in range(2):
                        re, im = ([edge_halves[index, mu - 1, part, spin, c] for c in range(3)] for part in (RE, IM))
                        got.append(three_products(*weights, re, im, [r + i for r, i in zip(re, im)]))
                    gather_hop(total, mu, index, got)
            weights = [[edge_time[form, row, col] for col in range(3)] for form in range(3)]
            for spin in range(2):
                re, im = ([mixed[part, spin, c] for c in range(3)] for part in (RE, IM))
                got = three_products(*weights, re, im, [r + i for r, i in zip(re, im)])
                for part in (RE, IM):
                    for lower, value in ((0, got[part]), (2, -facing * got[part])):
                        acc[part, lower + spin, row, 0] += jnp.where(early8, total[part, lower + spin], value)
                        acc[part, lower + spin, row, 1] += jnp.where(early8, value, total[part, lower + spin])

    def times_alpha(field, spin, colour, tile):
        re, im = field[RE, spin, colour, tile], field[IM, spin, colour, tile]
        a_re, a_im = alpha[0], alpha[1]
        return a_re * re - a_im * im, a_re * im + a_im * re

    def subtract_scaled(target, scaled, spin, colour, tile):
        for part in (RE, IM):
            target[part, spin, colour, tile] -= scaled[part]

    def next_margins():
        zero = jnp.zeros((SUB, LANE), jnp.float32)

        def one_tile(tile, carry):
            margin_re, margin_im, norm = carry
            for spin in range(4):
                for colour in range(3):
                    a_re, a_im = acc[RE, spin, colour, tile], acc[IM, spin, colour, tile]
                    r_re, r_im = rest[RE, spin, colour, tile], rest[IM, spin, colour, tile]
                    margin_re = margin_re + (a_re * r_re + a_im * r_im)
                    margin_im = margin_im + (a_re * r_im - a_im * r_re)
                    norm = norm + (a_re * a_re + a_im * a_im)
            return margin_re, margin_im, norm

        return lax.fori_loop(0, 2, one_tile, (zero, zero, zero))

    def set_alpha(margins):
        sum_re, sum_im, sum_norm = block_sums(margins)
        sum_norm = sum_norm + EPSILON
        alpha[0] = sum_re / sum_norm
        alpha[1] = sum_im / sum_norm

    def advance_correction(tile):
        for spin in range(4):
            for colour in range(3):
                scaled = times_alpha(rest, spin, colour, tile)
                for part in (RE, IM):
                    corr[part, spin, colour, tile] += scaled[part]

    def advance_rest(tile):
        for spin in range(4):
            for colour in range(3):
                subtract_scaled(rest, times_alpha(acc, spin, colour, tile), spin, colour, tile)

    def full_step(_, margins):
        set_alpha(margins)
        store_halves(acc)
        site_apply(acc, twice)
        add_inner_hops(twice)
        zero = jnp.zeros((SUB, LANE), jnp.float32)

        def one_tile(tile, carry):
            margin_re, margin_im, norm = carry
            advance_correction(tile)
            advance_rest(tile)
            for spin in range(4):
                for colour in range(3):
                    subtract_scaled(acc, times_alpha(twice, spin, colour, tile), spin, colour, tile)
                    a_re, a_im = acc[RE, spin, colour, tile], acc[IM, spin, colour, tile]
                    r_re, r_im = rest[RE, spin, colour, tile], rest[IM, spin, colour, tile]
                    margin_re = margin_re + (a_re * r_re + a_im * r_im)
                    margin_im = margin_im + (a_re * r_im - a_im * r_re)
                    norm = norm + (a_re * a_re + a_im * a_im)
            return margin_re, margin_im, norm

        return lax.fori_loop(0, 2, one_tile, (zero, zero, zero))

    store_halves(rest)
    site_apply(rest, acc)
    add_inner_hops(acc)
    faces_wait(0, 0)
    add_edge_operator(time_faces(0))
    margins = lax.fori_loop(0, MR_STEPS - 1, full_step, next_margins())
    set_alpha(margins)
    for tile in range(2):
        advance_correction(tile)

    last = me["ta"] == count["ta"] - 1
    prepare_behind(1, corr, 0, False)
    pl.when(last)(lambda: face_copy(1, 0, 1).start())
    prepare_ahead(1, corr, 0)
    face_copy(1, 0, 0).start()
    pl.when(jnp.logical_not(last))(lambda: face_copy(1, 0, 1).start())
    for mu in (2, 1):
        prepare_ahead(1, corr, mu)
        face_copy(1, mu, 0).start()
        prepare_behind(1, corr, mu, False)
        face_copy(1, mu, 1).start()
    for tile in range(2):
        advance_rest(tile)
    for part in (RE, IM):
        for spin in range(4):
            update_out[part, spin] = x[part, spin] + corr[part, spin]
    zero_acc()
    for a, ahead, behind in x_hops(corr):
        ahead = tuple(jnp.where(high[3], v, 0.0) for v in ahead)
        behind = tuple(jnp.where(coord[3] % BLOCK == 0, v, 0.0) for v in behind)
        add_hops(acc, 3, a, ahead, behind)
    for mu in (1, 2):
        faces_wait(1, mu)
        arrived = unpack(recv_buf.at[6 + mu * 2], mu, BLOCK - 1)
        below = unpack(recv_buf.at[6 + mu * 2 + 1], mu, 0)
        for a in range(3):
            ahead = tuple(jnp.where(high[mu], v, 0.0) for v in link_row(links, mu, a, arrived))
            behind = tuple(jnp.where(coord[mu] == 0, below[part][a], 0.0) for part in (RE, IM))
            add_hops(acc, mu, a, ahead, behind)
    middle_sq = edge_sq = jnp.zeros((SUB, LANE), jnp.float32)
    for part in (RE, IM):
        for spin in range(4):
            for colour in range(3):
                value = rest[part, spin, colour] + 0.5 * acc[part, spin, colour]
                edge[part, spin, colour] = outer(value[0], value[1])
                value = outer(value[1], value[0])
                middle_sq = middle_sq + value * value
    stat_send[0:1] = slice_sums(middle_sq, jnp.where(early8, 2, 1))
    faces_wait(1, 0)
    for key, value in time_faces(1).items():
        value = edge[key] + value
        edge_sq = edge_sq + value * value
    stat_send[0:1] += slice_sums(edge_sq, jnp.where(early8, 0, BLOCK - 1))

    stat_copies = [
        pltpu.make_async_remote_copy(
            src_ref=stat_send,
            dst_ref=stat_recv.at[index - 1],
            send_sem=stat_send_sem,
            recv_sem=stat_recv_sem,
            device_id=peer(index),
            device_id_type=pl.DeviceIdType.MESH,
        )
        for index in sorted(range(1, group), key=lambda i: -spread(i))
    ]
    for copy in stat_copies:
        copy.start()
    pltpu.make_async_copy(send_buf, send_buf, send_sem).wait()
    stats = stat_send[...]
    pltpu.make_async_copy(stat_recv, stat_recv, stat_recv_sem).wait()
    for index in range(1, group):
        stats = stats + stat_recv[index - 1]
    profile_out[...] = (stats[0:1] / stats[1:2])[0, 0 : profile_out.shape[0]]
    pltpu.make_async_copy(stat_recv, stat_recv, stat_send_sem).wait()


def finish(held, ratio, update, profile, sems):
    stores = [pltpu.make_async_copy(held, update, sems.at[0]), pltpu.make_async_copy(ratio, profile, sems.at[1])]
    for store in stores:
        store.start()
    for store in stores:
        store.wait()


in_hbm = functools.partial(pltpu.with_memory_space_constraint, memory_space=pltpu.HBM)
in_vmem = functools.partial(pltpu.with_memory_space_constraint, memory_space=pltpu.VMEM)


def solution(mesh):
    sizes = tuple(mesh.shape[axis] for axis in AXES)
    group = mesh.shape["gz"] * mesh.shape["gy"]

    def local(source, start_guess, gauge_links, clover):
        times, depth, flat = source.shape[3:]
        assert times == depth == BLOCK and flat == LANE == BLOCK * LX
        tiles = (times * depth // SUB, SUB, LANE)
        spinor = source.shape[:3] + tiles
        gauge = gauge_links.shape[:4] + tiles
        site = clover.shape[:4] + tiles
        face = (12, 3) + tiles
        f32 = jnp.float32
        update, profile = pl.pallas_call(
            functools.partial(kernel, sizes),
            out_shape=(pltpu.VMEM(spinor, f32), pltpu.VMEM((times,), f32)),
            in_specs=[pl.BlockSpec(memory_space=pltpu.HBM)] * 4,
            out_specs=(pl.BlockSpec(memory_space=pltpu.VMEM),) * 2,
            scratch_shapes=[
                pltpu.VMEM(spinor, f32),
                pltpu.VMEM(spinor, f32),
                pltpu.VMEM(gauge, f32),
                pltpu.VMEM(site, f32),
                pltpu.VMEM((2, 4, 3, 3, 3) + tiles, f32),
                pltpu.VMEM((2, len(PAIRS), 2) + tiles, f32),
                pltpu.VMEM(spinor, f32),
                pltpu.VMEM(spinor, f32),
                pltpu.VMEM(spinor, f32),
                pltpu.VMEM(spinor, f32),
                pltpu.VMEM((2, SUB, LANE), f32),
                pltpu.VMEM((2, 4, 2, 2, 3) + tiles, f32),
                pltpu.VMEM((2, 4, 3, SUB, LANE), f32),
                pltpu.VMEM((2, 4, 3, SUB, LANE), f32),
                pltpu.VMEM((2, 3, 2, 2, 3, SUB, LANE), f32),
                pltpu.VMEM((2, 3, 3, 3, 3, SUB, LANE), f32),
                pltpu.VMEM((3, 3, 3, SUB, LANE), f32),
                pltpu.VMEM((2, 6, SUB, LANE), f32),
                pltpu.VMEM((2, len(PAIRS), 3, SUB, LANE), f32),
                pltpu.VMEM((3, 2, 3, 2) + tiles, f32),
                pltpu.VMEM(face, f32),
                pltpu.VMEM(face, f32),
                pltpu.VMEM((2, LANE), f32),
                pltpu.VMEM((group - 1, 2, LANE), f32),
                pltpu.SemaphoreType.DMA((7,)),
                pltpu.SemaphoreType.DMA,
                pltpu.SemaphoreType.DMA((6,)),
                pltpu.SemaphoreType.DMA,
                pltpu.SemaphoreType.DMA,
            ],
            compiler_params=pltpu.CompilerParams(
                collective_id=0, has_side_effects=True, vmem_limit_bytes=VMEM_LIMIT,
            ),
        )(
            in_hbm(start_guess.reshape(spinor)),
            in_hbm(source.reshape(spinor)),
            in_hbm(gauge_links.reshape(gauge)),
            in_hbm(clover.reshape(site)),
        )
        update, profile = pl.pallas_call(
            finish,
            out_shape=(jax.ShapeDtypeStruct(spinor, f32), jax.ShapeDtypeStruct((times,), f32)),
            in_specs=[pl.BlockSpec(memory_space=pltpu.VMEM)] * 2,
            out_specs=(pl.BlockSpec(memory_space=pl.ANY),) * 2,
            scratch_shapes=[pltpu.SemaphoreType.DMA((2,))],
        )(
            in_vmem(update),
            in_vmem(profile),
        )
        return update.reshape(source.shape), profile

    spinor_spec = P(None, None, None, "ta", "gz", "gy")
    matrix_spec = P(None, None, None, None, "ta", "gz", "gy")
    return jax.shard_map(
        local,
        mesh=mesh,
        in_specs=(spinor_spec, spinor_spec, matrix_spec, matrix_spec),
        out_specs=(spinor_spec, P("ta")),
        check_vma=False,
    )
```

```python
import functools

import jax
import jax.numpy as jnp
from jax import lax
from jax.experimental import pallas as pl
from jax.experimental.pallas import tpu as pltpu
from jax.sharding import PartitionSpec as P

LX = 32
BLOCK = 4
MR_STEPS = 4
EPSILON = 1e-6
AXES = ("ta", "gz", "gy")
RE, IM = 0, 1
SUB, LANE = 8, 128
VMEM_LIMIT = 24 * 2**20

PAIR = (
    {(0, RE): (1, RE, 0), (0, IM): (1, IM, 0), (1, RE): (1, RE, 1), (1, IM): (1, IM, 1)},
    {(0, RE): (1, IM, 0), (0, IM): (-1, RE, 0), (1, RE): (-1, IM, 1), (1, IM): (1, RE, 1)},
    {(0, RE): (-1, RE, 1), (0, IM): (-1, IM, 1), (1, RE): (1, RE, 0), (1, IM): (1, IM, 0)},
    {(0, RE): (1, IM, 1), (0, IM): (-1, RE, 1), (1, RE): (1, IM, 0), (1, IM): (-1, RE, 0)},
)
PAIR_H = (
    {(0, RE): (1, RE, 0), (0, IM): (1, IM, 0), (1, RE): (1, RE, 1), (1, IM): (1, IM, 1)},
    {(0, RE): (-1, IM, 0), (0, IM): (1, RE, 0), (1, RE): (1, IM, 1), (1, IM): (-1, RE, 1)},
    {(0, RE): (1, RE, 1), (0, IM): (1, IM, 1), (1, RE): (-1, RE, 0), (1, IM): (-1, IM, 0)},
    {(0, RE): (-1, IM, 1), (0, IM): (1, RE, 1), (1, RE): (-1, IM, 0), (1, IM): (1, RE, 0)},
)


PAIRS = {pair: i for i, pair in enumerate((low, high) for high in range(6) for low in range(high))}


def signed_add(base, sign, value):
    return base + value if sign > 0 else base - value


def project(field, mu, s):
    parts = ([], [])
    for part in (RE, IM):
        for colour in range(3):
            spins = []
            for spin in range(2):
                sign, from_part, from_spin = PAIR[mu][(spin, part)]
                spins.append(
                    signed_add(field[part, spin, colour], -s * sign, field[from_part, 2 + from_spin, colour])
                )
            parts[part].append(jnp.stack(spins))
    return parts


def link_row(links, mu, row, half):
    re = im = None
    for col in range(3):
        u_re, u_im = links[mu, RE, row, col][None], links[mu, IM, row, col][None]
        h_re, h_im = half[RE][col], half[IM][col]
        t_re = u_re * h_re - u_im * h_im
        t_im = u_re * h_im + u_im * h_re
        re, im = (t_re, t_im) if re is None else (re + t_re, im + t_im)
    return re, im


def adjoint_row(links, mu, row, half):
    re = im = None
    for col in range(3):
        u_re, u_im = links[mu, RE, col, row][None], links[mu, IM, col, row][None]
        h_re, h_im = half[RE][col], half[IM][col]
        t_re = u_re * h_re + u_im * h_im
        t_im = u_re * h_im - u_im * h_re
        re, im = (t_re, t_im) if re is None else (re + t_re, im + t_im)
    return re, im


def add_hops(acc, mu, colour, ahead, behind):
    difference = tuple(b - a for a, b in zip(ahead, behind))
    for part in (RE, IM):
        acc[part, 0:2, colour] += ahead[part] + behind[part]
        for spin in range(2):
            sign, from_part, from_spin = PAIR_H[mu][(spin, part)]
            old = acc[part, 2 + spin, colour]
            acc[part, 2 + spin, colour] = signed_add(old, sign, difference[from_part][from_spin])


def site_term(clover, field, emit):
    def pair(part, index):
        return jnp.stack([field[part, index // 3, index % 3], field[part, 2 + index // 3, index % 3]])

    vec = [[pair(part, j) for j in range(6)] for part in (RE, IM)]
    for row in range(6):
        diagonal = clover[:, RE, row, row]
        re, im = diagonal * vec[RE][row], diagonal * vec[IM][row]
        for col in range(6):
            if col == row:
                continue
            low, high = min(row, col), max(row, col)
            m_re, m_im = clover[:, RE, low, high], clover[:, IM, low, high]
            if row < col:
                re = re + m_re * vec[RE][col] - m_im * vec[IM][col]
                im = im + m_re * vec[IM][col] + m_im * vec[RE][col]
            else:
                re = re + m_re * vec[RE][col] + m_im * vec[IM][col]
                im = im + m_re * vec[IM][col] - m_im * vec[RE][col]
        for chirality in range(2):
            emit(RE, 2 * chirality + row // 3, row % 3, re[chirality])
            emit(IM, 2 * chirality + row // 3, row % 3, im[chirality])


def three_products(first, second, third, re, im, both):
    def dot(weights, values):
        total = None
        for weight, value in zip(weights, values):
            total = weight * value if total is None else total + weight * value
        return total

    shared = dot(first, both)
    return shared - dot(third, im), shared + dot(second, re)


def block_site_term(diagonals, triples, field, emit):
    for chirality in range(2):
        vec = [[field(part, 2 * chirality + j // 3, j % 3) for j in range(6)] for part in (RE, IM)]
        both = [r + i for r, i in zip(*vec)]
        for row in range(6):
            diagonal = diagonals(chirality, row)
            re, im, shared = diagonal * vec[RE][row], diagonal * vec[IM][row], None
            for col in range(6):
                if col == row:
                    continue
                low, high = min(row, col), max(row, col)
                real, less, more = triples(chirality, low, high)
                term = real * both[col]
                shared = term if shared is None else shared + term
                if row < col:
                    re, im = re - more * vec[IM][col], im + less * vec[RE][col]
                else:
                    re, im = re + less * vec[IM][col], im - more * vec[RE][col]
            emit(RE, 2 * chirality + row // 3, row % 3, re + shared)
            emit(IM, 2 * chirality + row // 3, row % 3, im + shared)


def swap_halves(value):
    axis = value.ndim - 3
    return jnp.concatenate(
        [lax.slice_in_dim(value, 1, 2, axis=axis), lax.slice_in_dim(value, 0, 1, axis=axis)], axis=axis
    )


def turn(value, shift, axis):
    shift = shift % value.shape[axis]
    return pltpu.roll(value, shift, axis) if shift else value


def cyclic(value, mu, units, early):
    axis = value.ndim - 2
    if mu == 3:
        return turn(value, units, axis + 1)
    if mu == 2:
        return turn(value, units * LX, axis + 1)
    if mu == 1:
        return turn(value, units, axis)
    units = units % BLOCK
    if units == 0:
        return value
    if units == 2:
        return swap_halves(value)
    rolled = turn(value, BLOCK, axis)
    swapped = swap_halves(rolled)
    return jnp.where(early, swapped, rolled) if units == 1 else jnp.where(early, rolled, swapped)


def kernel(
    sizes, x_in, source_in, links_in, clover_in, update_out, profile_out,
    x, source, links, clover, inner, twist, rest, corr, acc, twice, alpha, halves, edge, edge_out, edge_halves,
    edge_inner, edge_time, edge_diagonal, edge_pair, behind_store,
    send_buf, recv_buf, stat_send, stat_recv,
    in_sem, send_sem, recv_sem, stat_send_sem, stat_recv_sem,
):
    count = {axis: size for axis, size in zip(AXES, sizes)}
    group = count["gz"] * count["gy"]
    me = {axis: lax.axis_index(axis) for axis in AXES}

    def peer(index):
        return {
            "gz": lax.rem(me["gz"] + index // count["gy"], count["gz"]),
            "gy": lax.rem(me["gy"] + index % count["gy"], count["gy"]),
        }

    def spread(index):
        depth = index // count["gy"]
        return 2 * min(depth, count["gz"] - depth) + 3 * (index % count["gy"] != 0)

    def beside(axis, step):
        return {axis: lax.rem(me[axis] + step + count[axis], count[axis])}

    barrier = pltpu.get_barrier_semaphore()
    for step in (1, -1):
        pl.semaphore_signal(barrier, inc=1, device_id=beside("ta", step), device_id_type=pl.DeviceIdType.MESH)
    loads = [pltpu.make_async_copy(x_in, x, in_sem.at[0])]
    loads += [pltpu.make_async_copy(links_in.at[mu], links.at[mu], in_sem.at[1 + mu]) for mu in range(4)]
    loads.append(pltpu.make_async_copy(clover_in, clover, in_sem.at[5]))
    loads.append(pltpu.make_async_copy(source_in, source, in_sem.at[6]))
    for load in loads:
        load.start()

    for index in range(1, group):
        pl.semaphore_signal(barrier, inc=1, device_id=peer(index), device_id_type=pl.DeviceIdType.MESH)

    site = (2, SUB, LANE)
    row = lax.broadcasted_iota(jnp.int32, site, 1)
    lane = lax.broadcasted_iota(jnp.int32, site, 2)
    coord = (
        lax.broadcasted_iota(jnp.int32, site, 0) * 2 + row // BLOCK,
        row % BLOCK,
        lane // LX,
        lane % LX,
    )
    early = row < BLOCK
    row8 = lax.broadcasted_iota(jnp.int32, (SUB, LANE), 0)
    lane8 = lax.broadcasted_iota(jnp.int32, (SUB, LANE), 1)
    early8 = row8 < BLOCK
    high = tuple(c % BLOCK == BLOCK - 1 for c in coord)

    def x_neighbour(value, step):
        axis = value.ndim - 1
        if step > 0:
            return jnp.where(coord[3] == LX - 1, turn(value, LX - 1, axis), turn(value, -1, axis))
        return jnp.where(coord[3] == 0, turn(value, 1 - LX, axis), turn(value, 1, axis))

    def flat(half):
        return [half[part][colour][spin] for part in (RE, IM) for spin in range(2) for colour in range(3)]

    def pack(half, mu, edge, store, factor=None):
        values = flat(half)
        for j in range(3):
            packed = cyclic(values[4 * j], mu, -edge, early)
            for k in range(1, BLOCK):
                packed = jnp.where(coord[mu] == k, cyclic(values[4 * j + k], mu, k - edge, early), packed)
            store[j] = packed if factor is None else packed * factor

    def unpack(store, mu, edge):
        values = []
        for j in range(3):
            packed = store[j]
            values += [cyclic(packed, mu, edge - k, early) for k in range(BLOCK)]
        return [[jnp.stack([values[6 * p + c], values[6 * p + 3 + c]]) for c in range(3)] for p in (RE, IM)]

    def face_copy(turn_index, mu, side):
        slot = turn_index * 6 + mu * 2 + side
        return pltpu.make_async_remote_copy(
            src_ref=send_buf.at[slot],
            dst_ref=recv_buf.at[slot],
            send_sem=send_sem,
            recv_sem=recv_sem.at[turn_index * 3 + mu],
            device_id=beside(AXES[mu], -1 if side == 0 else 1),
            device_id_type=pl.DeviceIdType.MESH,
        )

    def faces_wait(turn_index, mu):
        pair = recv_buf.at[pl.ds(turn_index * 6 + mu * 2, 2)]
        pltpu.make_async_copy(pair, pair, recv_sem.at[turn_index * 3 + mu]).wait()

    def start_wrapped_first(turn_index):
        last = me["ta"] == count["ta"] - 1

        @pl.when(last)
        def _():
            face_copy(turn_index, 0, 1).start()
            face_copy(turn_index, 0, 0).start()

        @pl.when(jnp.logical_not(last))
        def _():
            face_copy(turn_index, 0, 0).start()
            face_copy(turn_index, 0, 1).start()

    first_t = jnp.where(me["ta"] == 0, -1.0, 1.0).astype(jnp.float32)
    last_t = jnp.where(me["ta"] == count["ta"] - 1, -1.0, 1.0).astype(jnp.float32)

    def prepare_ahead(turn_index, field, mu):
        pack(project(field, mu, 1), mu, 0, send_buf.at[turn_index * 6 + mu * 2], first_t if mu == 0 else None)

    def prepare_behind(turn_index, field, mu, keep):
        half = project(field, mu, -1)
        rows = [adjoint_row(links, mu, a, half) for a in range(3)]
        behind = [[rows[a][part] for a in range(3)] for part in (RE, IM)]
        pack(behind, mu, BLOCK - 1, send_buf.at[turn_index * 6 + mu * 2 + 1], last_t if mu == 0 else None)
        if keep:
            for part in (RE, IM):
                for a in range(3):
                    behind_store[mu, part, a] = behind[part][a]

    loads[0].wait()
    prepare_ahead(0, x, 0)
    loads[1].wait()
    prepare_behind(0, x, 0, True)
    prepare_ahead(0, x, 2)
    pl.semaphore_wait(barrier, group - 1 + 2)
    start_wrapped_first(0)
    face_copy(0, 2, 0).start()
    loads[3].wait()
    prepare_behind(0, x, 2, True)
    face_copy(0, 2, 1).start()
    prepare_ahead(0, x, 1)
    face_copy(0, 1, 0).start()
    loads[2].wait()
    prepare_behind(0, x, 1, True)
    face_copy(0, 1, 1).start()

    def zero_acc():
        acc[...] = jnp.zeros_like(acc)

    zero_acc()
    loads[4].wait()

    def x_hops(field):
        ahead_half = [[x_neighbour(v, 1) for v in values] for values in project(field, 3, 1)]
        behind_half = project(field, 3, -1)
        for a in range(3):
            ahead = link_row(links, 3, a, ahead_half)
            behind = tuple(x_neighbour(v, -1) for v in adjoint_row(links, 3, a, behind_half))
            yield a, ahead, behind

    for a, ahead, behind in x_hops(x):
        add_hops(acc, 3, a, ahead, behind)

    for mu in range(4):
        factor = jnp.where(high[mu], 0.0, -0.5).astype(jnp.float32)
        for a in range(3):
            for b in range(3):
                re, im = links[mu, RE, a, b] * factor, links[mu, IM, a, b] * factor
                inner[0, mu, 0, a, b] = re
                inner[0, mu, 1, a, b] = im - re
                inner[0, mu, 2, a, b] = im + re
                re, im = cyclic(re, mu, 1, early), cyclic(im, mu, 1, early)
                inner[1, mu, 0, b, a] = re
                inner[1, mu, 1, b, a] = -im - re
                inner[1, mu, 2, b, a] = re - im

    loads[5].wait()
    for chirality in range(2):
        for (low, high_row), index in PAIRS.items():
            re, im = clover[chirality, RE, low, high_row], clover[chirality, IM, low, high_row]
            twist[chirality, index, 0] = im - re
            twist[chirality, index, 1] = im + re
    def outer(first, second):
        return jnp.where(early8, first, second)

    for index in range(2):
        for mu in range(1, 4):
            for form in range(3):
                for a in range(3):
                    for b in range(3):
                        edge_inner[index, mu - 1, form, a, b] = outer(*(inner[index, mu, form, a, b, i] for i in range(2)))
    for form in range(3):
        for a in range(3):
            for b in range(3):
                edge_time[form, a, b] = outer(inner[0, 0, form, a, b, 1], inner[1, 0, form, a, b, 0])
    for chirality in range(2):
        for a in range(6):
            edge_diagonal[chirality, a] = outer(*(clover[chirality, RE, a, a, i] for i in range(2)))
        for (low, high_row), index in PAIRS.items():
            edge_pair[chirality, index, 0] = outer(*(clover[chirality, RE, low, high_row, i] for i in range(2)))
            for form in range(2):
                edge_pair[chirality, index, 1 + form] = outer(*(twist[chirality, index, form, i] for i in range(2)))
    loads[6].wait()

    def emit_rest(part, spin, colour, value):
        rest[part, spin, colour] = source[part, spin, colour] - value

    site_term(clover, x, emit_rest)
    source_sq = jnp.zeros(site, jnp.float32)
    for part in (RE, IM):
        for spin in range(4):
            for colour in range(3):
                value = source[part, spin, colour]
                source_sq = source_sq + value * value

    def slice_sums(value, time):
        sums = jnp.broadcast_to(jnp.sum(value, axis=1, keepdims=True), (SUB, LANE))
        return jnp.sum(jnp.where(time == lane8, sums, 0.0), axis=0, keepdims=True)

    stat_send[1:2] = slice_sums(source_sq[0], coord[0][0]) + slice_sums(source_sq[1], coord[0][1])

    local = project(x, 0, 1)
    ahead_half = [
        [jnp.where(coord[0] == BLOCK - 1, 0.0, cyclic(local[part][c], 0, -1, early)) for c in range(3)]
        for part in (RE, IM)
    ]
    for a in range(3):
        ahead = link_row(links, 0, a, ahead_half)
        behind = tuple(
            jnp.where(coord[0] == 0, 0.0, cyclic(behind_store[0, part, a], 0, 1, early)) for part in (RE, IM)
        )
        add_hops(acc, 0, a, ahead, behind)

    for mu in (1, 2):
        faces_wait(0, mu)
        arrived = unpack(recv_buf.at[mu * 2], mu, BLOCK - 1)
        local = project(x, mu, 1)
        ahead_half = [
            [
                jnp.where(coord[mu] == BLOCK - 1, arrived[part][c], cyclic(local[part][c], mu, -1, early))
                for c in range(3)
            ]
            for part in (RE, IM)
        ]
        below = unpack(recv_buf.at[mu * 2 + 1], mu, 0)
        for a in range(3):
            ahead = link_row(links, mu, a, ahead_half)
            behind = tuple(
                jnp.where(coord[mu] == 0, below[part][a], cyclic(behind_store[mu, part, a], mu, 1, early))
                for part in (RE, IM)
            )
            add_hops(acc, mu, a, ahead, behind)

    for part in (RE, IM):
        for spin in range(4):
            rest[part, spin] += 0.5 * acc[part, spin]
            corr[part, spin] = jnp.zeros_like(corr[part, spin])

    def block_sums(values):
        packed = None
        for index, value in enumerate(values):
            total = jnp.sum(value, axis=0, keepdims=True)
            total = jnp.broadcast_to(total, (SUB, LANE))
            packed = total if packed is None else jnp.where(row8 == index, total, packed)
        place = lane8 % BLOCK
        total = None
        for offset in range(1 - BLOCK, BLOCK):
            moved = [turn(packed, start - offset, 1) for start in range(0, LANE, LX)]
            while len(moved) > 1:
                moved = [p + q for p, q in zip(moved[::2], moved[1::2])]
            part = moved[0]
            if offset:
                part = jnp.where((place + offset >= 0) & (place + offset < BLOCK), part, 0.0)
            total = part if total is None else total + part
        packed = total
        return [jnp.broadcast_to(packed[i : i + 1], (SUB, LANE)) for i in range(len(values))]

    def store_halves(origin):
        for mu in (3, 2, 1, 0):
            for index, s in enumerate((1, -1)):
                half = project(origin, mu, s)
                for part in (RE, IM):
                    for colour in range(3):
                        moved = cyclic(half[part][colour], mu, -s, early)
                        for spin in range(2):
                            halves[index, mu, part, spin, colour] = moved[spin]

    def site_apply(origin, target):
        for tile in range(2):
            def emit(part, spin, colour, value):
                target[part, spin, colour, tile] = value

            block_site_term(
                lambda chirality, row: clover[chirality, RE, row, row, tile],
                lambda chirality, low, high: (
                    clover[chirality, RE, low, high, tile],
                    twist[chirality, PAIRS[low, high], 0, tile],
                    twist[chirality, PAIRS[low, high], 1, tile],
                ),
                lambda part, spin, colour: origin[part, spin, colour, tile],
                emit,
            )

    def gather_hop(total, mu, index, got):
        for part in (RE, IM):
            for spin in range(2):
                total[part, spin] = total[part, spin] + got[spin][part]
                sign, from_part, from_spin = PAIR_H[mu][(spin, part)]
                total[part, 2 + spin] = signed_add(
                    total[part, 2 + spin], sign if index else -sign, got[from_spin][from_part]
                )

    def add_inner_hops(target):
        for tile in range(2):
            total = {
                (row, part, spin): target[part, spin, row, tile]
                for row in range(3) for part in (RE, IM) for spin in range(4)
            }
            for mu in range(4):
                for index in range(2):
                    vectors = []
                    for spin in range(2):
                        re, im = ([halves[index, mu, part, spin, c, tile] for c in range(3)] for part in (RE, IM))
                        vectors.append((re, im, [r + i for r, i in zip(re, im)]))
                    for row in range(3):
                        weights = [[inner[index, mu, form, row, col, tile] for col in range(3)] for form in range(3)]
                        got = [three_products(*weights, *vector) for vector in vectors]
                        part_total = {(p, sp): total[row, p, sp] for p in (RE, IM) for sp in range(4)}
                        gather_hop(part_total, mu, index, got)
                        for (p, sp), value in part_total.items():
                            total[row, p, sp] = value
            for (row, part, spin), value in total.items():
                target[part, spin, row, tile] = value

    def time_faces(turn_index):
        later, sooner = [], []
        for j in range(3):
            packed = recv_buf[turn_index * 6, j]
            moved = turn(packed, BLOCK, 1)
            later += [moved[0], packed[0], moved[1], packed[1]]
            packed = recv_buf[turn_index * 6 + 1, j]
            moved = turn(packed, BLOCK, 1)
            sooner += [packed[0], moved[0], packed[1], moved[1]]
        hops = {}
        for spin in range(2):
            for a in range(3):
                ahead = [None, None]
                for c in range(3):
                    u_re, u_im = links[0, RE, a, c, 1], links[0, IM, a, c, 1]
                    h_re, h_im = later[3 * spin + c], later[6 + 3 * spin + c]
                    terms = u_re * h_re - u_im * h_im, u_re * h_im + u_im * h_re
                    ahead = [t if old is None else old + t for old, t in zip(ahead, terms)]
                for part in (RE, IM):
                    behind = 0.5 * sooner[6 * part + 3 * spin + a]
                    hops[part, spin, a] = jnp.where(early8, behind, 0.5 * ahead[part])
                    hops[part, 2 + spin, a] = jnp.where(early8, behind, -0.5 * ahead[part])
        return hops

    facing = jnp.where(early8, 1.0, -1.0).astype(jnp.float32)

    def add_edge_operator(hops):
        for key, value in hops.items():
            edge[key] = value
            rest[key + (0,)] += jnp.where(early8, value, 0.0)
            rest[key + (1,)] += jnp.where(early8, 0.0, value)
        for mu in (3, 2, 1):
            for index, s in enumerate((1, -1)):
                half = project(edge, mu, s)
                for part in (RE, IM):
                    for colour in range(3):
                        moved = cyclic(half[part][colour], mu, -s, early)
                        for spin in range(2):
                            edge_halves[index, mu - 1, part, spin, colour] = moved[spin]
        mixed = {
            (part, spin, colour): turn(hops[part, spin, colour] + facing * hops[part, 2 + spin, colour], BLOCK, 0)
            for part in (RE, IM) for spin in range(2) for colour in range(3)
        }

        def emit(part, spin, colour, value):
            edge_out[part, spin, colour] = value

        block_site_term(
            lambda chirality, row: edge_diagonal[chirality, row],
            lambda chirality, low, high: tuple(edge_pair[chirality, PAIRS[low, high], form] for form in range(3)),
            lambda part, spin, colour: edge[part, spin, colour],
            emit,
        )
        for row in range(3):
            total = {(part, spin): edge_out[part, spin, row] for part in (RE, IM) for spin in range(4)}
            for mu in range(1, 4):
                for index in range(2):
                    weights = [[edge_inner[index, mu - 1, form, row, col] for col in range(3)] for form in range(3)]
                    got = []
                    for spin in range(2):
                        re, im = ([edge_halves[index, mu - 1, part, spin, c] for c in range(3)] for part in (RE, IM))
                        got.append(three_products(*weights, re, im, [r + i for r, i in zip(re, im)]))
                    gather_hop(total, mu, index, got)
            weights = [[edge_time[form, row, col] for col in range(3)] for form in range(3)]
            for spin in range(2):
                re, im = ([mixed[part, spin, c] for c in range(3)] for part in (RE, IM))
                got = three_products(*weights, re, im, [r + i for r, i in zip(re, im)])
                for part in (RE, IM):
                    for lower, value in ((0, got[part]), (2, -facing * got[part])):
                        acc[part, lower + spin, row, 0] += jnp.where(early8, total[part, lower + spin], value)
                        acc[part, lower + spin, row, 1] += jnp.where(early8, value, total[part, lower + spin])

    def times_alpha(field, spin, colour, tile):
        re, im = field[RE, spin, colour, tile], field[IM, spin, colour, tile]
        a_re, a_im = alpha[0], alpha[1]
        return a_re * re - a_im * im, a_re * im + a_im * re

    def subtract_scaled(target, scaled, spin, colour, tile):
        for part in (RE, IM):
            target[part, spin, colour, tile] -= scaled[part]

    def next_margins():
        zero = jnp.zeros((SUB, LANE), jnp.float32)

        def one_tile(tile, carry):
            margin_re, margin_im, norm = carry
            for spin in range(4):
                for colour in range(3):
                    a_re, a_im = acc[RE, spin, colour, tile], acc[IM, spin, colour, tile]
                    r_re, r_im = rest[RE, spin, colour, tile], rest[IM, spin, colour, tile]
                    margin_re = margin_re + (a_re * r_re + a_im * r_im)
                    margin_im = margin_im + (a_re * r_im - a_im * r_re)
                    norm = norm + (a_re * a_re + a_im * a_im)
            return margin_re, margin_im, norm

        return one_tile(1, one_tile(0, (zero, zero, zero)))

    def set_alpha(margins):
        sum_re, sum_im, sum_norm = block_sums(margins)
        sum_norm = sum_norm + EPSILON
        alpha[0] = sum_re / sum_norm
        alpha[1] = sum_im / sum_norm

    def advance_correction(tile):
        for spin in range(4):
            for colour in range(3):
                scaled = times_alpha(rest, spin, colour, tile)
                for part in (RE, IM):
                    corr[part, spin, colour, tile] += scaled[part]

    def advance_rest(tile):
        for spin in range(4):
            for colour in range(3):
                subtract_scaled(rest, times_alpha(acc, spin, colour, tile), spin, colour, tile)

    def full_step(_, margins):
        set_alpha(margins)
        store_halves(acc)
        site_apply(acc, twice)
        add_inner_hops(twice)
        zero = jnp.zeros((SUB, LANE), jnp.float32)

        def one_tile(tile, carry):
            margin_re, margin_im, norm = carry
            advance_correction(tile)
            advance_rest(tile)
            for spin in range(4):
                for colour in range(3):
                    subtract_scaled(acc, times_alpha(twice, spin, colour, tile), spin, colour, tile)
                    a_re, a_im = acc[RE, spin, colour, tile], acc[IM, spin, colour, tile]
                    r_re, r_im = rest[RE, spin, colour, tile], rest[IM, spin, colour, tile]
                    margin_re = margin_re + (a_re * r_re + a_im * r_im)
                    margin_im = margin_im + (a_re * r_im - a_im * r_re)
                    norm = norm + (a_re * a_re + a_im * a_im)
            return margin_re, margin_im, norm

        return one_tile(1, one_tile(0, (zero, zero, zero)))

    store_halves(rest)
    site_apply(rest, acc)
    add_inner_hops(acc)
    faces_wait(0, 0)
    add_edge_operator(time_faces(0))
    margins = next_margins()
    for step in range(MR_STEPS - 1):
        margins = full_step(step, margins)
    def time_edge(field, tile, s):
        half = [
            [[signed_add(field[part, spin, c, tile], -s, field[part, 2 + spin, c, tile]) for c in range(3)] for spin in range(2)]
            for part in (RE, IM)
        ]
        if s > 0:
            return half
        rows = [[[None] * 3 for _ in range(2)] for _ in range(2)]
        for spin in range(2):
            for a in range(3):
                for c in range(3):
                    u_re, u_im = links[0, RE, c, a, tile], links[0, IM, c, a, tile]
                    h_re, h_im = half[RE][spin][c], half[IM][spin][c]
                    for part, term in ((RE, u_re * h_re + u_im * h_im), (IM, u_re * h_im - u_im * h_re)):
                        old = rows[part][spin][a]
                        rows[part][spin][a] = term if old is None else old + term
        return rows

    def send_time_edge(side, known, residual, factor):
        a_re, a_im = alpha[0], alpha[1]
        values = [[], []]
        for spin in range(2):
            for c in range(3):
                r_re, r_im = residual[RE][spin][c], residual[IM][spin][c]
                values[RE].append((known[RE][spin][c] + (a_re * r_re - a_im * r_im)) * factor)
                values[IM].append((known[IM][spin][c] + (a_re * r_im + a_im * r_re)) * factor)
        values = values[RE] + values[IM]
        for j in range(3):
            for tile in range(2):
                first, second = values[4 * j + 2 * tile], values[4 * j + 2 * tile + 1]
                if side:
                    first = turn(first, BLOCK, 0)
                else:
                    second = turn(second, BLOCK, 0)
                send_buf[6 + side, j, tile] = outer(first, second)

    known = [time_edge(corr, 0, 1), time_edge(corr, 1, -1)]
    residual = [time_edge(rest, 0, 1), time_edge(rest, 1, -1)]
    set_alpha(margins)
    send_time_edge(1, known[1], residual[1], last_t)
    send_time_edge(0, known[0], residual[0], first_t)
    start_wrapped_first(1)
    for tile in range(2):
        advance_correction(tile)
    for mu in (2, 1):
        prepare_ahead(1, corr, mu)
        face_copy(1, mu, 0).start()
        prepare_behind(1, corr, mu, False)
        face_copy(1, mu, 1).start()
    for tile in range(2):
        advance_rest(tile)
    for part in (RE, IM):
        for spin in range(4):
            update_out[part, spin] = x[part, spin] + corr[part, spin]
    zero_acc()
    for a, ahead, behind in x_hops(corr):
        ahead = tuple(jnp.where(high[3], v, 0.0) for v in ahead)
        behind = tuple(jnp.where(coord[3] % BLOCK == 0, v, 0.0) for v in behind)
        add_hops(acc, 3, a, ahead, behind)
    for mu in (1, 2):
        faces_wait(1, mu)
        arrived = unpack(recv_buf.at[6 + mu * 2], mu, BLOCK - 1)
        below = unpack(recv_buf.at[6 + mu * 2 + 1], mu, 0)
        for a in range(3):
            ahead = tuple(jnp.where(high[mu], v, 0.0) for v in link_row(links, mu, a, arrived))
            behind = tuple(jnp.where(coord[mu] == 0, below[part][a], 0.0) for part in (RE, IM))
            add_hops(acc, mu, a, ahead, behind)
    middle_sq = edge_sq = jnp.zeros((SUB, LANE), jnp.float32)
    for part in (RE, IM):
        for spin in range(4):
            for colour in range(3):
                value = rest[part, spin, colour] + 0.5 * acc[part, spin, colour]
                edge[part, spin, colour] = outer(value[0], value[1])
                value = outer(value[1], value[0])
                middle_sq = middle_sq + value * value
    stat_send[0:1] = slice_sums(middle_sq, jnp.where(early8, 2, 1))
    faces_wait(1, 0)
    for key, value in time_faces(1).items():
        value = edge[key] + value
        edge_sq = edge_sq + value * value
    stat_send[0:1] += slice_sums(edge_sq, jnp.where(early8, 0, BLOCK - 1))

    stat_copies = [
        pltpu.make_async_remote_copy(
            src_ref=stat_send,
            dst_ref=stat_recv.at[index - 1],
            send_sem=stat_send_sem,
            recv_sem=stat_recv_sem,
            device_id=peer(index),
            device_id_type=pl.DeviceIdType.MESH,
        )
        for index in sorted(range(1, group), key=lambda i: -spread(i))
    ]
    for copy in stat_copies:
        copy.start()
    pltpu.make_async_copy(send_buf, send_buf, send_sem).wait()
    stats = stat_send[...]
    pltpu.make_async_copy(stat_recv, stat_recv, stat_recv_sem).wait()
    for index in range(1, group):
        stats = stats + stat_recv[index - 1]
    profile_out[...] = (stats[0:1] / stats[1:2])[0, 0 : profile_out.shape[0]]
    pltpu.make_async_copy(stat_recv, stat_recv, stat_send_sem).wait()


def finish(held, ratio, update, profile, sems):
    stores = [pltpu.make_async_copy(held, update, sems.at[0]), pltpu.make_async_copy(ratio, profile, sems.at[1])]
    for store in stores:
        store.start()
    for store in stores:
        store.wait()


in_hbm = functools.partial(pltpu.with_memory_space_constraint, memory_space=pltpu.HBM)
in_vmem = functools.partial(pltpu.with_memory_space_constraint, memory_space=pltpu.VMEM)


def solution(mesh):
    sizes = tuple(mesh.shape[axis] for axis in AXES)
    group = mesh.shape["gz"] * mesh.shape["gy"]

    def local(source, start_guess, gauge_links, clover):
        times, depth, flat = source.shape[3:]
        assert times == depth == BLOCK and flat == LANE == BLOCK * LX
        tiles = (times * depth // SUB, SUB, LANE)
        spinor = source.shape[:3] + tiles
        gauge = gauge_links.shape[:4] + tiles
        site = clover.shape[:4] + tiles
        face = (12, 3) + tiles
        f32 = jnp.float32
        update, profile = pl.pallas_call(
            functools.partial(kernel, sizes),
            out_shape=(pltpu.VMEM(spinor, f32), pltpu.VMEM((times,), f32)),
            in_specs=[pl.BlockSpec(memory_space=pltpu.HBM)] * 4,
            out_specs=(pl.BlockSpec(memory_space=pltpu.VMEM),) * 2,
            scratch_shapes=[
                pltpu.VMEM(spinor, f32),
                pltpu.VMEM(spinor, f32),
                pltpu.VMEM(gauge, f32),
                pltpu.VMEM(site, f32),
                pltpu.VMEM((2, 4, 3, 3, 3) + tiles, f32),
                pltpu.VMEM((2, len(PAIRS), 2) + tiles, f32),
                pltpu.VMEM(spinor, f32),
                pltpu.VMEM(spinor, f32),
                pltpu.VMEM(spinor, f32),
                pltpu.VMEM(spinor, f32),
                pltpu.VMEM((2, SUB, LANE), f32),
                pltpu.VMEM((2, 4, 2, 2, 3) + tiles, f32),
                pltpu.VMEM((2, 4, 3, SUB, LANE), f32),
                pltpu.VMEM((2, 4, 3, SUB, LANE), f32),
                pltpu.VMEM((2, 3, 2, 2, 3, SUB, LANE), f32),
                pltpu.VMEM((2, 3, 3, 3, 3, SUB, LANE), f32),
                pltpu.VMEM((3, 3, 3, SUB, LANE), f32),
                pltpu.VMEM((2, 6, SUB, LANE), f32),
                pltpu.VMEM((2, len(PAIRS), 3, SUB, LANE), f32),
                pltpu.VMEM((3, 2, 3, 2) + tiles, f32),
                pltpu.VMEM(face, f32),
                pltpu.VMEM(face, f32),
                pltpu.VMEM((2, LANE), f32),
                pltpu.VMEM((group - 1, 2, LANE), f32),
                pltpu.SemaphoreType.DMA((7,)),
                pltpu.SemaphoreType.DMA,
                pltpu.SemaphoreType.DMA((6,)),
                pltpu.SemaphoreType.DMA,
                pltpu.SemaphoreType.DMA,
            ],
            compiler_params=pltpu.CompilerParams(
                collective_id=0, has_side_effects=True, vmem_limit_bytes=VMEM_LIMIT,
            ),
        )(
            in_hbm(start_guess.reshape(spinor)),
            in_hbm(source.reshape(spinor)),
            in_hbm(gauge_links.reshape(gauge)),
            in_hbm(clover.reshape(site)),
        )
        update, profile = pl.pallas_call(
            finish,
            out_shape=(jax.ShapeDtypeStruct(spinor, f32), jax.ShapeDtypeStruct((times,), f32)),
            in_specs=[pl.BlockSpec(memory_space=pltpu.VMEM)] * 2,
            out_specs=(pl.BlockSpec(memory_space=pl.ANY),) * 2,
            scratch_shapes=[pltpu.SemaphoreType.DMA((2,))],
        )(
            in_vmem(update),
            in_vmem(profile),
        )
        return update.reshape(source.shape), profile

    spinor_spec = P(None, None, None, "ta", "gz", "gy")
    matrix_spec = P(None, None, None, None, "ta", "gz", "gy")
    return jax.shard_map(
        local,
        mesh=mesh,
        in_specs=(spinor_spec, spinor_spec, matrix_spec, matrix_spec),
        out_specs=(spinor_spec, P("ta")),
        check_vma=False,
    )
```

```python
import functools

import jax
import jax.numpy as jnp
from jax import lax
from jax.experimental import pallas as pl
from jax.experimental.pallas import tpu as pltpu
from jax.sharding import PartitionSpec as P

LX = 32
BLOCK = 4
MR_STEPS = 4
EPSILON = 1e-6
AXES = ("ta", "gz", "gy")
RE, IM = 0, 1
SUB, LANE = 8, 128
VMEM_LIMIT = 24 * 2**20

PAIR = (
    {(0, RE): (1, RE, 0), (0, IM): (1, IM, 0), (1, RE): (1, RE, 1), (1, IM): (1, IM, 1)},
    {(0, RE): (1, IM, 0), (0, IM): (-1, RE, 0), (1, RE): (-1, IM, 1), (1, IM): (1, RE, 1)},
    {(0, RE): (-1, RE, 1), (0, IM): (-1, IM, 1), (1, RE): (1, RE, 0), (1, IM): (1, IM, 0)},
    {(0, RE): (1, IM, 1), (0, IM): (-1, RE, 1), (1, RE): (1, IM, 0), (1, IM): (-1, RE, 0)},
)
PAIR_H = (
    {(0, RE): (1, RE, 0), (0, IM): (1, IM, 0), (1, RE): (1, RE, 1), (1, IM): (1, IM, 1)},
    {(0, RE): (-1, IM, 0), (0, IM): (1, RE, 0), (1, RE): (1, IM, 1), (1, IM): (-1, RE, 1)},
    {(0, RE): (1, RE, 1), (0, IM): (1, IM, 1), (1, RE): (-1, RE, 0), (1, IM): (-1, IM, 0)},
    {(0, RE): (-1, IM, 1), (0, IM): (1, RE, 1), (1, RE): (-1, IM, 0), (1, IM): (1, RE, 0)},
)


PAIRS = {pair: i for i, pair in enumerate((low, high) for high in range(6) for low in range(high))}


def signed_add(base, sign, value):
    return base + value if sign > 0 else base - value


def project(field, mu, s):
    parts = ([], [])
    for part in (RE, IM):
        for colour in range(3):
            spins = []
            for spin in range(2):
                sign, from_part, from_spin = PAIR[mu][(spin, part)]
                spins.append(
                    signed_add(field[part, spin, colour], -s * sign, field[from_part, 2 + from_spin, colour])
                )
            parts[part].append(jnp.stack(spins))
    return parts


def link_row(links, mu, row, half):
    re = im = None
    for col in range(3):
        u_re, u_im = links[mu, RE, row, col][None], links[mu, IM, row, col][None]
        h_re, h_im = half[RE][col], half[IM][col]
        t_re = u_re * h_re - u_im * h_im
        t_im = u_re * h_im + u_im * h_re
        re, im = (t_re, t_im) if re is None else (re + t_re, im + t_im)
    return re, im


def adjoint_row(links, mu, row, half):
    re = im = None
    for col in range(3):
        u_re, u_im = links[mu, RE, col, row][None], links[mu, IM, col, row][None]
        h_re, h_im = half[RE][col], half[IM][col]
        t_re = u_re * h_re + u_im * h_im
        t_im = u_re * h_im - u_im * h_re
        re, im = (t_re, t_im) if re is None else (re + t_re, im + t_im)
    return re, im


def add_hops(acc, mu, colour, ahead, behind):
    difference = tuple(b - a for a, b in zip(ahead, behind))
    for part in (RE, IM):
        acc[part, 0:2, colour] += ahead[part] + behind[part]
        for spin in range(2):
            sign, from_part, from_spin = PAIR_H[mu][(spin, part)]
            old = acc[part, 2 + spin, colour]
            acc[part, 2 + spin, colour] = signed_add(old, sign, difference[from_part][from_spin])


def site_term(clover, field, emit):
    def pair(part, index):
        return jnp.stack([field[part, index // 3, index % 3], field[part, 2 + index // 3, index % 3]])

    vec = [[pair(part, j) for j in range(6)] for part in (RE, IM)]
    for row in range(6):
        diagonal = clover[:, RE, row, row]
        re, im = diagonal * vec[RE][row], diagonal * vec[IM][row]
        for col in range(6):
            if col == row:
                continue
            low, high = min(row, col), max(row, col)
            m_re, m_im = clover[:, RE, low, high], clover[:, IM, low, high]
            if row < col:
                re = re + m_re * vec[RE][col] - m_im * vec[IM][col]
                im = im + m_re * vec[IM][col] + m_im * vec[RE][col]
            else:
                re = re + m_re * vec[RE][col] + m_im * vec[IM][col]
                im = im + m_re * vec[IM][col] - m_im * vec[RE][col]
        for chirality in range(2):
            emit(RE, 2 * chirality + row // 3, row % 3, re[chirality])
            emit(IM, 2 * chirality + row // 3, row % 3, im[chirality])


def three_products(first, second, third, re, im, both):
    def dot(weights, values):
        total = None
        for weight, value in zip(weights, values):
            total = weight * value if total is None else total + weight * value
        return total

    shared = dot(first, both)
    return shared - dot(third, im), shared + dot(second, re)


def block_site_term(diagonals, triples, field, emit):
    for chirality in range(2):
        vec = [[field(part, 2 * chirality + j // 3, j % 3) for j in range(6)] for part in (RE, IM)]
        both = [r + i for r, i in zip(*vec)]
        for row in range(6):
            diagonal = diagonals(chirality, row)
            re, im, shared = diagonal * vec[RE][row], diagonal * vec[IM][row], None
            for col in range(6):
                if col == row:
                    continue
                low, high = min(row, col), max(row, col)
                real, less, more = triples(chirality, low, high)
                term = real * both[col]
                shared = term if shared is None else shared + term
                if row < col:
                    re, im = re - more * vec[IM][col], im + less * vec[RE][col]
                else:
                    re, im = re + less * vec[IM][col], im - more * vec[RE][col]
            emit(RE, 2 * chirality + row // 3, row % 3, re + shared)
            emit(IM, 2 * chirality + row // 3, row % 3, im + shared)


def swap_halves(value):
    axis = value.ndim - 3
    return jnp.concatenate(
        [lax.slice_in_dim(value, 1, 2, axis=axis), lax.slice_in_dim(value, 0, 1, axis=axis)], axis=axis
    )


def turn(value, shift, axis):
    shift = shift % value.shape[axis]
    return pltpu.roll(value, shift, axis) if shift else value


def cyclic(value, mu, units, early):
    axis = value.ndim - 2
    if mu == 3:
        return turn(value, units, axis + 1)
    if mu == 2:
        return turn(value, units * LX, axis + 1)
    if mu == 1:
        return turn(value, units, axis)
    units = units % BLOCK
    if units == 0:
        return value
    if units == 2:
        return swap_halves(value)
    rolled = turn(value, BLOCK, axis)
    swapped = swap_halves(rolled)
    return jnp.where(early, swapped, rolled) if units == 1 else jnp.where(early, rolled, swapped)


def kernel(
    sizes, x_in, source_in, links_in, clover_in, update_out, profile_out,
    x, source, links, clover, inner, twist, rest, corr, acc, twice, alpha, halves, edge, edge_out, edge_halves,
    edge_inner, edge_time, edge_diagonal, edge_pair, behind_store,
    send_buf, recv_buf, relay_buf, stat_send, stat_recv,
    in_sem, send_sem, recv_sem, relay_sem, stat_send_sem, stat_recv_sem,
):
    count = {axis: size for axis, size in zip(AXES, sizes)}
    group = count["gz"] * count["gy"]
    me = {axis: lax.axis_index(axis) for axis in AXES}

    def peer(index):
        return {
            "gz": lax.rem(me["gz"] + index // count["gy"], count["gz"]),
            "gy": lax.rem(me["gy"] + index % count["gy"], count["gy"]),
        }

    def spread(index):
        depth = index // count["gy"]
        return 2 * min(depth, count["gz"] - depth) + 3 * (index % count["gy"] != 0)

    def beside(axis, step):
        return {axis: lax.rem(me[axis] + step + count[axis], count[axis])}

    barrier = pltpu.get_barrier_semaphore()
    opens, closes = me["ta"] == 0, me["ta"] == count["ta"] - 1
    outer_core = lax.rem(me["gz"], 2)
    through = me["gz"] + jnp.where(jnp.logical_and(closes, outer_core == 0), 1, 0)
    for target in ({"gz": through, **beside("ta", 1)}, beside("ta", -1)):
        pl.semaphore_signal(barrier, inc=1, device_id=target, device_id_type=pl.DeviceIdType.MESH)
    loads = [pltpu.make_async_copy(x_in, x, in_sem.at[0])]
    loads += [pltpu.make_async_copy(links_in.at[mu], links.at[mu], in_sem.at[1 + mu]) for mu in range(4)]
    loads.append(pltpu.make_async_copy(clover_in, clover, in_sem.at[5]))
    loads.append(pltpu.make_async_copy(source_in, source, in_sem.at[6]))
    for load in loads:
        load.start()

    for index in range(1, group):
        pl.semaphore_signal(barrier, inc=1, device_id=peer(index), device_id_type=pl.DeviceIdType.MESH)

    site = (2, SUB, LANE)
    row = lax.broadcasted_iota(jnp.int32, site, 1)
    lane = lax.broadcasted_iota(jnp.int32, site, 2)
    coord = (
        lax.broadcasted_iota(jnp.int32, site, 0) * 2 + row // BLOCK,
        row % BLOCK,
        lane // LX,
        lane % LX,
    )
    early = row < BLOCK
    row8 = lax.broadcasted_iota(jnp.int32, (SUB, LANE), 0)
    lane8 = lax.broadcasted_iota(jnp.int32, (SUB, LANE), 1)
    early8 = row8 < BLOCK
    high = tuple(c % BLOCK == BLOCK - 1 for c in coord)

    def x_neighbour(value, step):
        axis = value.ndim - 1
        if step > 0:
            return jnp.where(coord[3] == LX - 1, turn(value, LX - 1, axis), turn(value, -1, axis))
        return jnp.where(coord[3] == 0, turn(value, 1 - LX, axis), turn(value, 1, axis))

    def flat(half):
        return [half[part][colour][spin] for part in (RE, IM) for spin in range(2) for colour in range(3)]

    def pack(half, mu, edge, store, factor=None):
        values = flat(half)
        for j in range(3):
            packed = cyclic(values[4 * j], mu, -edge, early)
            for k in range(1, BLOCK):
                packed = jnp.where(coord[mu] == k, cyclic(values[4 * j + k], mu, k - edge, early), packed)
            store[j] = packed if factor is None else packed * factor

    def unpack(store, mu, edge):
        values = []
        for j in range(3):
            packed = store[j]
            values += [cyclic(packed, mu, edge - k, early) for k in range(BLOCK)]
        return [[jnp.stack([values[6 * p + c], values[6 * p + 3 + c]]) for c in range(3)] for p in (RE, IM)]

    def face_copy(turn_index, mu, side):
        slot = turn_index * 6 + mu * 2 + side
        return pltpu.make_async_remote_copy(
            src_ref=send_buf.at[slot],
            dst_ref=recv_buf.at[slot],
            send_sem=send_sem,
            recv_sem=recv_sem.at[turn_index * 3 + mu],
            device_id=beside(AXES[mu], -1 if side == 0 else 1),
            device_id_type=pl.DeviceIdType.MESH,
        )

    def faces_wait(turn_index, mu):
        pair = recv_buf.at[pl.ds(turn_index * 6 + mu * 2, 2)]
        pltpu.make_async_copy(pair, pair, recv_sem.at[turn_index * 3 + mu]).wait()

    def relay_copy():
        return pltpu.make_async_remote_copy(
            src_ref=send_buf.at[0],
            dst_ref=relay_buf,
            send_sem=send_sem,
            recv_sem=relay_sem.at[0],
            device_id={"gz": me["gz"] + 1 - 2 * outer_core},
            device_id_type=pl.DeviceIdType.MESH,
        )

    def forward_copy():
        return pltpu.make_async_remote_copy(
            src_ref=relay_buf,
            dst_ref=recv_buf.at[0],
            send_sem=relay_sem.at[1],
            recv_sem=recv_sem.at[0],
            device_id={"gz": me["gz"] + 1 - 2 * outer_core, **beside("ta", -1)},
            device_id_type=pl.DeviceIdType.MESH,
        )

    relays = jnp.logical_and(opens, outer_core == 1)

    def start_first_turn():
        @pl.when(jnp.logical_and(opens, outer_core == 0))
        def _():
            relay_copy().start()
            face_copy(0, 0, 1).start()

        @pl.when(relays)
        def _():
            relay_copy().wait_recv()
            forward_copy().start()

        @pl.when(jnp.logical_not(jnp.logical_and(opens, outer_core == 0)))
        def _():
            start_wrapped_first(0)

    def start_wrapped_first(turn_index):
        last = me["ta"] == count["ta"] - 1

        @pl.when(last)
        def _():
            face_copy(turn_index, 0, 1).start()
            face_copy(turn_index, 0, 0).start()

        @pl.when(jnp.logical_not(last))
        def _():
            face_copy(turn_index, 0, 0).start()
            face_copy(turn_index, 0, 1).start()

    first_t = jnp.where(me["ta"] == 0, -1.0, 1.0).astype(jnp.float32)
    last_t = jnp.where(me["ta"] == count["ta"] - 1, -1.0, 1.0).astype(jnp.float32)

    def prepare_ahead(turn_index, field, mu):
        pack(project(field, mu, 1), mu, 0, send_buf.at[turn_index * 6 + mu * 2], first_t if mu == 0 else None)

    def prepare_behind(turn_index, field, mu, keep):
        half = project(field, mu, -1)
        rows = [adjoint_row(links, mu, a, half) for a in range(3)]
        behind = [[rows[a][part] for a in range(3)] for part in (RE, IM)]
        pack(behind, mu, BLOCK - 1, send_buf.at[turn_index * 6 + mu * 2 + 1], last_t if mu == 0 else None)
        if keep:
            for part in (RE, IM):
                for a in range(3):
                    behind_store[mu, part, a] = behind[part][a]

    loads[0].wait()
    prepare_ahead(0, x, 0)
    loads[1].wait()
    prepare_behind(0, x, 0, True)
    prepare_ahead(0, x, 2)
    pl.semaphore_wait(barrier, group + 1 + jnp.where(opens, 2 * outer_core - 1, 0))
    start_first_turn()
    face_copy(0, 2, 0).start()
    loads[3].wait()
    prepare_behind(0, x, 2, True)
    face_copy(0, 2, 1).start()
    prepare_ahead(0, x, 1)
    face_copy(0, 1, 0).start()
    loads[2].wait()
    prepare_behind(0, x, 1, True)
    face_copy(0, 1, 1).start()

    def zero_acc():
        acc[...] = jnp.zeros_like(acc)

    zero_acc()
    loads[4].wait()

    def x_hops(field):
        ahead_half = [[x_neighbour(v, 1) for v in values] for values in project(field, 3, 1)]
        behind_half = project(field, 3, -1)
        for a in range(3):
            ahead = link_row(links, 3, a, ahead_half)
            behind = tuple(x_neighbour(v, -1) for v in adjoint_row(links, 3, a, behind_half))
            yield a, ahead, behind

    for a, ahead, behind in x_hops(x):
        add_hops(acc, 3, a, ahead, behind)

    for mu in range(4):
        factor = jnp.where(high[mu], 0.0, -0.5).astype(jnp.float32)
        for a in range(3):
            for b in range(3):
                re, im = links[mu, RE, a, b] * factor, links[mu, IM, a, b] * factor
                inner[0, mu, 0, a, b] = re
                inner[0, mu, 1, a, b] = im - re
                inner[0, mu, 2, a, b] = im + re
                re, im = cyclic(re, mu, 1, early), cyclic(im, mu, 1, early)
                inner[1, mu, 0, b, a] = re
                inner[1, mu, 1, b, a] = -im - re
                inner[1, mu, 2, b, a] = re - im

    loads[5].wait()
    for chirality in range(2):
        for (low, high_row), index in PAIRS.items():
            re, im = clover[chirality, RE, low, high_row], clover[chirality, IM, low, high_row]
            twist[chirality, index, 0] = im - re
            twist[chirality, index, 1] = im + re
    def outer(first, second):
        return jnp.where(early8, first, second)

    for index in range(2):
        for mu in range(1, 4):
            for form in range(3):
                for a in range(3):
                    for b in range(3):
                        edge_inner[index, mu - 1, form, a, b] = outer(*(inner[index, mu, form, a, b, i] for i in range(2)))
    for form in range(3):
        for a in range(3):
            for b in range(3):
                edge_time[form, a, b] = outer(inner[0, 0, form, a, b, 1], inner[1, 0, form, a, b, 0])
    for chirality in range(2):
        for a in range(6):
            edge_diagonal[chirality, a] = outer(*(clover[chirality, RE, a, a, i] for i in range(2)))
        for (low, high_row), index in PAIRS.items():
            edge_pair[chirality, index, 0] = outer(*(clover[chirality, RE, low, high_row, i] for i in range(2)))
            for form in range(2):
                edge_pair[chirality, index, 1 + form] = outer(*(twist[chirality, index, form, i] for i in range(2)))
    loads[6].wait()

    def emit_rest(part, spin, colour, value):
        rest[part, spin, colour] = source[part, spin, colour] - value

    site_term(clover, x, emit_rest)
    source_sq = jnp.zeros(site, jnp.float32)
    for part in (RE, IM):
        for spin in range(4):
            for colour in range(3):
                value = source[part, spin, colour]
                source_sq = source_sq + value * value

    def slice_sums(value, time):
        sums = jnp.broadcast_to(jnp.sum(value, axis=1, keepdims=True), (SUB, LANE))
        return jnp.sum(jnp.where(time == lane8, sums, 0.0), axis=0, keepdims=True)

    stat_send[1:2] = slice_sums(source_sq[0], coord[0][0]) + slice_sums(source_sq[1], coord[0][1])

    local = project(x, 0, 1)
    ahead_half = [
        [jnp.where(coord[0] == BLOCK - 1, 0.0, cyclic(local[part][c], 0, -1, early)) for c in range(3)]
        for part in (RE, IM)
    ]
    for a in range(3):
        ahead = link_row(links, 0, a, ahead_half)
        behind = tuple(
            jnp.where(coord[0] == 0, 0.0, cyclic(behind_store[0, part, a], 0, 1, early)) for part in (RE, IM)
        )
        add_hops(acc, 0, a, ahead, behind)

    for mu in (1, 2):
        faces_wait(0, mu)
        arrived = unpack(recv_buf.at[mu * 2], mu, BLOCK - 1)
        local = project(x, mu, 1)
        ahead_half = [
            [
                jnp.where(coord[mu] == BLOCK - 1, arrived[part][c], cyclic(local[part][c], mu, -1, early))
                for c in range(3)
            ]
            for part in (RE, IM)
        ]
        below = unpack(recv_buf.at[mu * 2 + 1], mu, 0)
        for a in range(3):
            ahead = link_row(links, mu, a, ahead_half)
            behind = tuple(
                jnp.where(coord[mu] == 0, below[part][a], cyclic(behind_store[mu, part, a], mu, 1, early))
                for part in (RE, IM)
            )
            add_hops(acc, mu, a, ahead, behind)

    for part in (RE, IM):
        for spin in range(4):
            rest[part, spin] += 0.5 * acc[part, spin]
            corr[part, spin] = jnp.zeros_like(corr[part, spin])

    def block_sums(values):
        packed = None
        for index, value in enumerate(values):
            total = jnp.sum(value, axis=0, keepdims=True)
            total = jnp.broadcast_to(total, (SUB, LANE))
            packed = total if packed is None else jnp.where(row8 == index, total, packed)
        place = lane8 % BLOCK
        total = None
        for offset in range(1 - BLOCK, BLOCK):
            moved = [turn(packed, start - offset, 1) for start in range(0, LANE, LX)]
            while len(moved) > 1:
                moved = [p + q for p, q in zip(moved[::2], moved[1::2])]
            part = moved[0]
            if offset:
                part = jnp.where((place + offset >= 0) & (place + offset < BLOCK), part, 0.0)
            total = part if total is None else total + part
        packed = total
        return [jnp.broadcast_to(packed[i : i + 1], (SUB, LANE)) for i in range(len(values))]

    def store_halves(origin):
        for mu in (3, 2, 1, 0):
            for index, s in enumerate((1, -1)):
                half = project(origin, mu, s)
                for part in (RE, IM):
                    for colour in range(3):
                        moved = cyclic(half[part][colour], mu, -s, early)
                        for spin in range(2):
                            halves[index, mu, part, spin, colour] = moved[spin]

    def site_apply(origin, target):
        for tile in range(2):
            def emit(part, spin, colour, value):
                target[part, spin, colour, tile] = value

            block_site_term(
                lambda chirality, row: clover[chirality, RE, row, row, tile],
                lambda chirality, low, high: (
                    clover[chirality, RE, low, high, tile],
                    twist[chirality, PAIRS[low, high], 0, tile],
                    twist[chirality, PAIRS[low, high], 1, tile],
                ),
                lambda part, spin, colour: origin[part, spin, colour, tile],
                emit,
            )

    def gather_hop(total, mu, index, got):
        for part in (RE, IM):
            for spin in range(2):
                total[part, spin] = total[part, spin] + got[spin][part]
                sign, from_part, from_spin = PAIR_H[mu][(spin, part)]
                total[part, 2 + spin] = signed_add(
                    total[part, 2 + spin], sign if index else -sign, got[from_spin][from_part]
                )

    def add_inner_hops(target):
        for tile in range(2):
            total = {
                (row, part, spin): target[part, spin, row, tile]
                for row in range(3) for part in (RE, IM) for spin in range(4)
            }
            for mu in range(4):
                for index in range(2):
                    vectors = []
                    for spin in range(2):
                        re, im = ([halves[index, mu, part, spin, c, tile] for c in range(3)] for part in (RE, IM))
                        vectors.append((re, im, [r + i for r, i in zip(re, im)]))
                    for row in range(3):
                        weights = [[inner[index, mu, form, row, col, tile] for col in range(3)] for form in range(3)]
                        got = [three_products(*weights, *vector) for vector in vectors]
                        part_total = {(p, sp): total[row, p, sp] for p in (RE, IM) for sp in range(4)}
                        gather_hop(part_total, mu, index, got)
                        for (p, sp), value in part_total.items():
                            total[row, p, sp] = value
            for (row, part, spin), value in total.items():
                target[part, spin, row, tile] = value

    def time_faces(turn_index):
        later, sooner = [], []
        for j in range(3):
            packed = recv_buf[turn_index * 6, j]
            moved = turn(packed, BLOCK, 1)
            later += [moved[0], packed[0], moved[1], packed[1]]
            packed = recv_buf[turn_index * 6 + 1, j]
            moved = turn(packed, BLOCK, 1)
            sooner += [packed[0], moved[0], packed[1], moved[1]]
        hops = {}
        for spin in range(2):
            for a in range(3):
                ahead = [None, None]
                for c in range(3):
                    u_re, u_im = links[0, RE, a, c, 1], links[0, IM, a, c, 1]
                    h_re, h_im = later[3 * spin + c], later[6 + 3 * spin + c]
                    terms = u_re * h_re - u_im * h_im, u_re * h_im + u_im * h_re
                    ahead = [t if old is None else old + t for old, t in zip(ahead, terms)]
                for part in (RE, IM):
                    behind = 0.5 * sooner[6 * part + 3 * spin + a]
                    hops[part, spin, a] = jnp.where(early8, behind, 0.5 * ahead[part])
                    hops[part, 2 + spin, a] = jnp.where(early8, behind, -0.5 * ahead[part])
        return hops

    facing = jnp.where(early8, 1.0, -1.0).astype(jnp.float32)

    def add_edge_operator(hops):
        for key, value in hops.items():
            edge[key] = value
            rest[key + (0,)] += jnp.where(early8, value, 0.0)
            rest[key + (1,)] += jnp.where(early8, 0.0, value)
        for mu in (3, 2, 1):
            for index, s in enumerate((1, -1)):
                half = project(edge, mu, s)
                for part in (RE, IM):
                    for colour in range(3):
                        moved = cyclic(half[part][colour], mu, -s, early)
                        for spin in range(2):
                            edge_halves[index, mu - 1, part, spin, colour] = moved[spin]
        mixed = {
            (part, spin, colour): turn(hops[part, spin, colour] + facing * hops[part, 2 + spin, colour], BLOCK, 0)
            for part in (RE, IM) for spin in range(2) for colour in range(3)
        }

        def emit(part, spin, colour, value):
            edge_out[part, spin, colour] = value

        block_site_term(
            lambda chirality, row: edge_diagonal[chirality, row],
            lambda chirality, low, high: tuple(edge_pair[chirality, PAIRS[low, high], form] for form in range(3)),
            lambda part, spin, colour: edge[part, spin, colour],
            emit,
        )
        for row in range(3):
            total = {(part, spin): edge_out[part, spin, row] for part in (RE, IM) for spin in range(4)}
            for mu in range(1, 4):
                for index in range(2):
                    weights = [[edge_inner[index, mu - 1, form, row, col] for col in range(3)] for form in range(3)]
                    got = []
                    for spin in range(2):
                        re, im = ([edge_halves[index, mu - 1, part, spin, c] for c in range(3)] for part in (RE, IM))
                        got.append(three_products(*weights, re, im, [r + i for r, i in zip(re, im)]))
                    gather_hop(total, mu, index, got)
            weights = [[edge_time[form, row, col] for col in range(3)] for form in range(3)]
            for spin in range(2):
                re, im = ([mixed[part, spin, c] for c in range(3)] for part in (RE, IM))
                got = three_products(*weights, re, im, [r + i for r, i in zip(re, im)])
                for part in (RE, IM):
                    for lower, value in ((0, got[part]), (2, -facing * got[part])):
                        acc[part, lower + spin, row, 0] += jnp.where(early8, total[part, lower + spin], value)
                        acc[part, lower + spin, row, 1] += jnp.where(early8, value, total[part, lower + spin])

    def times_alpha(field, spin, colour, tile):
        re, im = field[RE, spin, colour, tile], field[IM, spin, colour, tile]
        a_re, a_im = alpha[0], alpha[1]
        return a_re * re - a_im * im, a_re * im + a_im * re

    def subtract_scaled(target, scaled, spin, colour, tile):
        for part in (RE, IM):
            target[part, spin, colour, tile] -= scaled[part]

    def next_margins():
        zero = jnp.zeros((SUB, LANE), jnp.float32)

        def one_tile(tile, carry):
            margin_re, margin_im, norm = carry
            for spin in range(4):
                for colour in range(3):
                    a_re, a_im = acc[RE, spin, colour, tile], acc[IM, spin, colour, tile]
                    r_re, r_im = rest[RE, spin, colour, tile], rest[IM, spin, colour, tile]
                    margin_re = margin_re + (a_re * r_re + a_im * r_im)
                    margin_im = margin_im + (a_re * r_im - a_im * r_re)
                    norm = norm + (a_re * a_re + a_im * a_im)
            return margin_re, margin_im, norm

        return one_tile(1, one_tile(0, (zero, zero, zero)))

    def set_alpha(margins):
        sum_re, sum_im, sum_norm = block_sums(margins)
        sum_norm = sum_norm + EPSILON
        alpha[0] = sum_re / sum_norm
        alpha[1] = sum_im / sum_norm

    def advance_correction(tile):
        for spin in range(4):
            for colour in range(3):
                scaled = times_alpha(rest, spin, colour, tile)
                for part in (RE, IM):
                    corr[part, spin, colour, tile] += scaled[part]

    def advance_rest(tile):
        for spin in range(4):
            for colour in range(3):
                subtract_scaled(rest, times_alpha(acc, spin, colour, tile), spin, colour, tile)

    def full_step(_, margins):
        set_alpha(margins)
        store_halves(acc)
        site_apply(acc, twice)
        add_inner_hops(twice)
        zero = jnp.zeros((SUB, LANE), jnp.float32)

        def one_tile(tile, carry):
            margin_re, margin_im, norm = carry
            advance_correction(tile)
            advance_rest(tile)
            for spin in range(4):
                for colour in range(3):
                    subtract_scaled(acc, times_alpha(twice, spin, colour, tile), spin, colour, tile)
                    a_re, a_im = acc[RE, spin, colour, tile], acc[IM, spin, colour, tile]
                    r_re, r_im = rest[RE, spin, colour, tile], rest[IM, spin, colour, tile]
                    margin_re = margin_re + (a_re * r_re + a_im * r_im)
                    margin_im = margin_im + (a_re * r_im - a_im * r_re)
                    norm = norm + (a_re * a_re + a_im * a_im)
            return margin_re, margin_im, norm

        return one_tile(1, one_tile(0, (zero, zero, zero)))

    store_halves(rest)
    site_apply(rest, acc)
    add_inner_hops(acc)
    faces_wait(0, 0)
    add_edge_operator(time_faces(0))
    margins = lax.fori_loop(0, MR_STEPS - 1, full_step, next_margins())
    def time_edge(field, tile, s):
        half = [
            [[signed_add(field[part, spin, c, tile], -s, field[part, 2 + spin, c, tile]) for c in range(3)] for spin in range(2)]
            for part in (RE, IM)
        ]
        if s > 0:
            return half
        rows = [[[None] * 3 for _ in range(2)] for _ in range(2)]
        for spin in range(2):
            for a in range(3):
                for c in range(3):
                    u_re, u_im = links[0, RE, c, a, tile], links[0, IM, c, a, tile]
                    h_re, h_im = half[RE][spin][c], half[IM][spin][c]
                    for part, term in ((RE, u_re * h_re + u_im * h_im), (IM, u_re * h_im - u_im * h_re)):
                        old = rows[part][spin][a]
                        rows[part][spin][a] = term if old is None else old + term
        return rows

    def send_time_edge(side, known, residual, factor):
        a_re, a_im = alpha[0], alpha[1]
        values = [[], []]
        for spin in range(2):
            for c in range(3):
                r_re, r_im = residual[RE][spin][c], residual[IM][spin][c]
                values[RE].append((known[RE][spin][c] + (a_re * r_re - a_im * r_im)) * factor)
                values[IM].append((known[IM][spin][c] + (a_re * r_im + a_im * r_re)) * factor)
        values = values[RE] + values[IM]
        for j in range(3):
            for tile in range(2):
                first, second = values[4 * j + 2 * tile], values[4 * j + 2 * tile + 1]
                if side:
                    first = turn(first, BLOCK, 0)
                else:
                    second = turn(second, BLOCK, 0)
                send_buf[6 + side, j, tile] = outer(first, second)

    known = [time_edge(corr, 0, 1), time_edge(corr, 1, -1)]
    residual = [time_edge(rest, 0, 1), time_edge(rest, 1, -1)]
    set_alpha(margins)
    send_time_edge(1, known[1], residual[1], last_t)
    send_time_edge(0, known[0], residual[0], first_t)
    start_wrapped_first(1)
    for tile in range(2):
        advance_correction(tile)
    for mu in (2, 1):
        prepare_ahead(1, corr, mu)
        face_copy(1, mu, 0).start()
        prepare_behind(1, corr, mu, False)
        face_copy(1, mu, 1).start()
    for tile in range(2):
        advance_rest(tile)
    for part in (RE, IM):
        for spin in range(4):
            update_out[part, spin] = x[part, spin] + corr[part, spin]
    zero_acc()
    for a, ahead, behind in x_hops(corr):
        ahead = tuple(jnp.where(high[3], v, 0.0) for v in ahead)
        behind = tuple(jnp.where(coord[3] % BLOCK == 0, v, 0.0) for v in behind)
        add_hops(acc, 3, a, ahead, behind)
    for mu in (1, 2):
        faces_wait(1, mu)
        arrived = unpack(recv_buf.at[6 + mu * 2], mu, BLOCK - 1)
        below = unpack(recv_buf.at[6 + mu * 2 + 1], mu, 0)
        for a in range(3):
            ahead = tuple(jnp.where(high[mu], v, 0.0) for v in link_row(links, mu, a, arrived))
            behind = tuple(jnp.where(coord[mu] == 0, below[part][a], 0.0) for part in (RE, IM))
            add_hops(acc, mu, a, ahead, behind)
    middle_sq = edge_sq = jnp.zeros((SUB, LANE), jnp.float32)
    for part in (RE, IM):
        for spin in range(4):
            for colour in range(3):
                value = rest[part, spin, colour] + 0.5 * acc[part, spin, colour]
                edge[part, spin, colour] = outer(value[0], value[1])
                value = outer(value[1], value[0])
                middle_sq = middle_sq + value * value
    stat_send[0:1] = slice_sums(middle_sq, jnp.where(early8, 2, 1))
    faces_wait(1, 0)
    for key, value in time_faces(1).items():
        value = edge[key] + value
        edge_sq = edge_sq + value * value
    stat_send[0:1] += slice_sums(edge_sq, jnp.where(early8, 0, BLOCK - 1))

    stat_copies = [
        pltpu.make_async_remote_copy(
            src_ref=stat_send,
            dst_ref=stat_recv.at[index - 1],
            send_sem=stat_send_sem,
            recv_sem=stat_recv_sem,
            device_id=peer(index),
            device_id_type=pl.DeviceIdType.MESH,
        )
        for index in sorted(range(1, group), key=lambda i: -spread(i))
    ]
    for copy in stat_copies:
        copy.start()
    pltpu.make_async_copy(send_buf, send_buf, send_sem).wait()
    pl.when(relays)(lambda: forward_copy().wait_send())
    stats = stat_send[...]
    pltpu.make_async_copy(stat_recv, stat_recv, stat_recv_sem).wait()
    for index in range(1, group):
        stats = stats + stat_recv[index - 1]
    profile_out[...] = (stats[0:1] / stats[1:2])[0, 0 : profile_out.shape[0]]
    pltpu.make_async_copy(stat_recv, stat_recv, stat_send_sem).wait()


def finish(held, ratio, update, profile, sems):
    stores = [pltpu.make_async_copy(held, update, sems.at[0]), pltpu.make_async_copy(ratio, profile, sems.at[1])]
    for store in stores:
        store.start()
    for store in stores:
        store.wait()


in_hbm = functools.partial(pltpu.with_memory_space_constraint, memory_space=pltpu.HBM)
in_vmem = functools.partial(pltpu.with_memory_space_constraint, memory_space=pltpu.VMEM)


def solution(mesh):
    sizes = tuple(mesh.shape[axis] for axis in AXES)
    group = mesh.shape["gz"] * mesh.shape["gy"]

    def local(source, start_guess, gauge_links, clover):
        times, depth, flat = source.shape[3:]
        assert sizes[0] > 1 and sizes[1] % 2 == 0
        assert times == depth == BLOCK and flat == LANE == BLOCK * LX
        tiles = (times * depth // SUB, SUB, LANE)
        spinor = source.shape[:3] + tiles
        gauge = gauge_links.shape[:4] + tiles
        site = clover.shape[:4] + tiles
        face = (12, 3) + tiles
        f32 = jnp.float32
        update, profile = pl.pallas_call(
            functools.partial(kernel, sizes),
            out_shape=(pltpu.VMEM(spinor, f32), pltpu.VMEM((times,), f32)),
            in_specs=[pl.BlockSpec(memory_space=pltpu.HBM)] * 4,
            out_specs=(pl.BlockSpec(memory_space=pltpu.VMEM),) * 2,
            scratch_shapes=[
                pltpu.VMEM(spinor, f32),
                pltpu.VMEM(spinor, f32),
                pltpu.VMEM(gauge, f32),
                pltpu.VMEM(site, f32),
                pltpu.VMEM((2, 4, 3, 3, 3) + tiles, f32),
                pltpu.VMEM((2, len(PAIRS), 2) + tiles, f32),
                pltpu.VMEM(spinor, f32),
                pltpu.VMEM(spinor, f32),
                pltpu.VMEM(spinor, f32),
                pltpu.VMEM(spinor, f32),
                pltpu.VMEM((2, SUB, LANE), f32),
                pltpu.VMEM((2, 4, 2, 2, 3) + tiles, f32),
                pltpu.VMEM((2, 4, 3, SUB, LANE), f32),
                pltpu.VMEM((2, 4, 3, SUB, LANE), f32),
                pltpu.VMEM((2, 3, 2, 2, 3, SUB, LANE), f32),
                pltpu.VMEM((2, 3, 3, 3, 3, SUB, LANE), f32),
                pltpu.VMEM((3, 3, 3, SUB, LANE), f32),
                pltpu.VMEM((2, 6, SUB, LANE), f32),
                pltpu.VMEM((2, len(PAIRS), 3, SUB, LANE), f32),
                pltpu.VMEM((3, 2, 3, 2) + tiles, f32),
                pltpu.VMEM(face, f32),
                pltpu.VMEM(face, f32),
                pltpu.VMEM(face[1:], f32),
                pltpu.VMEM((2, LANE), f32),
                pltpu.VMEM((group - 1, 2, LANE), f32),
                pltpu.SemaphoreType.DMA((7,)),
                pltpu.SemaphoreType.DMA,
                pltpu.SemaphoreType.DMA((6,)),
                pltpu.SemaphoreType.DMA((2,)),
                pltpu.SemaphoreType.DMA,
                pltpu.SemaphoreType.DMA,
            ],
            compiler_params=pltpu.CompilerParams(
                collective_id=0, has_side_effects=True, vmem_limit_bytes=VMEM_LIMIT,
            ),
        )(
            in_hbm(start_guess.reshape(spinor)),
            in_hbm(source.reshape(spinor)),
            in_hbm(gauge_links.reshape(gauge)),
            in_hbm(clover.reshape(site)),
        )
        update, profile = pl.pallas_call(
            finish,
            out_shape=(jax.ShapeDtypeStruct(spinor, f32), jax.ShapeDtypeStruct((times,), f32)),
            in_specs=[pl.BlockSpec(memory_space=pltpu.VMEM)] * 2,
            out_specs=(pl.BlockSpec(memory_space=pl.ANY),) * 2,
            scratch_shapes=[pltpu.SemaphoreType.DMA((2,))],
        )(
            in_vmem(update),
            in_vmem(profile),
        )
        return update.reshape(source.shape), profile

    spinor_spec = P(None, None, None, "ta", "gz", "gy")
    matrix_spec = P(None, None, None, None, "ta", "gz", "gy")
    return jax.shard_map(
        local,
        mesh=mesh,
        in_specs=(spinor_spec, spinor_spec, matrix_spec, matrix_spec),
        out_specs=(spinor_spec, P("ta")),
        check_vma=False,
    )
```

```python
import functools

import jax
import jax.numpy as jnp
from jax import lax
from jax.experimental import pallas as pl
from jax.experimental.pallas import tpu as pltpu
from jax.sharding import PartitionSpec as P

LX = 32
BLOCK = 4
MR_STEPS = 4
EPSILON = 1e-6
AXES = ("ta", "gz", "gy")
RE, IM = 0, 1
SUB, LANE = 8, 128
VMEM_LIMIT = 24 * 2**20

PAIR = (
    {(0, RE): (1, RE, 0), (0, IM): (1, IM, 0), (1, RE): (1, RE, 1), (1, IM): (1, IM, 1)},
    {(0, RE): (1, IM, 0), (0, IM): (-1, RE, 0), (1, RE): (-1, IM, 1), (1, IM): (1, RE, 1)},
    {(0, RE): (-1, RE, 1), (0, IM): (-1, IM, 1), (1, RE): (1, RE, 0), (1, IM): (1, IM, 0)},
    {(0, RE): (1, IM, 1), (0, IM): (-1, RE, 1), (1, RE): (1, IM, 0), (1, IM): (-1, RE, 0)},
)
PAIR_H = (
    {(0, RE): (1, RE, 0), (0, IM): (1, IM, 0), (1, RE): (1, RE, 1), (1, IM): (1, IM, 1)},
    {(0, RE): (-1, IM, 0), (0, IM): (1, RE, 0), (1, RE): (1, IM, 1), (1, IM): (-1, RE, 1)},
    {(0, RE): (1, RE, 1), (0, IM): (1, IM, 1), (1, RE): (-1, RE, 0), (1, IM): (-1, IM, 0)},
    {(0, RE): (-1, IM, 1), (0, IM): (1, RE, 1), (1, RE): (-1, IM, 0), (1, IM): (1, RE, 0)},
)


PAIRS = {pair: i for i, pair in enumerate((low, high) for high in range(6) for low in range(high))}


def signed_add(base, sign, value):
    return base + value if sign > 0 else base - value


def project(field, mu, s):
    parts = ([], [])
    for part in (RE, IM):
        for colour in range(3):
            spins = []
            for spin in range(2):
                sign, from_part, from_spin = PAIR[mu][(spin, part)]
                spins.append(
                    signed_add(field[part, spin, colour], -s * sign, field[from_part, 2 + from_spin, colour])
                )
            parts[part].append(jnp.stack(spins))
    return parts


def link_row(links, mu, row, half):
    re = im = None
    for col in range(3):
        u_re, u_im = links[mu, RE, row, col][None], links[mu, IM, row, col][None]
        h_re, h_im = half[RE][col], half[IM][col]
        t_re = u_re * h_re - u_im * h_im
        t_im = u_re * h_im + u_im * h_re
        re, im = (t_re, t_im) if re is None else (re + t_re, im + t_im)
    return re, im


def adjoint_row(links, mu, row, half):
    re = im = None
    for col in range(3):
        u_re, u_im = links[mu, RE, col, row][None], links[mu, IM, col, row][None]
        h_re, h_im = half[RE][col], half[IM][col]
        t_re = u_re * h_re + u_im * h_im
        t_im = u_re * h_im - u_im * h_re
        re, im = (t_re, t_im) if re is None else (re + t_re, im + t_im)
    return re, im


def add_hops(acc, mu, colour, ahead, behind):
    difference = tuple(b - a for a, b in zip(ahead, behind))
    for part in (RE, IM):
        acc[part, 0:2, colour] += ahead[part] + behind[part]
        for spin in range(2):
            sign, from_part, from_spin = PAIR_H[mu][(spin, part)]
            old = acc[part, 2 + spin, colour]
            acc[part, 2 + spin, colour] = signed_add(old, sign, difference[from_part][from_spin])


def site_term(clover, field, emit):
    def pair(part, index):
        return jnp.stack([field[part, index // 3, index % 3], field[part, 2 + index // 3, index % 3]])

    vec = [[pair(part, j) for j in range(6)] for part in (RE, IM)]
    for row in range(6):
        diagonal = clover[:, RE, row, row]
        re, im = diagonal * vec[RE][row], diagonal * vec[IM][row]
        for col in range(6):
            if col == row:
                continue
            low, high = min(row, col), max(row, col)
            m_re, m_im = clover[:, RE, low, high], clover[:, IM, low, high]
            if row < col:
                re = re + m_re * vec[RE][col] - m_im * vec[IM][col]
                im = im + m_re * vec[IM][col] + m_im * vec[RE][col]
            else:
                re = re + m_re * vec[RE][col] + m_im * vec[IM][col]
                im = im + m_re * vec[IM][col] - m_im * vec[RE][col]
        for chirality in range(2):
            emit(RE, 2 * chirality + row // 3, row % 3, re[chirality])
            emit(IM, 2 * chirality + row // 3, row % 3, im[chirality])


def three_products(first, second, third, re, im, both):
    def dot(weights, values):
        total = None
        for weight, value in zip(weights, values):
            total = weight * value if total is None else total + weight * value
        return total

    shared = dot(first, both)
    return shared - dot(third, im), shared + dot(second, re)


def block_site_term(diagonals, triples, field, emit):
    for chirality in range(2):
        vec = [[field(part, 2 * chirality + j // 3, j % 3) for j in range(6)] for part in (RE, IM)]
        both = [r + i for r, i in zip(*vec)]
        for row in range(6):
            diagonal = diagonals(chirality, row)
            re, im, shared = diagonal * vec[RE][row], diagonal * vec[IM][row], None
            for col in range(6):
                if col == row:
                    continue
                low, high = min(row, col), max(row, col)
                real, less, more = triples(chirality, low, high)
                term = real * both[col]
                shared = term if shared is None else shared + term
                if row < col:
                    re, im = re - more * vec[IM][col], im + less * vec[RE][col]
                else:
                    re, im = re + less * vec[IM][col], im - more * vec[RE][col]
            emit(RE, 2 * chirality + row // 3, row % 3, re + shared)
            emit(IM, 2 * chirality + row // 3, row % 3, im + shared)


def swap_halves(value):
    axis = value.ndim - 3
    return jnp.concatenate(
        [lax.slice_in_dim(value, 1, 2, axis=axis), lax.slice_in_dim(value, 0, 1, axis=axis)], axis=axis
    )


def turn(value, shift, axis):
    shift = shift % value.shape[axis]
    return pltpu.roll(value, shift, axis) if shift else value


def cyclic(value, mu, units, early):
    axis = value.ndim - 2
    if mu == 3:
        return turn(value, units, axis + 1)
    if mu == 2:
        return turn(value, units * LX, axis + 1)
    if mu == 1:
        return turn(value, units, axis)
    units = units % BLOCK
    if units == 0:
        return value
    if units == 2:
        return swap_halves(value)
    rolled = turn(value, BLOCK, axis)
    swapped = swap_halves(rolled)
    return jnp.where(early, swapped, rolled) if units == 1 else jnp.where(early, rolled, swapped)


def kernel(
    sizes, x_in, source_in, links_in, clover_in, update_out, profile_out,
    x, source, links, clover, inner, twist, rest, corr, acc, twice, alpha, halves, edge, edge_out, edge_halves,
    edge_inner, edge_time, edge_diagonal, edge_pair, behind_store,
    send_buf, recv_buf, relay_buf, stat_send, stat_recv,
    in_sem, send_sem, recv_sem, relay_sem, stat_send_sem, stat_recv_sem,
):
    count = {axis: size for axis, size in zip(AXES, sizes)}
    group = count["gz"] * count["gy"]
    me = {axis: lax.axis_index(axis) for axis in AXES}

    def peer(index):
        return {
            "gz": lax.rem(me["gz"] + index // count["gy"], count["gz"]),
            "gy": lax.rem(me["gy"] + index % count["gy"], count["gy"]),
        }

    def distance(index):
        depth, width = index // count["gy"], index % count["gy"]
        return min(depth, count["gz"] - depth) + min(width, count["gy"] - width)

    def spread(index):
        depth = index // count["gy"]
        return 2 * min(depth, count["gz"] - depth) + 3 * (index % count["gy"] != 0)

    def beside(axis, step):
        return {axis: lax.rem(me[axis] + step + count[axis], count[axis])}

    barrier = pltpu.get_barrier_semaphore()
    opens, closes = me["ta"] == 0, me["ta"] == count["ta"] - 1
    outer_core = lax.rem(me["gz"], 2)
    through = me["gz"] + jnp.where(jnp.logical_and(closes, outer_core == 0), 1, 0)
    for target in ({"gz": through, **beside("ta", 1)}, beside("ta", -1)):
        pl.semaphore_signal(barrier, inc=1, device_id=target, device_id_type=pl.DeviceIdType.MESH)
    loads = [pltpu.make_async_copy(x_in, x, in_sem.at[0])]
    loads += [pltpu.make_async_copy(links_in.at[mu], links.at[mu], in_sem.at[1 + mu]) for mu in range(4)]
    loads.append(pltpu.make_async_copy(clover_in, clover, in_sem.at[5]))
    loads.append(pltpu.make_async_copy(source_in, source, in_sem.at[6]))
    for load in loads:
        load.start()

    greeted = [index for index in range(1, group) if distance(index) == 1 or distance(index) > 3]
    for index in greeted:
        pl.semaphore_signal(barrier, inc=1, device_id=peer(index), device_id_type=pl.DeviceIdType.MESH)

    site = (2, SUB, LANE)
    row = lax.broadcasted_iota(jnp.int32, site, 1)
    lane = lax.broadcasted_iota(jnp.int32, site, 2)
    coord = (
        lax.broadcasted_iota(jnp.int32, site, 0) * 2 + row // BLOCK,
        row % BLOCK,
        lane // LX,
        lane % LX,
    )
    early = row < BLOCK
    row8 = lax.broadcasted_iota(jnp.int32, (SUB, LANE), 0)
    lane8 = lax.broadcasted_iota(jnp.int32, (SUB, LANE), 1)
    early8 = row8 < BLOCK
    high = tuple(c % BLOCK == BLOCK - 1 for c in coord)

    def x_neighbour(value, step):
        axis = value.ndim - 1
        if step > 0:
            return jnp.where(coord[3] == LX - 1, turn(value, LX - 1, axis), turn(value, -1, axis))
        return jnp.where(coord[3] == 0, turn(value, 1 - LX, axis), turn(value, 1, axis))

    def flat(half):
        return [half[part][colour][spin] for part in (RE, IM) for spin in range(2) for colour in range(3)]

    def pack(half, mu, edge, store, factor=None):
        values = flat(half)
        for j in range(3):
            packed = cyclic(values[4 * j], mu, -edge, early)
            for k in range(1, BLOCK):
                packed = jnp.where(coord[mu] == k, cyclic(values[4 * j + k], mu, k - edge, early), packed)
            store[j] = packed if factor is None else packed * factor

    def unpack(store, mu, edge):
        values = []
        for j in range(3):
            packed = store[j]
            values += [cyclic(packed, mu, edge - k, early) for k in range(BLOCK)]
        return [[jnp.stack([values[6 * p + c], values[6 * p + 3 + c]]) for c in range(3)] for p in (RE, IM)]

    def face_copy(turn_index, mu, side):
        slot = turn_index * 6 + mu * 2 + side
        return pltpu.make_async_remote_copy(
            src_ref=send_buf.at[slot],
            dst_ref=recv_buf.at[slot],
            send_sem=send_sem,
            recv_sem=recv_sem.at[turn_index * 3 + mu],
            device_id=beside(AXES[mu], -1 if side == 0 else 1),
            device_id_type=pl.DeviceIdType.MESH,
        )

    def faces_wait(turn_index, mu):
        pair = recv_buf.at[pl.ds(turn_index * 6 + mu * 2, 2)]
        pltpu.make_async_copy(pair, pair, recv_sem.at[turn_index * 3 + mu]).wait()

    def relay_copy():
        return pltpu.make_async_remote_copy(
            src_ref=send_buf.at[0],
            dst_ref=relay_buf,
            send_sem=send_sem,
            recv_sem=relay_sem.at[0],
            device_id={"gz": me["gz"] + 1 - 2 * outer_core},
            device_id_type=pl.DeviceIdType.MESH,
        )

    def forward_copy():
        return pltpu.make_async_remote_copy(
            src_ref=relay_buf,
            dst_ref=recv_buf.at[0],
            send_sem=relay_sem.at[1],
            recv_sem=recv_sem.at[0],
            device_id={"gz": me["gz"] + 1 - 2 * outer_core, **beside("ta", -1)},
            device_id_type=pl.DeviceIdType.MESH,
        )

    relays = jnp.logical_and(opens, outer_core == 1)

    def start_wrapped_first(turn_index):
        last = me["ta"] == count["ta"] - 1

        @pl.when(last)
        def _():
            face_copy(turn_index, 0, 1).start()
            face_copy(turn_index, 0, 0).start()

        @pl.when(jnp.logical_not(last))
        def _():
            face_copy(turn_index, 0, 0).start()
            face_copy(turn_index, 0, 1).start()

    first_t = jnp.where(me["ta"] == 0, -1.0, 1.0).astype(jnp.float32)
    last_t = jnp.where(me["ta"] == count["ta"] - 1, -1.0, 1.0).astype(jnp.float32)

    def prepare_ahead(turn_index, field, mu):
        pack(project(field, mu, 1), mu, 0, send_buf.at[turn_index * 6 + mu * 2], first_t if mu == 0 else None)

    def prepare_behind(turn_index, field, mu, keep):
        half = project(field, mu, -1)
        rows = [adjoint_row(links, mu, a, half) for a in range(3)]
        behind = [[rows[a][part] for a in range(3)] for part in (RE, IM)]
        pack(behind, mu, BLOCK - 1, send_buf.at[turn_index * 6 + mu * 2 + 1], last_t if mu == 0 else None)
        if keep:
            for part in (RE, IM):
                for a in range(3):
                    behind_store[mu, part, a] = behind[part][a]

    follows = jnp.logical_not(opens)

    def enter():
        pl.semaphore_wait(barrier, len(greeted) + 2 + jnp.where(opens, 2 * outer_core - 1, 0))

    loads[0].wait()
    prepare_ahead(0, x, 0)
    loads[1].wait()
    prepare_behind(0, x, 0, True)
    prepare_ahead(0, x, 2)

    @pl.when(follows)
    def _():
        enter()
        start_wrapped_first(0)
        face_copy(0, 2, 0).start()

    loads[3].wait()
    prepare_behind(0, x, 2, True)
    pl.when(follows)(lambda: face_copy(0, 2, 1).start())
    prepare_ahead(0, x, 1)
    pl.when(follows)(lambda: face_copy(0, 1, 0).start())
    loads[2].wait()
    prepare_behind(0, x, 1, True)
    pl.when(follows)(lambda: face_copy(0, 1, 1).start())

    @pl.when(opens)
    def _():
        enter()

        @pl.when(outer_core == 0)
        def _():
            relay_copy().start()

        @pl.when(outer_core == 1)
        def _():
            relay_copy().wait_recv()
            forward_copy().start()
            face_copy(0, 0, 0).start()

        for mu, side in ((0, 1), (1, 0), (1, 1), (2, 0), (2, 1)):
            face_copy(0, mu, side).start()

    def zero_acc():
        acc[...] = jnp.zeros_like(acc)

    zero_acc()
    loads[4].wait()

    def x_hops(field):
        ahead_half = [[x_neighbour(v, 1) for v in values] for values in project(field, 3, 1)]
        behind_half = project(field, 3, -1)
        for a in range(3):
            ahead = link_row(links, 3, a, ahead_half)
            behind = tuple(x_neighbour(v, -1) for v in adjoint_row(links, 3, a, behind_half))
            yield a, ahead, behind

    for a, ahead, behind in x_hops(x):
        add_hops(acc, 3, a, ahead, behind)

    for mu in range(4):
        factor = jnp.where(high[mu], 0.0, -0.5).astype(jnp.float32)
        for a in range(3):
            for b in range(3):
                re, im = links[mu, RE, a, b] * factor, links[mu, IM, a, b] * factor
                inner[0, mu, 0, a, b] = re
                inner[0, mu, 1, a, b] = im - re
                inner[0, mu, 2, a, b] = im + re
                re, im = cyclic(re, mu, 1, early), cyclic(im, mu, 1, early)
                inner[1, mu, 0, b, a] = re
                inner[1, mu, 1, b, a] = -im - re
                inner[1, mu, 2, b, a] = re - im

    loads[5].wait()
    for chirality in range(2):
        for (low, high_row), index in PAIRS.items():
            re, im = clover[chirality, RE, low, high_row], clover[chirality, IM, low, high_row]
            twist[chirality, index, 0] = im - re
            twist[chirality, index, 1] = im + re
    def outer(first, second):
        return jnp.where(early8, first, second)

    for index in range(2):
        for mu in range(1, 4):
            for form in range(3):
                for a in range(3):
                    for b in range(3):
                        edge_inner[index, mu - 1, form, a, b] = outer(*(inner[index, mu, form, a, b, i] for i in range(2)))
    for form in range(3):
        for a in range(3):
            for b in range(3):
                edge_time[form, a, b] = outer(inner[0, 0, form, a, b, 1], inner[1, 0, form, a, b, 0])
    for chirality in range(2):
        for a in range(6):
            edge_diagonal[chirality, a] = outer(*(clover[chirality, RE, a, a, i] for i in range(2)))
        for (low, high_row), index in PAIRS.items():
            edge_pair[chirality, index, 0] = outer(*(clover[chirality, RE, low, high_row, i] for i in range(2)))
            for form in range(2):
                edge_pair[chirality, index, 1 + form] = outer(*(twist[chirality, index, form, i] for i in range(2)))
    loads[6].wait()

    def emit_rest(part, spin, colour, value):
        rest[part, spin, colour] = source[part, spin, colour] - value

    site_term(clover, x, emit_rest)
    source_sq = jnp.zeros(site, jnp.float32)
    for part in (RE, IM):
        for spin in range(4):
            for colour in range(3):
                value = source[part, spin, colour]
                source_sq = source_sq + value * value

    def slice_sums(value, time):
        sums = jnp.broadcast_to(jnp.sum(value, axis=1, keepdims=True), (SUB, LANE))
        return jnp.sum(jnp.where(time == lane8, sums, 0.0), axis=0, keepdims=True)

    stat_send[1:2] = slice_sums(source_sq[0], coord[0][0]) + slice_sums(source_sq[1], coord[0][1])

    local = project(x, 0, 1)
    ahead_half = [
        [jnp.where(coord[0] == BLOCK - 1, 0.0, cyclic(local[part][c], 0, -1, early)) for c in range(3)]
        for part in (RE, IM)
    ]
    for a in range(3):
        ahead = link_row(links, 0, a, ahead_half)
        behind = tuple(
            jnp.where(coord[0] == 0, 0.0, cyclic(behind_store[0, part, a], 0, 1, early)) for part in (RE, IM)
        )
        add_hops(acc, 0, a, ahead, behind)

    for mu in (1, 2):
        faces_wait(0, mu)
        arrived = unpack(recv_buf.at[mu * 2], mu, BLOCK - 1)
        local = project(x, mu, 1)
        ahead_half = [
            [
                jnp.where(coord[mu] == BLOCK - 1, arrived[part][c], cyclic(local[part][c], mu, -1, early))
                for c in range(3)
            ]
            for part in (RE, IM)
        ]
        below = unpack(recv_buf.at[mu * 2 + 1], mu, 0)
        for a in range(3):
            ahead = link_row(links, mu, a, ahead_half)
            behind = tuple(
                jnp.where(coord[mu] == 0, below[part][a], cyclic(behind_store[mu, part, a], mu, 1, early))
                for part in (RE, IM)
            )
            add_hops(acc, mu, a, ahead, behind)

    for part in (RE, IM):
        for spin in range(4):
            rest[part, spin] += 0.5 * acc[part, spin]
            corr[part, spin] = jnp.zeros_like(corr[part, spin])

    def block_sums(values):
        packed = None
        for index, value in enumerate(values):
            total = jnp.sum(value, axis=0, keepdims=True)
            total = jnp.broadcast_to(total, (SUB, LANE))
            packed = total if packed is None else jnp.where(row8 == index, total, packed)
        place = lane8 % BLOCK
        total = None
        for offset in range(1 - BLOCK, BLOCK):
            moved = [turn(packed, start - offset, 1) for start in range(0, LANE, LX)]
            while len(moved) > 1:
                moved = [p + q for p, q in zip(moved[::2], moved[1::2])]
            part = moved[0]
            if offset:
                part = jnp.where((place + offset >= 0) & (place + offset < BLOCK), part, 0.0)
            total = part if total is None else total + part
        packed = total
        return [jnp.broadcast_to(packed[i : i + 1], (SUB, LANE)) for i in range(len(values))]

    def store_halves(origin):
        for mu in (3, 2, 1, 0):
            for index, s in enumerate((1, -1)):
                half = project(origin, mu, s)
                for part in (RE, IM):
                    for colour in range(3):
                        moved = cyclic(half[part][colour], mu, -s, early)
                        for spin in range(2):
                            halves[index, mu, part, spin, colour] = moved[spin]

    def site_apply(origin, target):
        for tile in range(2):
            def emit(part, spin, colour, value):
                target[part, spin, colour, tile] = value

            block_site_term(
                lambda chirality, row: clover[chirality, RE, row, row, tile],
                lambda chirality, low, high: (
                    clover[chirality, RE, low, high, tile],
                    twist[chirality, PAIRS[low, high], 0, tile],
                    twist[chirality, PAIRS[low, high], 1, tile],
                ),
                lambda part, spin, colour: origin[part, spin, colour, tile],
                emit,
            )

    def gather_hop(total, mu, index, got):
        for part in (RE, IM):
            for spin in range(2):
                total[part, spin] = total[part, spin] + got[spin][part]
                sign, from_part, from_spin = PAIR_H[mu][(spin, part)]
                total[part, 2 + spin] = signed_add(
                    total[part, 2 + spin], sign if index else -sign, got[from_spin][from_part]
                )

    def add_inner_hops(target):
        for tile in range(2):
            total = {
                (row, part, spin): target[part, spin, row, tile]
                for row in range(3) for part in (RE, IM) for spin in range(4)
            }
            for mu in range(4):
                for index in range(2):
                    vectors = []
                    for spin in range(2):
                        re, im = ([halves[index, mu, part, spin, c, tile] for c in range(3)] for part in (RE, IM))
                        vectors.append((re, im, [r + i for r, i in zip(re, im)]))
                    for row in range(3):
                        weights = [[inner[index, mu, form, row, col, tile] for col in range(3)] for form in range(3)]
                        got = [three_products(*weights, *vector) for vector in vectors]
                        part_total = {(p, sp): total[row, p, sp] for p in (RE, IM) for sp in range(4)}
                        gather_hop(part_total, mu, index, got)
                        for (p, sp), value in part_total.items():
                            total[row, p, sp] = value
            for (row, part, spin), value in total.items():
                target[part, spin, row, tile] = value

    def time_faces(turn_index):
        later, sooner = [], []
        for j in range(3):
            packed = recv_buf[turn_index * 6, j]
            moved = turn(packed, BLOCK, 1)
            later += [moved[0], packed[0], moved[1], packed[1]]
            packed = recv_buf[turn_index * 6 + 1, j]
            moved = turn(packed, BLOCK, 1)
            sooner += [packed[0], moved[0], packed[1], moved[1]]
        hops = {}
        for spin in range(2):
            for a in range(3):
                ahead = [None, None]
                for c in range(3):
                    u_re, u_im = links[0, RE, a, c, 1], links[0, IM, a, c, 1]
                    h_re, h_im = later[3 * spin + c], later[6 + 3 * spin + c]
                    terms = u_re * h_re - u_im * h_im, u_re * h_im + u_im * h_re
                    ahead = [t if old is None else old + t for old, t in zip(ahead, terms)]
                for part in (RE, IM):
                    behind = 0.5 * sooner[6 * part + 3 * spin + a]
                    hops[part, spin, a] = jnp.where(early8, behind, 0.5 * ahead[part])
                    hops[part, 2 + spin, a] = jnp.where(early8, behind, -0.5 * ahead[part])
        return hops

    facing = jnp.where(early8, 1.0, -1.0).astype(jnp.float32)

    def add_edge_operator(hops):
        for key, value in hops.items():
            edge[key] = value
            rest[key + (0,)] += jnp.where(early8, value, 0.0)
            rest[key + (1,)] += jnp.where(early8, 0.0, value)
        for mu in (3, 2, 1):
            for index, s in enumerate((1, -1)):
                half = project(edge, mu, s)
                for part in (RE, IM):
                    for colour in range(3):
                        moved = cyclic(half[part][colour], mu, -s, early)
                        for spin in range(2):
                            edge_halves[index, mu - 1, part, spin, colour] = moved[spin]
        mixed = {
            (part, spin, colour): turn(hops[part, spin, colour] + facing * hops[part, 2 + spin, colour], BLOCK, 0)
            for part in (RE, IM) for spin in range(2) for colour in range(3)
        }

        def emit(part, spin, colour, value):
            edge_out[part, spin, colour] = value

        block_site_term(
            lambda chirality, row: edge_diagonal[chirality, row],
            lambda chirality, low, high: tuple(edge_pair[chirality, PAIRS[low, high], form] for form in range(3)),
            lambda part, spin, colour: edge[part, spin, colour],
            emit,
        )
        for row in range(3):
            total = {(part, spin): edge_out[part, spin, row] for part in (RE, IM) for spin in range(4)}
            for mu in range(1, 4):
                for index in range(2):
                    weights = [[edge_inner[index, mu - 1, form, row, col] for col in range(3)] for form in range(3)]
                    got = []
                    for spin in range(2):
                        re, im = ([edge_halves[index, mu - 1, part, spin, c] for c in range(3)] for part in (RE, IM))
                        got.append(three_products(*weights, re, im, [r + i for r, i in zip(re, im)]))
                    gather_hop(total, mu, index, got)
            weights = [[edge_time[form, row, col] for col in range(3)] for form in range(3)]
            for spin in range(2):
                re, im = ([mixed[part, spin, c] for c in range(3)] for part in (RE, IM))
                got = three_products(*weights, re, im, [r + i for r, i in zip(re, im)])
                for part in (RE, IM):
                    for lower, value in ((0, got[part]), (2, -facing * got[part])):
                        acc[part, lower + spin, row, 0] += jnp.where(early8, total[part, lower + spin], value)
                        acc[part, lower + spin, row, 1] += jnp.where(early8, value, total[part, lower + spin])

    def times_alpha(field, spin, colour, tile):
        re, im = field[RE, spin, colour, tile], field[IM, spin, colour, tile]
        a_re, a_im = alpha[0], alpha[1]
        return a_re * re - a_im * im, a_re * im + a_im * re

    def subtract_scaled(target, scaled, spin, colour, tile):
        for part in (RE, IM):
            target[part, spin, colour, tile] -= scaled[part]

    def next_margins():
        zero = jnp.zeros((SUB, LANE), jnp.float32)

        def one_tile(tile, carry):
            margin_re, margin_im, norm = carry
            for spin in range(4):
                for colour in range(3):
                    a_re, a_im = acc[RE, spin, colour, tile], acc[IM, spin, colour, tile]
                    r_re, r_im = rest[RE, spin, colour, tile], rest[IM, spin, colour, tile]
                    margin_re = margin_re + (a_re * r_re + a_im * r_im)
                    margin_im = margin_im + (a_re * r_im - a_im * r_re)
                    norm = norm + (a_re * a_re + a_im * a_im)
            return margin_re, margin_im, norm

        return one_tile(1, one_tile(0, (zero, zero, zero)))

    def set_alpha(margins):
        sum_re, sum_im, sum_norm = block_sums(margins)
        sum_norm = sum_norm + EPSILON
        alpha[0] = sum_re / sum_norm
        alpha[1] = sum_im / sum_norm

    def advance_correction(tile):
        for spin in range(4):
            for colour in range(3):
                scaled = times_alpha(rest, spin, colour, tile)
                for part in (RE, IM):
                    corr[part, spin, colour, tile] += scaled[part]

    def advance_rest(tile):
        for spin in range(4):
            for colour in range(3):
                subtract_scaled(rest, times_alpha(acc, spin, colour, tile), spin, colour, tile)

    def full_step(_, margins):
        set_alpha(margins)
        store_halves(acc)
        site_apply(acc, twice)
        add_inner_hops(twice)
        zero = jnp.zeros((SUB, LANE), jnp.float32)

        def one_tile(tile, carry):
            margin_re, margin_im, norm = carry
            advance_correction(tile)
            advance_rest(tile)
            for spin in range(4):
                for colour in range(3):
                    subtract_scaled(acc, times_alpha(twice, spin, colour, tile), spin, colour, tile)
                    a_re, a_im = acc[RE, spin, colour, tile], acc[IM, spin, colour, tile]
                    r_re, r_im = rest[RE, spin, colour, tile], rest[IM, spin, colour, tile]
                    margin_re = margin_re + (a_re * r_re + a_im * r_im)
                    margin_im = margin_im + (a_re * r_im - a_im * r_re)
                    norm = norm + (a_re * a_re + a_im * a_im)
            return margin_re, margin_im, norm

        return one_tile(1, one_tile(0, (zero, zero, zero)))

    store_halves(rest)
    site_apply(rest, acc)
    add_inner_hops(acc)
    faces_wait(0, 0)
    add_edge_operator(time_faces(0))
    margins = lax.fori_loop(0, MR_STEPS - 1, full_step, next_margins())
    def time_edge(field, tile, s):
        half = [
            [[signed_add(field[part, spin, c, tile], -s, field[part, 2 + spin, c, tile]) for c in range(3)] for spin in range(2)]
            for part in (RE, IM)
        ]
        if s > 0:
            return half
        rows = [[[None] * 3 for _ in range(2)] for _ in range(2)]
        for spin in range(2):
            for a in range(3):
                for c in range(3):
                    u_re, u_im = links[0, RE, c, a, tile], links[0, IM, c, a, tile]
                    h_re, h_im = half[RE][spin][c], half[IM][spin][c]
                    for part, term in ((RE, u_re * h_re + u_im * h_im), (IM, u_re * h_im - u_im * h_re)):
                        old = rows[part][spin][a]
                        rows[part][spin][a] = term if old is None else old + term
        return rows

    def send_time_edge(side, known, residual, factor):
        a_re, a_im = alpha[0], alpha[1]
        values = [[], []]
        for spin in range(2):
            for c in range(3):
                r_re, r_im = residual[RE][spin][c], residual[IM][spin][c]
                values[RE].append((known[RE][spin][c] + (a_re * r_re - a_im * r_im)) * factor)
                values[IM].append((known[IM][spin][c] + (a_re * r_im + a_im * r_re)) * factor)
        values = values[RE] + values[IM]
        for j in range(3):
            for tile in range(2):
                first, second = values[4 * j + 2 * tile], values[4 * j + 2 * tile + 1]
                if side:
                    first = turn(first, BLOCK, 0)
                else:
                    second = turn(second, BLOCK, 0)
                send_buf[6 + side, j, tile] = outer(first, second)

    known = [time_edge(corr, 0, 1), time_edge(corr, 1, -1)]
    residual = [time_edge(rest, 0, 1), time_edge(rest, 1, -1)]
    set_alpha(margins)
    send_time_edge(1, known[1], residual[1], last_t)
    send_time_edge(0, known[0], residual[0], first_t)
    start_wrapped_first(1)
    for tile in range(2):
        advance_correction(tile)
    for mu in (2, 1):
        prepare_ahead(1, corr, mu)
        face_copy(1, mu, 0).start()
        prepare_behind(1, corr, mu, False)
        face_copy(1, mu, 1).start()
    for tile in range(2):
        advance_rest(tile)
    for part in (RE, IM):
        for spin in range(4):
            update_out[part, spin] = x[part, spin] + corr[part, spin]
    zero_acc()
    for a, ahead, behind in x_hops(corr):
        ahead = tuple(jnp.where(high[3], v, 0.0) for v in ahead)
        behind = tuple(jnp.where(coord[3] % BLOCK == 0, v, 0.0) for v in behind)
        add_hops(acc, 3, a, ahead, behind)
    for mu in (1, 2):
        faces_wait(1, mu)
        arrived = unpack(recv_buf.at[6 + mu * 2], mu, BLOCK - 1)
        below = unpack(recv_buf.at[6 + mu * 2 + 1], mu, 0)
        for a in range(3):
            ahead = tuple(jnp.where(high[mu], v, 0.0) for v in link_row(links, mu, a, arrived))
            behind = tuple(jnp.where(coord[mu] == 0, below[part][a], 0.0) for part in (RE, IM))
            add_hops(acc, mu, a, ahead, behind)
    middle_sq = edge_sq = jnp.zeros((SUB, LANE), jnp.float32)
    for part in (RE, IM):
        for spin in range(4):
            for colour in range(3):
                value = rest[part, spin, colour] + 0.5 * acc[part, spin, colour]
                edge[part, spin, colour] = outer(value[0], value[1])
                value = outer(value[1], value[0])
                middle_sq = middle_sq + value * value
    stat_send[0:1] = slice_sums(middle_sq, jnp.where(early8, 2, 1))
    faces_wait(1, 0)
    for key, value in time_faces(1).items():
        value = edge[key] + value
        edge_sq = edge_sq + value * value
    stat_send[0:1] += slice_sums(edge_sq, jnp.where(early8, 0, BLOCK - 1))

    stat_copies = [
        pltpu.make_async_remote_copy(
            src_ref=stat_send,
            dst_ref=stat_recv.at[index - 1],
            send_sem=stat_send_sem,
            recv_sem=stat_recv_sem,
            device_id=peer(index),
            device_id_type=pl.DeviceIdType.MESH,
        )
        for index in sorted(range(1, group), key=lambda i: -spread(i))
    ]
    for copy in stat_copies:
        copy.start()
    pltpu.make_async_copy(send_buf, send_buf, send_sem).wait()
    pl.when(relays)(lambda: forward_copy().wait_send())
    stats = stat_send[...]
    pltpu.make_async_copy(stat_recv, stat_recv, stat_recv_sem).wait()
    for index in range(1, group):
        stats = stats + stat_recv[index - 1]
    profile_out[...] = (stats[0:1] / stats[1:2])[0, 0 : profile_out.shape[0]]
    pltpu.make_async_copy(stat_recv, stat_recv, stat_send_sem).wait()


def finish(held, ratio, update, profile, sems):
    stores = [pltpu.make_async_copy(held, update, sems.at[0]), pltpu.make_async_copy(ratio, profile, sems.at[1])]
    for store in stores:
        store.start()
    for store in stores:
        store.wait()


in_hbm = functools.partial(pltpu.with_memory_space_constraint, memory_space=pltpu.HBM)
in_vmem = functools.partial(pltpu.with_memory_space_constraint, memory_space=pltpu.VMEM)


def solution(mesh):
    sizes = tuple(mesh.shape[axis] for axis in AXES)
    group = mesh.shape["gz"] * mesh.shape["gy"]

    def local(source, start_guess, gauge_links, clover):
        times, depth, flat = source.shape[3:]
        assert sizes[0] > 1 and sizes[1] % 2 == 0
        assert times == depth == BLOCK and flat == LANE == BLOCK * LX
        tiles = (times * depth // SUB, SUB, LANE)
        spinor = source.shape[:3] + tiles
        gauge = gauge_links.shape[:4] + tiles
        site = clover.shape[:4] + tiles
        face = (12, 3) + tiles
        f32 = jnp.float32
        update, profile = pl.pallas_call(
            functools.partial(kernel, sizes),
            out_shape=(pltpu.VMEM(spinor, f32), pltpu.VMEM((times,), f32)),
            in_specs=[pl.BlockSpec(memory_space=pltpu.HBM)] * 4,
            out_specs=(pl.BlockSpec(memory_space=pltpu.VMEM),) * 2,
            scratch_shapes=[
                pltpu.VMEM(spinor, f32),
                pltpu.VMEM(spinor, f32),
                pltpu.VMEM(gauge, f32),
                pltpu.VMEM(site, f32),
                pltpu.VMEM((2, 4, 3, 3, 3) + tiles, f32),
                pltpu.VMEM((2, len(PAIRS), 2) + tiles, f32),
                pltpu.VMEM(spinor, f32),
                pltpu.VMEM(spinor, f32),
                pltpu.VMEM(spinor, f32),
                pltpu.VMEM(spinor, f32),
                pltpu.VMEM((2, SUB, LANE), f32),
                pltpu.VMEM((2, 4, 2, 2, 3) + tiles, f32),
                pltpu.VMEM((2, 4, 3, SUB, LANE), f32),
                pltpu.VMEM((2, 4, 3, SUB, LANE), f32),
                pltpu.VMEM((2, 3, 2, 2, 3, SUB, LANE), f32),
                pltpu.VMEM((2, 3, 3, 3, 3, SUB, LANE), f32),
                pltpu.VMEM((3, 3, 3, SUB, LANE), f32),
                pltpu.VMEM((2, 6, SUB, LANE), f32),
                pltpu.VMEM((2, len(PAIRS), 3, SUB, LANE), f32),
                pltpu.VMEM((3, 2, 3, 2) + tiles, f32),
                pltpu.VMEM(face, f32),
                pltpu.VMEM(face, f32),
                pltpu.VMEM(face[1:], f32),
                pltpu.VMEM((2, LANE), f32),
                pltpu.VMEM((group - 1, 2, LANE), f32),
                pltpu.SemaphoreType.DMA((7,)),
                pltpu.SemaphoreType.DMA,
                pltpu.SemaphoreType.DMA((6,)),
                pltpu.SemaphoreType.DMA((2,)),
                pltpu.SemaphoreType.DMA,
                pltpu.SemaphoreType.DMA,
            ],
            compiler_params=pltpu.CompilerParams(
                collective_id=0, has_side_effects=True, vmem_limit_bytes=VMEM_LIMIT,
            ),
        )(
            in_hbm(start_guess.reshape(spinor)),
            in_hbm(source.reshape(spinor)),
            in_hbm(gauge_links.reshape(gauge)),
            in_hbm(clover.reshape(site)),
        )
        update, profile = pl.pallas_call(
            finish,
            out_shape=(jax.ShapeDtypeStruct(spinor, f32), jax.ShapeDtypeStruct((times,), f32)),
            in_specs=[pl.BlockSpec(memory_space=pltpu.VMEM)] * 2,
            out_specs=(pl.BlockSpec(memory_space=pl.ANY),) * 2,
            scratch_shapes=[pltpu.SemaphoreType.DMA((2,))],
        )(
            in_vmem(update),
            in_vmem(profile),
        )
        return update.reshape(source.shape), profile

    spinor_spec = P(None, None, None, "ta", "gz", "gy")
    matrix_spec = P(None, None, None, None, "ta", "gz", "gy")
    return jax.shard_map(
        local,
        mesh=mesh,
        in_specs=(spinor_spec, spinor_spec, matrix_spec, matrix_spec),
        out_specs=(spinor_spec, P("ta")),
        check_vma=False,
    )
```

```python
import functools

import jax
import jax.numpy as jnp
from jax import lax
from jax.experimental import pallas as pl
from jax.experimental.pallas import tpu as pltpu
from jax.sharding import PartitionSpec as P

LX = 32
BLOCK = 4
MR_STEPS = 4
EPSILON = 1e-6
AXES = ("ta", "gz", "gy")
RE, IM = 0, 1
SUB, LANE = 8, 128
VMEM_LIMIT = 24 * 2**20

PAIR = (
    {(0, RE): (1, RE, 0), (0, IM): (1, IM, 0), (1, RE): (1, RE, 1), (1, IM): (1, IM, 1)},
    {(0, RE): (1, IM, 0), (0, IM): (-1, RE, 0), (1, RE): (-1, IM, 1), (1, IM): (1, RE, 1)},
    {(0, RE): (-1, RE, 1), (0, IM): (-1, IM, 1), (1, RE): (1, RE, 0), (1, IM): (1, IM, 0)},
    {(0, RE): (1, IM, 1), (0, IM): (-1, RE, 1), (1, RE): (1, IM, 0), (1, IM): (-1, RE, 0)},
)
PAIR_H = (
    {(0, RE): (1, RE, 0), (0, IM): (1, IM, 0), (1, RE): (1, RE, 1), (1, IM): (1, IM, 1)},
    {(0, RE): (-1, IM, 0), (0, IM): (1, RE, 0), (1, RE): (1, IM, 1), (1, IM): (-1, RE, 1)},
    {(0, RE): (1, RE, 1), (0, IM): (1, IM, 1), (1, RE): (-1, RE, 0), (1, IM): (-1, IM, 0)},
    {(0, RE): (-1, IM, 1), (0, IM): (1, RE, 1), (1, RE): (-1, IM, 0), (1, IM): (1, RE, 0)},
)


PAIRS = {pair: i for i, pair in enumerate((low, high) for high in range(6) for low in range(high))}


def signed_add(base, sign, value):
    return base + value if sign > 0 else base - value


def project(field, mu, s):
    parts = ([], [])
    for part in (RE, IM):
        for colour in range(3):
            spins = []
            for spin in range(2):
                sign, from_part, from_spin = PAIR[mu][(spin, part)]
                spins.append(
                    signed_add(field[part, spin, colour], -s * sign, field[from_part, 2 + from_spin, colour])
                )
            parts[part].append(jnp.stack(spins))
    return parts


def link_row(links, mu, row, half):
    re = im = None
    for col in range(3):
        u_re, u_im = links[mu, RE, row, col][None], links[mu, IM, row, col][None]
        h_re, h_im = half[RE][col], half[IM][col]
        t_re = u_re * h_re - u_im * h_im
        t_im = u_re * h_im + u_im * h_re
        re, im = (t_re, t_im) if re is None else (re + t_re, im + t_im)
    return re, im


def adjoint_row(links, mu, row, half):
    re = im = None
    for col in range(3):
        u_re, u_im = links[mu, RE, col, row][None], links[mu, IM, col, row][None]
        h_re, h_im = half[RE][col], half[IM][col]
        t_re = u_re * h_re + u_im * h_im
        t_im = u_re * h_im - u_im * h_re
        re, im = (t_re, t_im) if re is None else (re + t_re, im + t_im)
    return re, im


def add_hops(acc, mu, colour, ahead, behind):
    difference = tuple(b - a for a, b in zip(ahead, behind))
    for part in (RE, IM):
        acc[part, 0:2, colour] += ahead[part] + behind[part]
        for spin in range(2):
            sign, from_part, from_spin = PAIR_H[mu][(spin, part)]
            old = acc[part, 2 + spin, colour]
            acc[part, 2 + spin, colour] = signed_add(old, sign, difference[from_part][from_spin])


def site_term(clover, field, emit):
    def pair(part, index):
        return jnp.stack([field[part, index // 3, index % 3], field[part, 2 + index // 3, index % 3]])

    vec = [[pair(part, j) for j in range(6)] for part in (RE, IM)]
    for row in range(6):
        diagonal = clover[:, RE, row, row]
        re, im = diagonal * vec[RE][row], diagonal * vec[IM][row]
        for col in range(6):
            if col == row:
                continue
            low, high = min(row, col), max(row, col)
            m_re, m_im = clover[:, RE, low, high], clover[:, IM, low, high]
            if row < col:
                re = re + m_re * vec[RE][col] - m_im * vec[IM][col]
                im = im + m_re * vec[IM][col] + m_im * vec[RE][col]
            else:
                re = re + m_re * vec[RE][col] + m_im * vec[IM][col]
                im = im + m_re * vec[IM][col] - m_im * vec[RE][col]
        for chirality in range(2):
            emit(RE, 2 * chirality + row // 3, row % 3, re[chirality])
            emit(IM, 2 * chirality + row // 3, row % 3, im[chirality])


def three_products(first, second, third, re, im, both):
    def dot(weights, values):
        total = None
        for weight, value in zip(weights, values):
            total = weight * value if total is None else total + weight * value
        return total

    shared = dot(first, both)
    return shared - dot(third, im), shared + dot(second, re)


def block_site_term(diagonals, triples, field, emit):
    for chirality in range(2):
        vec = [[field(part, 2 * chirality + j // 3, j % 3) for j in range(6)] for part in (RE, IM)]
        both = [r + i for r, i in zip(*vec)]
        for row in range(6):
            diagonal = diagonals(chirality, row)
            re, im, shared = diagonal * vec[RE][row], diagonal * vec[IM][row], None
            for col in range(6):
                if col == row:
                    continue
                low, high = min(row, col), max(row, col)
                real, less, more = triples(chirality, low, high)
                term = real * both[col]
                shared = term if shared is None else shared + term
                if row < col:
                    re, im = re - more * vec[IM][col], im + less * vec[RE][col]
                else:
                    re, im = re + less * vec[IM][col], im - more * vec[RE][col]
            emit(RE, 2 * chirality + row // 3, row % 3, re + shared)
            emit(IM, 2 * chirality + row // 3, row % 3, im + shared)


def swap_halves(value):
    axis = value.ndim - 3
    return jnp.concatenate(
        [lax.slice_in_dim(value, 1, 2, axis=axis), lax.slice_in_dim(value, 0, 1, axis=axis)], axis=axis
    )


def turn(value, shift, axis):
    shift = shift % value.shape[axis]
    return pltpu.roll(value, shift, axis) if shift else value


def cyclic(value, mu, units, early):
    axis = value.ndim - 2
    if mu == 3:
        return turn(value, units, axis + 1)
    if mu == 2:
        return turn(value, units * LX, axis + 1)
    if mu == 1:
        return turn(value, units, axis)
    units = units % BLOCK
    if units == 0:
        return value
    if units == 2:
        return swap_halves(value)
    rolled = turn(value, BLOCK, axis)
    swapped = swap_halves(rolled)
    return jnp.where(early, swapped, rolled) if units == 1 else jnp.where(early, rolled, swapped)


def kernel(
    sizes, x_in, source_in, links_in, clover_in, update_out, profile_out,
    x, source, links, clover, inner, twist, rest, corr, acc, twice, alpha, halves, edge, edge_out, edge_halves,
    edge_inner, edge_time, edge_diagonal, edge_pair, behind_store,
    send_buf, recv_buf, relay_buf, stat_send, stat_recv,
    in_sem, send_sem, recv_sem, relay_sem, stat_send_sem, stat_recv_sem,
):
    count = {axis: size for axis, size in zip(AXES, sizes)}
    group = count["gz"] * count["gy"]
    me = {axis: lax.axis_index(axis) for axis in AXES}

    def peer(index):
        return {
            "gz": lax.rem(me["gz"] + index // count["gy"], count["gz"]),
            "gy": lax.rem(me["gy"] + index % count["gy"], count["gy"]),
        }

    def distance(index):
        depth, width = index // count["gy"], index % count["gy"]
        return min(depth, count["gz"] - depth) + min(width, count["gy"] - width)

    def spread(index):
        depth = index // count["gy"]
        return 2 * min(depth, count["gz"] - depth) + 3 * (index % count["gy"] != 0)

    def beside(axis, step):
        return {axis: lax.rem(me[axis] + step + count[axis], count[axis])}

    barrier = pltpu.get_barrier_semaphore()
    opens, closes = me["ta"] == 0, me["ta"] == count["ta"] - 1
    outer_core = lax.rem(me["gz"], 2)
    through = me["gz"] + jnp.where(jnp.logical_and(closes, outer_core == 0), 1, 0)
    for target in ({"gz": through, **beside("ta", 1)}, beside("ta", -1)):
        pl.semaphore_signal(barrier, inc=1, device_id=target, device_id_type=pl.DeviceIdType.MESH)
    loads = [pltpu.make_async_copy(x_in, x, in_sem.at[0])]
    loads += [pltpu.make_async_copy(links_in.at[mu], links.at[mu], in_sem.at[1 + mu]) for mu in range(4)]
    loads.append(pltpu.make_async_copy(clover_in, clover, in_sem.at[5]))
    loads.append(pltpu.make_async_copy(source_in, source, in_sem.at[6]))
    for load in loads:
        load.start()

    greeted = [index for index in range(1, group) if distance(index) == 1 or distance(index) > 3]
    for index in greeted:
        pl.semaphore_signal(barrier, inc=1, device_id=peer(index), device_id_type=pl.DeviceIdType.MESH)

    site = (2, SUB, LANE)
    row = lax.broadcasted_iota(jnp.int32, site, 1)
    lane = lax.broadcasted_iota(jnp.int32, site, 2)
    coord = (
        lax.broadcasted_iota(jnp.int32, site, 0) * 2 + row // BLOCK,
        row % BLOCK,
        lane // LX,
        lane % LX,
    )
    early = row < BLOCK
    row8 = lax.broadcasted_iota(jnp.int32, (SUB, LANE), 0)
    lane8 = lax.broadcasted_iota(jnp.int32, (SUB, LANE), 1)
    early8 = row8 < BLOCK
    high = tuple(c % BLOCK == BLOCK - 1 for c in coord)

    def x_neighbour(value, step):
        axis = value.ndim - 1
        if step > 0:
            return jnp.where(coord[3] == LX - 1, turn(value, LX - 1, axis), turn(value, -1, axis))
        return jnp.where(coord[3] == 0, turn(value, 1 - LX, axis), turn(value, 1, axis))

    def flat(half):
        return [half[part][colour][spin] for part in (RE, IM) for spin in range(2) for colour in range(3)]

    def pack(half, mu, edge, store, factor=None):
        values = flat(half)
        for j in range(3):
            packed = cyclic(values[4 * j], mu, -edge, early)
            for k in range(1, BLOCK):
                packed = jnp.where(coord[mu] == k, cyclic(values[4 * j + k], mu, k - edge, early), packed)
            store[j] = packed if factor is None else packed * factor

    def unpack(store, mu, edge):
        values = []
        for j in range(3):
            packed = store[j]
            values += [cyclic(packed, mu, edge - k, early) for k in range(BLOCK)]
        return [[jnp.stack([values[6 * p + c], values[6 * p + 3 + c]]) for c in range(3)] for p in (RE, IM)]

    def face_copy(turn_index, mu, side):
        slot = turn_index * 6 + mu * 2 + side
        return pltpu.make_async_remote_copy(
            src_ref=send_buf.at[slot],
            dst_ref=recv_buf.at[slot],
            send_sem=send_sem,
            recv_sem=recv_sem.at[turn_index * 3 + mu],
            device_id=beside(AXES[mu], -1 if side == 0 else 1),
            device_id_type=pl.DeviceIdType.MESH,
        )

    def faces_wait(turn_index, mu):
        pair = recv_buf.at[pl.ds(turn_index * 6 + mu * 2, 2)]
        pltpu.make_async_copy(pair, pair, recv_sem.at[turn_index * 3 + mu]).wait()

    def relay_copy():
        return pltpu.make_async_remote_copy(
            src_ref=send_buf.at[0],
            dst_ref=relay_buf,
            send_sem=send_sem,
            recv_sem=relay_sem.at[0],
            device_id={"gz": me["gz"] + 1 - 2 * outer_core},
            device_id_type=pl.DeviceIdType.MESH,
        )

    def forward_copy():
        return pltpu.make_async_remote_copy(
            src_ref=relay_buf,
            dst_ref=recv_buf.at[0],
            send_sem=relay_sem.at[1],
            recv_sem=recv_sem.at[0],
            device_id={"gz": me["gz"] + 1 - 2 * outer_core, **beside("ta", -1)},
            device_id_type=pl.DeviceIdType.MESH,
        )

    relays = jnp.logical_and(opens, outer_core == 1)

    def start_wrapped_first(turn_index):
        last = me["ta"] == count["ta"] - 1

        @pl.when(last)
        def _():
            face_copy(turn_index, 0, 1).start()
            face_copy(turn_index, 0, 0).start()

        @pl.when(jnp.logical_not(last))
        def _():
            face_copy(turn_index, 0, 0).start()
            face_copy(turn_index, 0, 1).start()

    first_t = jnp.where(me["ta"] == 0, -1.0, 1.0).astype(jnp.float32)
    last_t = jnp.where(me["ta"] == count["ta"] - 1, -1.0, 1.0).astype(jnp.float32)

    def prepare_ahead(turn_index, field, mu):
        pack(project(field, mu, 1), mu, 0, send_buf.at[turn_index * 6 + mu * 2], first_t if mu == 0 else None)

    def prepare_behind(turn_index, field, mu, keep):
        half = project(field, mu, -1)
        rows = [adjoint_row(links, mu, a, half) for a in range(3)]
        behind = [[rows[a][part] for a in range(3)] for part in (RE, IM)]
        pack(behind, mu, BLOCK - 1, send_buf.at[turn_index * 6 + mu * 2 + 1], last_t if mu == 0 else None)
        if keep:
            for part in (RE, IM):
                for a in range(3):
                    behind_store[mu, part, a] = behind[part][a]

    follows = jnp.logical_not(opens)

    def enter():
        pl.semaphore_wait(barrier, len(greeted) + 2 + jnp.where(opens, 2 * outer_core - 1, 0))

    loads[0].wait()
    prepare_ahead(0, x, 0)
    loads[1].wait()
    prepare_behind(0, x, 0, True)

    @pl.when(follows)
    def _():
        enter()
        start_wrapped_first(0)

    prepare_ahead(0, x, 2)
    pl.when(follows)(lambda: face_copy(0, 2, 0).start())
    loads[3].wait()
    prepare_behind(0, x, 2, True)
    pl.when(follows)(lambda: face_copy(0, 2, 1).start())
    prepare_ahead(0, x, 1)
    pl.when(follows)(lambda: face_copy(0, 1, 0).start())
    loads[2].wait()
    prepare_behind(0, x, 1, True)
    pl.when(follows)(lambda: face_copy(0, 1, 1).start())

    @pl.when(opens)
    def _():
        enter()

        @pl.when(outer_core == 0)
        def _():
            relay_copy().start()

        @pl.when(outer_core == 1)
        def _():
            relay_copy().wait_recv()
            forward_copy().start()
            face_copy(0, 0, 0).start()

        for mu, side in ((0, 1), (1, 0), (1, 1), (2, 0), (2, 1)):
            face_copy(0, mu, side).start()

    def zero_acc():
        acc[...] = jnp.zeros_like(acc)

    zero_acc()
    loads[4].wait()

    def x_hops(field):
        ahead_half = [[x_neighbour(v, 1) for v in values] for values in project(field, 3, 1)]
        behind_half = project(field, 3, -1)
        for a in range(3):
            ahead = link_row(links, 3, a, ahead_half)
            behind = tuple(x_neighbour(v, -1) for v in adjoint_row(links, 3, a, behind_half))
            yield a, ahead, behind

    for a, ahead, behind in x_hops(x):
        add_hops(acc, 3, a, ahead, behind)

    for mu in range(4):
        factor = jnp.where(high[mu], 0.0, -0.5).astype(jnp.float32)
        for a in range(3):
            for b in range(3):
                re, im = links[mu, RE, a, b] * factor, links[mu, IM, a, b] * factor
                inner[0, mu, 0, a, b] = re
                inner[0, mu, 1, a, b] = im - re
                inner[0, mu, 2, a, b] = im + re
                re, im = cyclic(re, mu, 1, early), cyclic(im, mu, 1, early)
                inner[1, mu, 0, b, a] = re
                inner[1, mu, 1, b, a] = -im - re
                inner[1, mu, 2, b, a] = re - im

    loads[5].wait()
    for chirality in range(2):
        for (low, high_row), index in PAIRS.items():
            re, im = clover[chirality, RE, low, high_row], clover[chirality, IM, low, high_row]
            twist[chirality, index, 0] = im - re
            twist[chirality, index, 1] = im + re
    def outer(first, second):
        return jnp.where(early8, first, second)

    for index in range(2):
        for mu in range(1, 4):
            for form in range(3):
                for a in range(3):
                    for b in range(3):
                        edge_inner[index, mu - 1, form, a, b] = outer(*(inner[index, mu, form, a, b, i] for i in range(2)))
    for form in range(3):
        for a in range(3):
            for b in range(3):
                edge_time[form, a, b] = outer(inner[0, 0, form, a, b, 1], inner[1, 0, form, a, b, 0])
    for chirality in range(2):
        for a in range(6):
            edge_diagonal[chirality, a] = outer(*(clover[chirality, RE, a, a, i] for i in range(2)))
        for (low, high_row), index in PAIRS.items():
            edge_pair[chirality, index, 0] = outer(*(clover[chirality, RE, low, high_row, i] for i in range(2)))
            for form in range(2):
                edge_pair[chirality, index, 1 + form] = outer(*(twist[chirality, index, form, i] for i in range(2)))
    loads[6].wait()

    def emit_rest(part, spin, colour, value):
        rest[part, spin, colour] = source[part, spin, colour] - value

    site_term(clover, x, emit_rest)
    source_sq = jnp.zeros(site, jnp.float32)
    for part in (RE, IM):
        for spin in range(4):
            for colour in range(3):
                value = source[part, spin, colour]
                source_sq = source_sq + value * value

    def slice_sums(value, time):
        sums = jnp.broadcast_to(jnp.sum(value, axis=1, keepdims=True), (SUB, LANE))
        return jnp.sum(jnp.where(time == lane8, sums, 0.0), axis=0, keepdims=True)

    stat_send[1:2] = slice_sums(source_sq[0], coord[0][0]) + slice_sums(source_sq[1], coord[0][1])

    local = project(x, 0, 1)
    ahead_half = [
        [jnp.where(coord[0] == BLOCK - 1, 0.0, cyclic(local[part][c], 0, -1, early)) for c in range(3)]
        for part in (RE, IM)
    ]
    for a in range(3):
        ahead = link_row(links, 0, a, ahead_half)
        behind = tuple(
            jnp.where(coord[0] == 0, 0.0, cyclic(behind_store[0, part, a], 0, 1, early)) for part in (RE, IM)
        )
        add_hops(acc, 0, a, ahead, behind)

    for mu in (1, 2):
        faces_wait(0, mu)
        arrived = unpack(recv_buf.at[mu * 2], mu, BLOCK - 1)
        local = project(x, mu, 1)
        ahead_half = [
            [
                jnp.where(coord[mu] == BLOCK - 1, arrived[part][c], cyclic(local[part][c], mu, -1, early))
                for c in range(3)
            ]
            for part in (RE, IM)
        ]
        below = unpack(recv_buf.at[mu * 2 + 1], mu, 0)
        for a in range(3):
            ahead = link_row(links, mu, a, ahead_half)
            behind = tuple(
                jnp.where(coord[mu] == 0, below[part][a], cyclic(behind_store[mu, part, a], mu, 1, early))
                for part in (RE, IM)
            )
            add_hops(acc, mu, a, ahead, behind)

    for part in (RE, IM):
        for spin in range(4):
            rest[part, spin] += 0.5 * acc[part, spin]
            corr[part, spin] = jnp.zeros_like(corr[part, spin])

    def block_sums(values):
        packed = None
        for index, value in enumerate(values):
            total = jnp.sum(value, axis=0, keepdims=True)
            total = jnp.broadcast_to(total, (SUB, LANE))
            packed = total if packed is None else jnp.where(row8 == index, total, packed)
        place = lane8 % BLOCK
        total = None
        for offset in range(1 - BLOCK, BLOCK):
            moved = [turn(packed, start - offset, 1) for start in range(0, LANE, LX)]
            while len(moved) > 1:
                moved = [p + q for p, q in zip(moved[::2], moved[1::2])]
            part = moved[0]
            if offset:
                part = jnp.where((place + offset >= 0) & (place + offset < BLOCK), part, 0.0)
            total = part if total is None else total + part
        packed = total
        return [jnp.broadcast_to(packed[i : i + 1], (SUB, LANE)) for i in range(len(values))]

    def store_halves(origin):
        for mu in (3, 2, 1, 0):
            for index, s in enumerate((1, -1)):
                half = project(origin, mu, s)
                for part in (RE, IM):
                    for colour in range(3):
                        moved = cyclic(half[part][colour], mu, -s, early)
                        for spin in range(2):
                            halves[index, mu, part, spin, colour] = moved[spin]

    def site_apply(origin, target):
        for tile in range(2):
            def emit(part, spin, colour, value):
                target[part, spin, colour, tile] = value

            block_site_term(
                lambda chirality, row: clover[chirality, RE, row, row, tile],
                lambda chirality, low, high: (
                    clover[chirality, RE, low, high, tile],
                    twist[chirality, PAIRS[low, high], 0, tile],
                    twist[chirality, PAIRS[low, high], 1, tile],
                ),
                lambda part, spin, colour: origin[part, spin, colour, tile],
                emit,
            )

    def gather_hop(total, mu, index, got):
        for part in (RE, IM):
            for spin in range(2):
                total[part, spin] = total[part, spin] + got[spin][part]
                sign, from_part, from_spin = PAIR_H[mu][(spin, part)]
                total[part, 2 + spin] = signed_add(
                    total[part, 2 + spin], sign if index else -sign, got[from_spin][from_part]
                )

    def add_inner_hops(target):
        for tile in range(2):
            total = {
                (row, part, spin): target[part, spin, row, tile]
                for row in range(3) for part in (RE, IM) for spin in range(4)
            }
            for mu in range(4):
                for index in range(2):
                    vectors = []
                    for spin in range(2):
                        re, im = ([halves[index, mu, part, spin, c, tile] for c in range(3)] for part in (RE, IM))
                        vectors.append((re, im, [r + i for r, i in zip(re, im)]))
                    for row in range(3):
                        weights = [[inner[index, mu, form, row, col, tile] for col in range(3)] for form in range(3)]
                        got = [three_products(*weights, *vector) for vector in vectors]
                        part_total = {(p, sp): total[row, p, sp] for p in (RE, IM) for sp in range(4)}
                        gather_hop(part_total, mu, index, got)
                        for (p, sp), value in part_total.items():
                            total[row, p, sp] = value
            for (row, part, spin), value in total.items():
                target[part, spin, row, tile] = value

    def time_faces(turn_index):
        later, sooner = [], []
        for j in range(3):
            packed = recv_buf[turn_index * 6, j]
            moved = turn(packed, BLOCK, 1)
            later += [moved[0], packed[0], moved[1], packed[1]]
            packed = recv_buf[turn_index * 6 + 1, j]
            moved = turn(packed, BLOCK, 1)
            sooner += [packed[0], moved[0], packed[1], moved[1]]
        hops = {}
        for spin in range(2):
            for a in range(3):
                ahead = [None, None]
                for c in range(3):
                    u_re, u_im = links[0, RE, a, c, 1], links[0, IM, a, c, 1]
                    h_re, h_im = later[3 * spin + c], later[6 + 3 * spin + c]
                    terms = u_re * h_re - u_im * h_im, u_re * h_im + u_im * h_re
                    ahead = [t if old is None else old + t for old, t in zip(ahead, terms)]
                for part in (RE, IM):
                    behind = 0.5 * sooner[6 * part + 3 * spin + a]
                    hops[part, spin, a] = jnp.where(early8, behind, 0.5 * ahead[part])
                    hops[part, 2 + spin, a] = jnp.where(early8, behind, -0.5 * ahead[part])
        return hops

    facing = jnp.where(early8, 1.0, -1.0).astype(jnp.float32)

    def add_edge_operator(hops):
        for key, value in hops.items():
            edge[key] = value
            rest[key + (0,)] += jnp.where(early8, value, 0.0)
            rest[key + (1,)] += jnp.where(early8, 0.0, value)
        for mu in (3, 2, 1):
            for index, s in enumerate((1, -1)):
                half = project(edge, mu, s)
                for part in (RE, IM):
                    for colour in range(3):
                        moved = cyclic(half[part][colour], mu, -s, early)
                        for spin in range(2):
                            edge_halves[index, mu - 1, part, spin, colour] = moved[spin]
        mixed = {
            (part, spin, colour): turn(hops[part, spin, colour] + facing * hops[part, 2 + spin, colour], BLOCK, 0)
            for part in (RE, IM) for spin in range(2) for colour in range(3)
        }

        def emit(part, spin, colour, value):
            edge_out[part, spin, colour] = value

        block_site_term(
            lambda chirality, row: edge_diagonal[chirality, row],
            lambda chirality, low, high: tuple(edge_pair[chirality, PAIRS[low, high], form] for form in range(3)),
            lambda part, spin, colour: edge[part, spin, colour],
            emit,
        )
        for row in range(3):
            total = {(part, spin): edge_out[part, spin, row] for part in (RE, IM) for spin in range(4)}
            for mu in range(1, 4):
                for index in range(2):
                    weights = [[edge_inner[index, mu - 1, form, row, col] for col in range(3)] for form in range(3)]
                    got = []
                    for spin in range(2):
                        re, im = ([edge_halves[index, mu - 1, part, spin, c] for c in range(3)] for part in (RE, IM))
                        got.append(three_products(*weights, re, im, [r + i for r, i in zip(re, im)]))
                    gather_hop(total, mu, index, got)
            weights = [[edge_time[form, row, col] for col in range(3)] for form in range(3)]
            for spin in range(2):
                re, im = ([mixed[part, spin, c] for c in range(3)] for part in (RE, IM))
                got = three_products(*weights, re, im, [r + i for r, i in zip(re, im)])
                for part in (RE, IM):
                    for lower, value in ((0, got[part]), (2, -facing * got[part])):
                        acc[part, lower + spin, row, 0] += jnp.where(early8, total[part, lower + spin], value)
                        acc[part, lower + spin, row, 1] += jnp.where(early8, value, total[part, lower + spin])

    def times_alpha(field, spin, colour, tile):
        re, im = field[RE, spin, colour, tile], field[IM, spin, colour, tile]
        a_re, a_im = alpha[0], alpha[1]
        return a_re * re - a_im * im, a_re * im + a_im * re

    def subtract_scaled(target, scaled, spin, colour, tile):
        for part in (RE, IM):
            target[part, spin, colour, tile] -= scaled[part]

    def next_margins():
        zero = jnp.zeros((SUB, LANE), jnp.float32)

        def one_tile(tile, carry):
            margin_re, margin_im, norm = carry
            for spin in range(4):
                for colour in range(3):
                    a_re, a_im = acc[RE, spin, colour, tile], acc[IM, spin, colour, tile]
                    r_re, r_im = rest[RE, spin, colour, tile], rest[IM, spin, colour, tile]
                    margin_re = margin_re + (a_re * r_re + a_im * r_im)
                    margin_im = margin_im + (a_re * r_im - a_im * r_re)
                    norm = norm + (a_re * a_re + a_im * a_im)
            return margin_re, margin_im, norm

        return one_tile(1, one_tile(0, (zero, zero, zero)))

    def set_alpha(margins):
        sum_re, sum_im, sum_norm = block_sums(margins)
        sum_norm = sum_norm + EPSILON
        alpha[0] = sum_re / sum_norm
        alpha[1] = sum_im / sum_norm

    def advance_correction(tile):
        for spin in range(4):
            for colour in range(3):
                scaled = times_alpha(rest, spin, colour, tile)
                for part in (RE, IM):
                    corr[part, spin, colour, tile] += scaled[part]

    def advance_rest(tile):
        for spin in range(4):
            for colour in range(3):
                subtract_scaled(rest, times_alpha(acc, spin, colour, tile), spin, colour, tile)

    def full_step(_, margins):
        set_alpha(margins)
        store_halves(acc)
        site_apply(acc, twice)
        add_inner_hops(twice)
        zero = jnp.zeros((SUB, LANE), jnp.float32)

        def one_tile(tile, carry):
            margin_re, margin_im, norm = carry
            advance_correction(tile)
            advance_rest(tile)
            for spin in range(4):
                for colour in range(3):
                    subtract_scaled(acc, times_alpha(twice, spin, colour, tile), spin, colour, tile)
                    a_re, a_im = acc[RE, spin, colour, tile], acc[IM, spin, colour, tile]
                    r_re, r_im = rest[RE, spin, colour, tile], rest[IM, spin, colour, tile]
                    margin_re = margin_re + (a_re * r_re + a_im * r_im)
                    margin_im = margin_im + (a_re * r_im - a_im * r_re)
                    norm = norm + (a_re * a_re + a_im * a_im)
            return margin_re, margin_im, norm

        return one_tile(1, one_tile(0, (zero, zero, zero)))

    store_halves(rest)
    site_apply(rest, acc)
    add_inner_hops(acc)
    faces_wait(0, 0)
    add_edge_operator(time_faces(0))
    margins = lax.fori_loop(0, MR_STEPS - 1, full_step, next_margins())
    def time_edge(field, tile, s):
        half = [
            [[signed_add(field[part, spin, c, tile], -s, field[part, 2 + spin, c, tile]) for c in range(3)] for spin in range(2)]
            for part in (RE, IM)
        ]
        if s > 0:
            return half
        rows = [[[None] * 3 for _ in range(2)] for _ in range(2)]
        for spin in range(2):
            for a in range(3):
                for c in range(3):
                    u_re, u_im = links[0, RE, c, a, tile], links[0, IM, c, a, tile]
                    h_re, h_im = half[RE][spin][c], half[IM][spin][c]
                    for part, term in ((RE, u_re * h_re + u_im * h_im), (IM, u_re * h_im - u_im * h_re)):
                        old = rows[part][spin][a]
                        rows[part][spin][a] = term if old is None else old + term
        return rows

    def send_time_edge(side, known, residual, factor):
        a_re, a_im = alpha[0], alpha[1]
        values = [[], []]
        for spin in range(2):
            for c in range(3):
                r_re, r_im = residual[RE][spin][c], residual[IM][spin][c]
                values[RE].append((known[RE][spin][c] + (a_re * r_re - a_im * r_im)) * factor)
                values[IM].append((known[IM][spin][c] + (a_re * r_im + a_im * r_re)) * factor)
        values = values[RE] + values[IM]
        for j in range(3):
            for tile in range(2):
                first, second = values[4 * j + 2 * tile], values[4 * j + 2 * tile + 1]
                if side:
                    first = turn(first, BLOCK, 0)
                else:
                    second = turn(second, BLOCK, 0)
                send_buf[6 + side, j, tile] = outer(first, second)

    known = [time_edge(corr, 0, 1), time_edge(corr, 1, -1)]
    residual = [time_edge(rest, 0, 1), time_edge(rest, 1, -1)]
    set_alpha(margins)
    send_time_edge(1, known[1], residual[1], last_t)
    pl.when(closes)(lambda: face_copy(1, 0, 1).start())
    send_time_edge(0, known[0], residual[0], first_t)
    face_copy(1, 0, 0).start()
    pl.when(jnp.logical_not(closes))(lambda: face_copy(1, 0, 1).start())
    for tile in range(2):
        advance_correction(tile)
    for mu in (2, 1):
        prepare_ahead(1, corr, mu)
        face_copy(1, mu, 0).start()
        prepare_behind(1, corr, mu, False)
        face_copy(1, mu, 1).start()
    for tile in range(2):
        advance_rest(tile)
    for part in (RE, IM):
        for spin in range(4):
            update_out[part, spin] = x[part, spin] + corr[part, spin]
    zero_acc()
    for a, ahead, behind in x_hops(corr):
        ahead = tuple(jnp.where(high[3], v, 0.0) for v in ahead)
        behind = tuple(jnp.where(coord[3] % BLOCK == 0, v, 0.0) for v in behind)
        add_hops(acc, 3, a, ahead, behind)
    for mu in (1, 2):
        faces_wait(1, mu)
        arrived = unpack(recv_buf.at[6 + mu * 2], mu, BLOCK - 1)
        below = unpack(recv_buf.at[6 + mu * 2 + 1], mu, 0)
        for a in range(3):
            ahead = tuple(jnp.where(high[mu], v, 0.0) for v in link_row(links, mu, a, arrived))
            behind = tuple(jnp.where(coord[mu] == 0, below[part][a], 0.0) for part in (RE, IM))
            add_hops(acc, mu, a, ahead, behind)
    middle_sq = edge_sq = jnp.zeros((SUB, LANE), jnp.float32)
    for part in (RE, IM):
        for spin in range(4):
            for colour in range(3):
                value = rest[part, spin, colour] + 0.5 * acc[part, spin, colour]
                edge[part, spin, colour] = outer(value[0], value[1])
                value = outer(value[1], value[0])
                middle_sq = middle_sq + value * value
    stat_send[0:1] = slice_sums(middle_sq, jnp.where(early8, 2, 1))
    faces_wait(1, 0)
    for key, value in time_faces(1).items():
        value = edge[key] + value
        edge_sq = edge_sq + value * value
    stat_send[0:1] += slice_sums(edge_sq, jnp.where(early8, 0, BLOCK - 1))

    stat_copies = [
        pltpu.make_async_remote_copy(
            src_ref=stat_send,
            dst_ref=stat_recv.at[index - 1],
            send_sem=stat_send_sem,
            recv_sem=stat_recv_sem,
            device_id=peer(index),
            device_id_type=pl.DeviceIdType.MESH,
        )
        for index in sorted(range(1, group), key=lambda i: -spread(i))
    ]
    for copy in stat_copies:
        copy.start()
    pltpu.make_async_copy(send_buf, send_buf, send_sem).wait()
    pl.when(relays)(lambda: forward_copy().wait_send())
    stats = stat_send[...]
    pltpu.make_async_copy(stat_recv, stat_recv, stat_recv_sem).wait()
    for index in range(1, group):
        stats = stats + stat_recv[index - 1]
    profile_out[...] = (stats[0:1] / stats[1:2])[0, 0 : profile_out.shape[0]]
    pltpu.make_async_copy(stat_recv, stat_recv, stat_send_sem).wait()


def finish(held, ratio, update, profile, sems):
    stores = [pltpu.make_async_copy(held, update, sems.at[0]), pltpu.make_async_copy(ratio, profile, sems.at[1])]
    for store in stores:
        store.start()
    for store in stores:
        store.wait()


in_hbm = functools.partial(pltpu.with_memory_space_constraint, memory_space=pltpu.HBM)
in_vmem = functools.partial(pltpu.with_memory_space_constraint, memory_space=pltpu.VMEM)


def solution(mesh):
    sizes = tuple(mesh.shape[axis] for axis in AXES)
    group = mesh.shape["gz"] * mesh.shape["gy"]

    def local(source, start_guess, gauge_links, clover):
        times, depth, flat = source.shape[3:]
        assert sizes[0] > 1 and sizes[1] % 2 == 0
        assert times == depth == BLOCK and flat == LANE == BLOCK * LX
        tiles = (times * depth // SUB, SUB, LANE)
        spinor = source.shape[:3] + tiles
        gauge = gauge_links.shape[:4] + tiles
        site = clover.shape[:4] + tiles
        face = (12, 3) + tiles
        f32 = jnp.float32
        update, profile = pl.pallas_call(
            functools.partial(kernel, sizes),
            out_shape=(pltpu.VMEM(spinor, f32), pltpu.VMEM((times,), f32)),
            in_specs=[pl.BlockSpec(memory_space=pltpu.HBM)] * 4,
            out_specs=(pl.BlockSpec(memory_space=pltpu.VMEM),) * 2,
            scratch_shapes=[
                pltpu.VMEM(spinor, f32),
                pltpu.VMEM(spinor, f32),
                pltpu.VMEM(gauge, f32),
                pltpu.VMEM(site, f32),
                pltpu.VMEM((2, 4, 3, 3, 3) + tiles, f32),
                pltpu.VMEM((2, len(PAIRS), 2) + tiles, f32),
                pltpu.VMEM(spinor, f32),
                pltpu.VMEM(spinor, f32),
                pltpu.VMEM(spinor, f32),
                pltpu.VMEM(spinor, f32),
                pltpu.VMEM((2, SUB, LANE), f32),
                pltpu.VMEM((2, 4, 2, 2, 3) + tiles, f32),
                pltpu.VMEM((2, 4, 3, SUB, LANE), f32),
                pltpu.VMEM((2, 4, 3, SUB, LANE), f32),
                pltpu.VMEM((2, 3, 2, 2, 3, SUB, LANE), f32),
                pltpu.VMEM((2, 3, 3, 3, 3, SUB, LANE), f32),
                pltpu.VMEM((3, 3, 3, SUB, LANE), f32),
                pltpu.VMEM((2, 6, SUB, LANE), f32),
                pltpu.VMEM((2, len(PAIRS), 3, SUB, LANE), f32),
                pltpu.VMEM((3, 2, 3, 2) + tiles, f32),
                pltpu.VMEM(face, f32),
                pltpu.VMEM(face, f32),
                pltpu.VMEM(face[1:], f32),
                pltpu.VMEM((2, LANE), f32),
                pltpu.VMEM((group - 1, 2, LANE), f32),
                pltpu.SemaphoreType.DMA((7,)),
                pltpu.SemaphoreType.DMA,
                pltpu.SemaphoreType.DMA((6,)),
                pltpu.SemaphoreType.DMA((2,)),
                pltpu.SemaphoreType.DMA,
                pltpu.SemaphoreType.DMA,
            ],
            compiler_params=pltpu.CompilerParams(
                collective_id=0, has_side_effects=True, vmem_limit_bytes=VMEM_LIMIT,
            ),
        )(
            in_hbm(start_guess.reshape(spinor)),
            in_hbm(source.reshape(spinor)),
            in_hbm(gauge_links.reshape(gauge)),
            in_hbm(clover.reshape(site)),
        )
        update, profile = pl.pallas_call(
            finish,
            out_shape=(jax.ShapeDtypeStruct(spinor, f32), jax.ShapeDtypeStruct((times,), f32)),
            in_specs=[pl.BlockSpec(memory_space=pltpu.VMEM)] * 2,
            out_specs=(pl.BlockSpec(memory_space=pl.ANY),) * 2,
            scratch_shapes=[pltpu.SemaphoreType.DMA((2,))],
        )(
            in_vmem(update),
            in_vmem(profile),
        )
        return update.reshape(source.shape), profile

    spinor_spec = P(None, None, None, "ta", "gz", "gy")
    matrix_spec = P(None, None, None, None, "ta", "gz", "gy")
    return jax.shard_map(
        local,
        mesh=mesh,
        in_specs=(spinor_spec, spinor_spec, matrix_spec, matrix_spec),
        out_specs=(spinor_spec, P("ta")),
        check_vma=False,
    )
```
